32 devices in a mesh: dp: 8 (over y, x, core), tp: 4 (over z).
Axes of the slice: x: 2, y: 2, z: 4, core: 2. Of those that a mesh axis runs over, the one named last changes fastest.
Arguments:
- tokens: bfloat16 [32768, 768], P('dp'), may hold values from -6 to 6
- cotangent: bfloat16 [32768, 768], P('dp'), may hold values from -6 to 6
- size_tags: int32 [8], P('dp'), may hold values from 0 to 1
- time_index: int32 [32], replicated, may hold values from 0 to 999
- class_index: int32 [32], replicated, may hold values from 0 to 999
- time_table: bfloat16 [1000, 768], replicated, may hold values from -6 to 6
- class_table: bfloat16 [1000, 768], replicated, may hold values from -6 to 6
- w_mod: bfloat16 [768, 4608], P(None, 'tp'), may hold values from -0.21875 to 0.21875
- w_qkv: bfloat16 [768, 2304], P(None, 'tp'), may hold values from -0.21875 to 0.21875
- conv_qkv: bfloat16 [9, 2304], P(None, 'tp'), may hold values from -2 to 2
- w_out: bfloat16 [768, 768], P('tp'), may hold values from -0.75 to 0.75
- w_up: bfloat16 [768, 3072], P(None, 'tp'), may hold values from -0.21875 to 0.21875
- conv_ffn: bfloat16 [9, 3072], P(None, 'tp'), may hold values from -2 to 2
- w_down: bfloat16 [3072, 768], P('tp'), may hold values from -0.109375 to 0.109375
Outputs:
- mixed: bfloat16 [32768, 768], P('dp')
- grad_tokens: float32 [32768, 768], P(('dp', 'tp'))
- grad_time: float32 [1000, 768], P(None, 'dp')
- grad_class: float32 [1000, 768], P(None, 'dp')
- grad_mod: float32 [768, 4608], P('dp', 'tp')
- grad_qkv: float32 [768, 2304], P('dp', 'tp')
- grad_conv_qkv: float32 [9, 2304], P(None, ('tp', 'dp'))
- grad_out: float32 [768, 768], P('tp', 'dp')
- grad_up: float32 [768, 3072], P('dp', 'tp')
- grad_conv_ffn: float32 [9, 3072], P(None, ('tp', 'dp'))
- grad_down: float32 [3072, 768], P('tp', 'dp')
The draws below stay inside these ranges and needn't reach their ends.
Inputs may be any that keep to these rules, and one draw needn't show every extreme that they name: `size_tags`: 1: the buffer holds one item of 64 x 64 tokens and only its slot 0 is used; 0: four items, one in each quadrant of the grid, in slots of quadrant order.
All inputs are finite; a program needn't handle non-finite values.
Results may differ from the reference program's by a relative error of at most 0.018.
The reference program's roundings to bfloat16 on the way count: a program that leaves them out, or rounds other values in their place, can miss the bound.
Values may be sent and summed in bfloat16 or wider, within the bound.
A program may use at most 384 MiB of HBM per device.

```python
import jax
import jax.numpy as jnp
from jax import lax

D = 768
HEADS = 12
HEAD_SIZE = 64
FF = 3072
TSTEPS = 1000
CLASSES = 1000
SIDE = 64
SLOTS = 4
TOK_DEV = 4096
TOKENS = 32768
ITEMS = 32
N_DP = 8
N_TP = 4


def plant(values, rng, low, high):
    longest = values.shape.index(max(values.shape))
    spots = []
    for shift in (0, 1):
        where = [jax.random.randint(jax.random.fold_in(rng, axis), (), 0, length) for axis, length in enumerate(values.shape)]
        where[longest] = (where[longest] + shift) % values.shape[longest]
        spots.append(tuple(where))
    return values.at[spots[0]].set(low).at[spots[1]].set(high)


def levels(stream_key, dims, cuts, least, high):
    def one(dim, parts):
        heights = jax.random.uniform(jax.random.fold_in(jax.random.fold_in(stream_key, 6), dim), (parts,), jnp.float32, least / len(cuts), high / len(cuts))
        return jnp.repeat(jnp.exp(heights), dims[dim] // parts).reshape((-1,) + (1,) * (len(dims) - dim - 1))

    level = one(*cuts[0])
    for cut in cuts[1:]:
        level = level * one(*cut)
    return level


def scatter_about(rng, extent, deviation, bound, split=(), held_as=jnp.bfloat16):
    gain = levels(rng, extent, split, -0.22, 0.18) if split else 1.0
    array = jax.random.normal(rng, extent, jnp.float32) * deviation * gain
    return jnp.minimum(jnp.maximum(array, -bound), bound).astype(held_as)


def setup_inputs(seed: int = 0) -> dict:
    seeds = jax.random.split(jax.random.key(seed), 15)
    tokens = scatter_about(seeds[0], (TOKENS, D), 1.0, 6.0, ((0, 8),))
    cotangent = scatter_about(seeds[1], (TOKENS, D), 1.0, 6.0, ((0, 8),))
    size_tags = plant(jax.random.randint(seeds[2], (N_DP,), 0, 2), jax.random.fold_in(seeds[2], 1), 0, 1).astype(jnp.int32)
    time_index = plant(jax.random.randint(seeds[3], (ITEMS,), 0, TSTEPS), jax.random.fold_in(seeds[3], 1), 0, TSTEPS - 1).astype(jnp.int32)
    class_index = plant(jax.random.randint(seeds[4], (ITEMS,), 0, CLASSES), jax.random.fold_in(seeds[4], 1), 0, CLASSES - 1).astype(jnp.int32)
    time_table = scatter_about(seeds[5], (TSTEPS, D), 1.0, 6.0)
    class_table = scatter_about(seeds[6], (CLASSES, D), 1.0, 6.0)
    w_mod = scatter_about(seeds[7], (D, 6 * D), D ** -0.5, 0.21875, ((1, 4),))
    w_qkv = scatter_about(seeds[8], (D, 3 * D), D ** -0.5, 0.21875, ((1, 4),))
    conv_qkv = scatter_about(seeds[9], (9, 3 * D), 9 ** -0.5, 2.0, ((1, 4),))
    w_out = scatter_about(seeds[10], (D, D), HEAD_SIZE ** -0.5, 0.75, ((0, 4),))
    w_up = scatter_about(seeds[11], (D, FF), D ** -0.5, 0.21875, ((1, 4),))
    conv_ffn = scatter_about(seeds[12], (9, FF), 9 ** -0.5, 2.0, ((1, 4),))
    w_down = scatter_about(seeds[13], (FF, D), FF ** -0.5, 0.109375, ((0, 4),))
    return {"tokens": tokens, "cotangent": cotangent, "size_tags": size_tags, "time_index": time_index, "class_index": class_index, "time_table": time_table, "class_table": class_table, "w_mod": w_mod, "w_qkv": w_qkv, "conv_qkv": conv_qkv, "w_out": w_out, "w_up": w_up, "conv_ffn": conv_ffn, "w_down": w_down}


@jax.custom_vjp
def coarse_latent(v):
    return lax.optimization_barrier(v.astype(jnp.bfloat16)).astype(jnp.float32)

@jax.custom_vjp
def coarse_gradient(v):
    return v

def low_keep(v):
    return (coarse_latent(v), None)

def low_pass(kept, grad):
    return (grad,)

def back_keep(v):
    return (v, None)

def back_low(kept, grad):
    return (coarse_latent(grad),)
coarse_latent.defvjp(low_keep, low_pass)
coarse_gradient.defvjp(back_keep, back_low)
precise_setting = lax.Precision.HIGHEST

def layer_norm(values):
    average = lax.optimization_barrier(jnp.mean(values, axis=-1, keepdims=True))
    centred = values - average
    variance = lax.optimization_barrier(jnp.mean(centred * centred, axis=-1, keepdims=True))
    return centred * lax.rsqrt(variance + 1e-06)

def item_ids(size_tag, grid_side):
    row_index = lax.broadcasted_iota(jnp.int32, (grid_side, grid_side), 0)
    col_index = lax.broadcasted_iota(jnp.int32, (grid_side, grid_side), 1)
    quadrant = row_index // (grid_side // 2) * 2 + col_index // (grid_side // 2)
    return jnp.where(size_tag == 1, jnp.zeros_like(quadrant), quadrant)

def depthwise(field, kernel, labels):
    grid_side = field.shape[0]
    padded = jnp.pad(field, ((1, 1), (1, 1), (0, 0)))
    padded_ids = jnp.pad(labels, 1, constant_values=-1)
    result = jnp.zeros_like(field)
    for tap_index in range(9):
        row_off = tap_index // 3
        col_off = tap_index % 3
        moved = padded[row_off:row_off + grid_side, col_off:col_off + grid_side]
        same_item = padded_ids[row_off:row_off + grid_side, col_off:col_off + grid_side] == labels
        result = result + kernel[tap_index] * jnp.where(same_item[:, :, None], moved, jnp.zeros_like(moved))
    return result

def unshuffle(field):
    half_side = field.shape[0] // 2
    trailing = field.shape[2:]
    shaped = field.reshape((half_side, 2, half_side, 2) + trailing)
    order = (1, 3, 0, 2) + tuple(range(4, 4 + len(trailing)))
    return shaped.transpose(order).reshape((4, half_side * half_side) + trailing)

def shuffle(groups, grid_side):
    half_side = grid_side // 2
    trailing = groups.shape[2:]
    shaped = groups.reshape((2, 2, half_side, half_side) + trailing)
    order = (2, 0, 3, 1) + tuple(range(4, 4 + len(trailing)))
    return shaped.transpose(order).reshape((grid_side, grid_side) + trailing)

def group_attention(block, allowed):
    input_query = block[:, :, 0]
    input_keys = block[:, :, 1]
    input_values = block[:, :, 2]
    logit_scores = coarse_gradient(jnp.einsum('yoe,goe->oyg', input_query, input_keys, precision=precise_setting) * HEAD_SIZE ** (-0.5))
    logit_scores = jnp.where(allowed[None], logit_scores, -jnp.inf)
    probabilities = coarse_latent(jax.nn.softmax(logit_scores, axis=-1))
    return coarse_latent(coarse_gradient(jnp.einsum('xbg,gxy->bxy', probabilities, input_values, precision=precise_setting)))

def buffer_forward(params, buffer_tokens, size_tag, times, labels):
    time_table, class_table, w_mod, w_qkv, conv_qkv, w_out, w_up, conv_ffn, w_down = params
    half_side = SIDE // 2
    condition = time_table[times] + class_table[labels]
    activated = coarse_latent(jax.nn.silu(condition))
    modulation = jnp.dot(activated, w_mod, precision=precise_setting)
    per_quad = jnp.where(size_tag == 1, jnp.broadcast_to(modulation[0:1], modulation.shape), modulation)
    per_quad = per_quad.reshape(2, 1, 2, 1, 6 * D)
    shift_one = per_quad[..., 0:D]
    scale_one = per_quad[..., D:2 * D]
    gate_one = per_quad[..., 2 * D:3 * D]
    shift_two = per_quad[..., 3 * D:4 * D]
    scale_two = per_quad[..., 4 * D:5 * D]
    gate_two = per_quad[..., 5 * D:6 * D]
    labels_grid = item_ids(size_tag, SIDE)
    group_labels = item_ids(size_tag, half_side).reshape(-1)
    allowed = group_labels[:, None] == group_labels[None, :]
    grid = buffer_tokens.reshape(2, half_side, 2, half_side, D)
    hidden_one = coarse_latent(layer_norm(grid) * (1.0 + scale_one) + shift_one).reshape(TOK_DEV, D)
    qkv_cols = 3 * D // N_TP
    pieces = [jnp.dot(coarse_gradient(hidden_one), w_qkv[:, group * qkv_cols:(group + 1) * qkv_cols], precision=precise_setting) for group in range(N_TP)]
    projected = coarse_gradient(jnp.concatenate(pieces, axis=1))
    mixed_qkv = coarse_latent(depthwise(projected.reshape(SIDE, SIDE, 3 * D), conv_qkv, labels_grid))
    grouped = unshuffle(mixed_qkv.reshape(SIDE, SIDE, HEADS, 3, HEAD_SIZE))

    def one_group(block):
        return group_attention(block, allowed)
    attended = lax.map(jax.checkpoint(one_group), grouped)
    heads_out = shuffle(attended, SIDE).reshape(TOK_DEV, D)
    out_rows = D // N_TP
    attention = jnp.zeros((TOK_DEV, D), jnp.float32)
    for group in range(N_TP):
        term = jnp.dot(heads_out[:, group * out_rows:(group + 1) * out_rows], w_out[group * out_rows:(group + 1) * out_rows], precision=precise_setting)
        attention = attention + coarse_latent(coarse_gradient(term))
    after_attention = grid + gate_one * attention.reshape(grid.shape)
    hidden_two = coarse_latent(layer_norm(after_attention) * (1.0 + scale_two) + shift_two).reshape(TOK_DEV, D)
    ffn_cols = FF // N_TP
    ups = [jnp.dot(coarse_gradient(hidden_two), w_up[:, group * ffn_cols:(group + 1) * ffn_cols], precision=precise_setting) for group in range(N_TP)]
    upward = coarse_gradient(jnp.concatenate(ups, axis=1))
    activation = coarse_latent(jax.nn.gelu(depthwise(upward.reshape(SIDE, SIDE, FF), conv_ffn, labels_grid), approximate=False)).reshape(TOK_DEV, FF)
    feed = jnp.zeros((TOK_DEV, D), jnp.float32)
    for group in range(N_TP):
        term = jnp.dot(activation[:, group * ffn_cols:(group + 1) * ffn_cols], w_down[group * ffn_cols:(group + 1) * ffn_cols], precision=precise_setting)
        feed = feed + coarse_latent(coarse_gradient(term))
    result = after_attention + gate_two * feed.reshape(grid.shape)
    return result.reshape(TOK_DEV, D)

def reference(tokens, cotangent, size_tags, time_index, class_index, time_table, class_table, w_mod, w_qkv, conv_qkv, w_out, w_up, conv_ffn, w_down):
    params = tuple((weight.astype(jnp.float32) for weight in (time_table, class_table, w_mod, w_qkv, conv_qkv, w_out, w_up, conv_ffn, w_down)))
    tokens_all = tokens.astype(jnp.float32).reshape(N_DP, TOK_DEV, D)
    times_all = time_index.reshape(N_DP, SLOTS)
    labels_all = class_index.reshape(N_DP, SLOTS)

    def whole_forward(weights, inputs):

        def step(carried, sliced):
            buffer_tokens, size_tag, times, labels = sliced
            return (carried, jax.checkpoint(buffer_forward)(weights, buffer_tokens, size_tag, times, labels))
        carried_out, results = lax.scan(step, jnp.zeros((), jnp.float32), (inputs, size_tags, times_all, labels_all))
        return results
    results, pull = jax.vjp(whole_forward, params, tokens_all)
    grads, grad_inputs = pull(cotangent.astype(jnp.float32).reshape(N_DP, TOK_DEV, D))
    grad_time_t, grad_class_t, grad_mod_w, grad_qkv_w, grad_conv_q, grad_out_w, grad_up_w, grad_conv_f, grad_down_w = grads
    return (results.reshape(TOKENS, D).astype(jnp.bfloat16), grad_inputs.reshape(TOKENS, D), grad_time_t, grad_class_t, grad_mod_w, grad_qkv_w, grad_conv_q, grad_out_w, grad_up_w, grad_conv_f, grad_down_w)
```

```python
from functools import partial

import jax
import jax.numpy as jnp
import numpy as np
from jax import lax
from jax.experimental import pallas as pl
from jax.experimental.pallas import tpu as pltpu
from jax.sharding import PartitionSpec as P

D = 768
HEAD_SIZE = 64
SIDE = 64
SLOTS = 4
TOK = SIDE * SIDE
HALO = 2
QROWS = 16
QTOK = QROWS * SIDE
XTOK = (QROWS + 2 * HALO) * SIDE
F32 = jnp.float32
BF16 = jnp.bfloat16
VMEM_MAX = 66_000_000


def dot_nn(a, b):
    return lax.dot_general(a, b, (((1,), (0,)), ((), ())), preferred_element_type=F32)


def dot_nt(a, b):
    return lax.dot_general(a, b, (((1,), (1,)), ((), ())), preferred_element_type=F32)


def dot_tn(a, b):
    return lax.dot_general(a, b, (((0,), (0,)), ((), ())), preferred_element_type=F32)


def parity_matrix():
    one = np.zeros((SIDE, SIDE), np.float32)
    for parity in range(2):
        for j in range(SIDE // 2):
            one[parity * 32 + j, 2 * j + parity] = 1.0
    return jnp.asarray(np.kron(np.eye(4, dtype=np.float32), one), BF16)


def normalised(values):
    mean = jnp.mean(values, axis=-1, keepdims=True)
    centred = values - mean
    variance = jnp.mean(centred * centred, axis=-1, keepdims=True)
    rstd = lax.rsqrt(variance + 1e-06)
    return centred * rstd, rstd


def by_half(values, part):
    rows = values.shape[0]
    shaped = values.reshape(rows // 32, 2, 16, values.shape[-1])
    return (shaped * part[None, :, None, :]).reshape(values.shape)


def spread(part, rows):
    width = part.shape[-1]
    full = jnp.broadcast_to(part[None, :, None, :], (rows // 32, 2, 16, width))
    return full.reshape(rows, width)


def half_sums(values):
    return jnp.sum(values.reshape(values.shape[0] // 32, 2, 16, values.shape[-1]), axis=0)


def column_masks(tag, width):
    j = lax.broadcasted_iota(jnp.int32, (32, width), 0)
    split = tag == 0
    left = jnp.where((j == 0) | ((j == 16) & split), 0.0, 1.0)
    right = jnp.where((j == 31) | ((j == 15) & split), 0.0, 1.0)
    return left, right


def row_scales(tag, row):
    inside = (row >= 0) & (row < SIDE)
    down = jnp.where(inside & jnp.logical_not((tag == 0) & (row == 31)), 1.0, 0.0)
    up = jnp.where(inside & jnp.logical_not((tag == 0) & (row == 32)), 1.0, 0.0)
    return down, up


def conv_step(even, odd, masks, taps, down, up, carry):
    left, right = masks
    odd_left = pltpu.roll(odd, 1, 0) * left
    even_right = pltpu.roll(even, 31, 0) * right
    before_e, before_o, here_e, here_o = carry

    def terms(k):
        return (
            k[0] * odd_left + k[1] * even + k[2] * odd,
            k[0] * even + k[1] * odd + k[2] * even_right,
        )

    last = [t * up for t in taps[6:9]]
    middle = taps[3:6]
    first = [t * down for t in taps[0:3]]
    last_e, last_o = terms(last)
    mid_e, mid_o = terms(middle)
    first_e, first_o = terms(first)
    done = (before_e + last_e, before_o + last_o)
    return done, (here_e + mid_e, here_o + mid_o, first_e, first_o), (odd_left, even_right)


def no_carry(width):
    zero = jnp.zeros((32, width), F32)
    return (zero, zero, zero, zero)


def first_kernel(tag_ref, tok_ref, shift_ref, scale_ref, w_ref, taps_ref, perm_ref, hid_ref, proj_ref, mix_ref, field):
    step = pl.program_id(0)
    tag = tag_ref[0]
    width = w_ref.shape[1]

    @pl.when(step == 0)
    def _():
        field[pl.ds(0, SIDE), :] = jnp.zeros((SIDE, width), F32)
        field[pl.ds((SIDE + 1) * SIDE, SIDE), :] = jnp.zeros((SIDE, width), F32)

    @pl.when(step < 4)
    def _():
        half = step // 2
        shift = shift_ref[half]
        scale = 1.0 + scale_ref[half]

        def chunk(i, carry):
            rows = pl.ds(pl.multiple_of(i * 256, 256), 256)
            ordered = dot_nn(perm_ref[...], tok_ref[rows, :])
            unit, _ = normalised(ordered)
            hidden = (by_half(unit, scale) + spread(shift, 256)).astype(BF16)
            hid_ref[rows, :] = hidden
            out = dot_nn(hidden, w_ref[...])
            proj_ref[rows, :] = out
            field[pl.ds(pl.multiple_of((step * 16 + 1) * SIDE + i * 256, 64), 256), :] = out
            return carry

        lax.fori_loop(0, 4, chunk, 0)

    @pl.when(step > 0)
    def _():
        base = (step - 1) * 16 - 1
        for lane in range(0, width, 128):
            size = min(128, width - lane)
            lanes = slice(lane, lane + size)
            masks = column_masks(tag, size)
            taps = [taps_ref[t : t + 1, lanes] for t in range(9)]

            def one(n, carry):
                row = base + n
                start = pl.multiple_of((row + 1) * SIDE, SIDE)
                even = field[pl.ds(start, 32), lanes]
                odd = field[pl.ds(start + 32, 32), lanes]
                down, up = row_scales(tag, row)
                done, carry, _ = conv_step(even, odd, masks, taps, down, up, carry)
                return done, carry

            def loop(n, carry):
                done, carry = one(n, carry)
                start = pl.multiple_of((n - 2) * SIDE, SIDE)
                mix_ref[pl.ds(start, 32), lanes] = done[0].astype(BF16)
                mix_ref[pl.ds(start + 32, 32), lanes] = done[1].astype(BF16)
                return carry

            _, carry = one(0, no_carry(size))
            _, carry = one(1, carry)
            lax.fori_loop(2, 18, loop, carry)


def first_stage(tag, tokens, shift, scale, w_qkv, taps, perm):
    width = w_qkv.shape[1]
    whole = lambda shape: pl.BlockSpec(shape, lambda s: (0,) * len(shape))
    ahead = lambda w: pl.BlockSpec((1024, w), lambda s: (jnp.minimum(s, 3), 0))
    return pl.pallas_call(
        first_kernel,
        grid=(5,),
        in_specs=[
            pl.BlockSpec(memory_space=pltpu.SMEM),
            ahead(D),
            whole((2, 2, D)),
            whole((2, 2, D)),
            whole((D, width)),
            whole((9, width)),
            whole((256, 256)),
        ],
        out_specs=[
            ahead(D),
            ahead(width),
            pl.BlockSpec((1024, width), lambda s: (jnp.maximum(s - 1, 0), 0)),
        ],
        out_shape=[
            jax.ShapeDtypeStruct((TOK, D), BF16),
            jax.ShapeDtypeStruct((TOK, width), F32),
            jax.ShapeDtypeStruct((TOK, width), BF16),
        ],
        scratch_shapes=[pltpu.VMEM(((SIDE + 2) * SIDE, width), F32)],
        compiler_params=pltpu.CompilerParams(vmem_limit_bytes=VMEM_MAX),
        name="first_stage",
    )(tag, tokens, shift, scale, w_qkv, taps, perm)


def to_row(column, count):
    return jnp.transpose(jnp.broadcast_to(column, (count, 128)))[0:1, :]


def attend_kernel(tag_ref, x_ref, o_ref, lse_ref, *, heads):
    tag = tag_ref[0]

    def run(split):
        for head in range(heads):
            base = head * 192

            def chunk(c, carry):
                query = x_ref[pl.ds(c * 8, 8), 0, 0, :, base : base + 64].reshape(256, 64)
                query = query * jnp.asarray(0.125, BF16)
                if split:
                    rows = pl.ds((c // 2) * 16, 16)
                    count = 512
                else:
                    rows = pl.ds(0, 32)
                    count = 1024
                keys = x_ref[rows, 0, 0, :, base + 64 : base + 128].reshape(count, 64)
                values = x_ref[rows, 0, 0, :, base + 128 : base + 192].reshape(count, 64)
                scores = dot_nt(query, keys)
                if split:
                    qj = lax.broadcasted_iota(jnp.int32, (256, count), 0) & 16
                    kj = lax.broadcasted_iota(jnp.int32, (256, count), 1) & 16
                    scores = jnp.where(qj == kj, scores, -1e30)
                top = jnp.max(scores, axis=-1, keepdims=True)
                expo = jnp.exp(scores - top)
                total = jnp.sum(expo, axis=-1, keepdims=True)
                out = dot_nn(expo.astype(BF16), values) / total
                o_ref[pl.ds(c * 8, 8), 0, 0, :, head * 64 : head * 64 + 64] = out.astype(BF16).reshape(8, 32, 64)
                lse_ref[0, head : head + 1, pl.ds(pl.multiple_of(c * 256, 256), 256)] = to_row(top + jnp.log(total), 256)
                return carry

            lax.fori_loop(0, 4, chunk, 0)

    pl.when(tag == 1)(lambda: run(False))
    pl.when(tag != 1)(lambda: run(True))


def group_block(width):
    return pl.BlockSpec((32, 1, 1, 32, width), lambda g: (0, g // 2, g % 2, 0, 0))


def attend_stage(tag, mixed_qkv, heads):
    view = mixed_qkv.reshape(32, 2, 2, 32, 192 * heads)
    out, lse = pl.pallas_call(
        partial(attend_kernel, heads=heads),
        grid=(4,),
        in_specs=[pl.BlockSpec(memory_space=pltpu.SMEM), group_block(192 * heads)],
        out_specs=[group_block(64 * heads), pl.BlockSpec((1, 8, 1024), lambda g: (g, 0, 0))],
        out_shape=[
            jax.ShapeDtypeStruct((32, 2, 2, 32, 64 * heads), BF16),
            jax.ShapeDtypeStruct((4, 8, 1024), F32),
        ],
        compiler_params=pltpu.CompilerParams(vmem_limit_bytes=VMEM_MAX),
        name="attend_stage",
    )(tag, view)
    return out, lse


def attend_back_kernel(tag_ref, x_ref, o_ref, do_ref, lse_ref, g_ref, acc_ref, *, heads):
    tag = tag_ref[0]

    def run(split):
        for head in range(heads):
            base = head * 192
            acc_ref[...] = jnp.zeros_like(acc_ref)

            def chunk(c, carry):
                mine = pl.ds(c * 8, 8)
                query = x_ref[mine, 0, 0, :, base : base + 64].reshape(256, 64)
                query = query * jnp.asarray(0.125, BF16)
                grad = do_ref[mine, 0, 0, :, head * 64 : head * 64 + 64].reshape(256, 64)
                out = o_ref[mine, 0, 0, :, head * 64 : head * 64 + 64].reshape(256, 64)
                if split:
                    first = (c // 2) * 16
                    count = 512
                else:
                    first = 0
                    count = 1024
                rows = pl.ds(first, count // 32)
                keys = x_ref[rows, 0, 0, :, base + 64 : base + 128].reshape(count, 64)
                values = x_ref[rows, 0, 0, :, base + 128 : base + 192].reshape(count, 64)
                lse = lse_ref[0, head : head + 1, pl.ds(pl.multiple_of(c * 256, 256), 256)]
                delta = jnp.sum(grad.astype(F32) * out.astype(F32), axis=-1, keepdims=True)
                delta = to_row(delta, 256)
                probs = jnp.exp(dot_nt(keys, query) - lse)
                if split:
                    qj = lax.broadcasted_iota(jnp.int32, (count, 256), 1) & 16
                    kj = lax.broadcasted_iota(jnp.int32, (count, 256), 0) & 16
                    probs = jnp.where(qj == kj, probs, 0.0)
                scores = (probs * (dot_nt(values, grad) - delta)).astype(BF16)
                zero = jnp.zeros((256, 64), BF16)
                part = dot_nn(scores, jnp.concatenate([query, zero], axis=1))
                part += dot_nn(probs.astype(BF16), jnp.concatenate([zero, grad], axis=1))
                target = pl.ds(pl.multiple_of(first * 32, 256), count)
                acc_ref[target, :] += part
                grad_query = dot_tn(scores, keys) * 0.125
                g_ref[mine, 0, 0, :, base : base + 64] = grad_query.reshape(8, 32, 64)
                return carry

            lax.fori_loop(0, 4, chunk, 0)
            g_ref[:, 0, 0, :, base + 64 : base + 192] = acc_ref[...].reshape(32, 32, 128)

    pl.when(tag == 1)(lambda: run(False))
    pl.when(tag != 1)(lambda: run(True))


def attend_back_stage(tag, mixed_qkv, heads_out, grad_heads, lse, heads):
    view = mixed_qkv.reshape(32, 2, 2, 32, 192 * heads)
    grads = grad_heads.reshape(32, 2, 2, 32, 64 * heads)
    out = pl.pallas_call(
        partial(attend_back_kernel, heads=heads),
        grid=(4,),
        in_specs=[
            pl.BlockSpec(memory_space=pltpu.SMEM),
            group_block(192 * heads),
            group_block(64 * heads),
            group_block(64 * heads),
            pl.BlockSpec((1, 8, 1024), lambda g: (g, 0, 0)),
        ],
        out_specs=group_block(192 * heads),
        out_shape=jax.ShapeDtypeStruct((32, 2, 2, 32, 192 * heads), F32),
        scratch_shapes=[pltpu.VMEM((1024, 128), F32)],
        compiler_params=pltpu.CompilerParams(vmem_limit_bytes=VMEM_MAX),
        name="attend_back_stage",
    )(tag, view, heads_out, grads, lse)
    return out.reshape(TOK, 192 * heads)


def kernel_sums(acc, even, odd, odd_left, even_right, plain, scale, first):
    plain_e, plain_o = plain

    def fold(values):
        return jnp.sum(values.reshape(4, 8, values.shape[-1]), axis=0)

    terms = [
        fold(odd * plain_e) + fold(even_right * plain_o),
        fold(even * plain_e) + fold(odd * plain_o),
        fold(odd_left * plain_e) + fold(even * plain_o),
    ]
    out = list(acc)
    for t in range(3):
        term = terms[t] if scale is None else terms[t] * scale
        out[first + t] = acc[first + t] + term
    return out


POLY = (
    0.13241715506535054,
    0.12108811680396304,
    0.17555028579228482,
    -0.0796444980816301,
    0.3217932733518851,
    -0.21571441684424994,
    0.04451008654080756,
)


def gelu_parts(z):
    size = jnp.abs(z)
    t = 1.0 / (1.0 + 0.33 * size)
    expo = jnp.exp(z * z * -0.5)
    poly = POLY[6]
    for c in POLY[5::-1]:
        poly = poly * t + c
    tail = poly * t * expo
    cdf = jnp.where(z >= 0.0, 1.0 - tail, tail)
    value = z * cdf
    slope = cdf + z * (expo * 0.3989422804014327)
    return value, slope


def feed_kernel(
    info_ref,
    heads_ref,
    w_out_ref,
    tok_ref,
    cot_ref,
    mods_ref,
    w_up_ref,
    w_down_ref,
    taps_ref,
    perm_ref,
    mixed_ref,
    gheads_ref,
    gup_ref,
    gdown_ref,
    gout_ref,
    gtaps_ref,
    gafter_ref,
    sums_ref,
    after_ref,
    att_ref,
    hidden_ref,
    hidden_t,
    gfeed_ref,
    gfeed_t,
    feed_ref,
    ghid_ref,
    up_ref,
    slope_ref,
    act_ref,
    gupw_ref,
    sum_ref,
):
    step = pl.program_id(0)
    tag = info_ref[0]
    first_row = info_ref[1] * QROWS - HALO
    chans = up_ref.shape[1]
    groups = heads_ref.shape[0]

    def mod(i):
        return mods_ref[:, i * D : (i + 1) * D]

    @pl.when(step == 0)
    def _():
        gate_one, shift_two, scale_two, gate_two = mod(2), mod(3), 1.0 + mod(4), mod(5)

        def part(start, size):
            rows = pl.ds(start, size)
            perm = perm_ref[0:size, 0:size]
            ordered = dot_nn(perm, tok_ref[rows, :])
            attention = jnp.zeros((size, D), F32)
            for g in range(groups):
                term = dot_nn(heads_ref[g, rows, :], w_out_ref[g])
                attention = attention + term.astype(BF16).astype(F32)
            att_ref[rows, :] = attention
            after = ordered + by_half(attention, gate_one)
            after_ref[rows, :] = after
            unit, _ = normalised(after)
            hidden_ref[rows, :] = (by_half(unit, scale_two) + spread(shift_two, size)).astype(BF16)
            gfeed_ref[rows, :] = by_half(dot_nn(perm, cot_ref[rows, :]), gate_two).astype(BF16)

        part(0, 128)
        part(XTOK - 128, 128)

        def loop(i, carry):
            part(pl.multiple_of(128 + i * 256, 128), 256)
            return carry

        lax.fori_loop(0, 4, loop, 0)
        hidden_t[...] = jnp.transpose(hidden_ref[pl.ds(128, QTOK), :])
        gfeed_t[...] = jnp.transpose(gfeed_ref[pl.ds(128, QTOK), :])
        feed_ref[...] = jnp.zeros_like(feed_ref)
        ghid_ref[...] = jnp.zeros_like(ghid_ref)

    w_up = w_up_ref[...].reshape(D, chans)
    w_down = w_down_ref[...].reshape(chans, D)

    def up_loop(i, carry):
        rows = pl.ds(pl.multiple_of(i * 640, 128), 640)
        up_ref[rows, :] = dot_nn(hidden_ref[rows, :], w_up)
        return carry

    lax.fori_loop(0, 2, up_loop, 0)

    for lane in range(0, chans, 128):
        lanes = slice(lane, lane + 128)
        masks = column_masks(tag, 128)
        taps = [taps_ref[0, t : t + 1, lanes] for t in range(9)]

        def one(n, carry):
            start = pl.multiple_of(n * SIDE, SIDE)
            even = up_ref[pl.ds(start, 32), lanes]
            odd = up_ref[pl.ds(start + 32, 32), lanes]
            down, up = row_scales(tag, first_row + n)
            done, carry, _ = conv_step(even, odd, masks, taps, down, up, carry)
            return done, carry

        def loop(n, carry):
            done, carry = one(n, carry)
            for k in range(2):
                start = pl.multiple_of((n - 2) * SIDE + 32 * k, 32)
                value, slope = gelu_parts(done[k])
                act_ref[pl.ds(start, 32), lanes] = value.astype(BF16)
                slope_ref[pl.ds(start, 32), lanes] = slope
            return carry

        _, carry = one(0, no_carry(128))
        _, carry = one(1, carry)
        lax.fori_loop(2, QROWS + 2 * HALO, loop, carry)

    def gact_loop(i, carry):
        rows = pl.ds(pl.multiple_of(i * 576, 64), 576)
        out = dot_nt(gfeed_ref[pl.ds(pl.multiple_of(64 + i * 576, 64), 576), :], w_down)
        slope_ref[rows, :] = out * slope_ref[rows, :]
        return carry

    lax.fori_loop(0, 2, gact_loop, 0)

    for lane in range(0, chans, 128):
        lanes = slice(lane, lane + 128)
        masks = column_masks(tag, 128)
        taps = [taps_ref[0, 8 - t : 9 - t, lanes] for t in range(9)]

        def one(n, carry, sums):
            start = pl.multiple_of(n * SIDE, SIDE)
            low, high = pl.ds(start, 32), pl.ds(start + 32, 32)
            even, odd = slope_ref[low, lanes], slope_ref[high, lanes]
            row = first_row + 1 + n
            down, up = row_scales(tag, row)
            done, carry, shifted = conv_step(even, odd, masks, taps, down, up, carry)
            if sums is not None:
                above = jnp.where((row == 0) | ((tag == 0) & (row == 32)), 0.0, 1.0)
                below = jnp.where((row == SIDE - 1) | ((tag == 0) & (row == 31)), 0.0, 1.0)
                for i, scale in ((0, above), (1, None), (2, below)):
                    at = pl.multiple_of((n + i) * SIDE, SIDE)
                    plain = (up_ref[pl.ds(at, 32), lanes], up_ref[pl.ds(at + 32, 32), lanes])
                    sums = kernel_sums(sums, even, odd, *shifted, plain, scale, 3 * i)
            return done, carry, sums

        def put(n, done):
            for k in range(2):
                start = pl.multiple_of((n - 2) * SIDE + 32 * k, 32)
                gupw_ref[pl.ds(start, 32), lanes] = done[k].astype(BF16)

        def loop(n, state):
            done, carry, sums = one(n, state[0], list(state[1]))
            put(n, done)
            return carry, tuple(sums)

        zero = jnp.zeros((8, 128), F32)
        _, carry, _ = one(0, no_carry(128), None)
        _, carry, sums = one(1, carry, [zero] * 9)
        carry, sums = lax.fori_loop(2, QROWS + 1, loop, (carry, tuple(sums)))
        done, carry, _ = one(QROWS + 1, carry, None)
        put(QROWS + 1, done)
        for t in range(9):
            gtaps_ref[0, t : t + 1, lanes] = jnp.sum(sums[t], axis=0, keepdims=True)

    def token_loop(i, carry):
        rows = pl.ds(pl.multiple_of(i * 512, 512), 512)
        feed_ref[rows, :] += dot_nn(act_ref[pl.ds(pl.multiple_of(64 + i * 512, 64), 512), :], w_down)
        ghid_ref[rows, :] += dot_nt(gupw_ref[rows, :], w_up)
        return carry

    lax.fori_loop(0, 2, token_loop, 0)
    dps, per = gup_ref.shape[0], gup_ref.shape[2]

    def weight_loop(i, carry):
        rows = pl.ds(pl.multiple_of(i * 384, 128), 384)
        blocks = pl.ds(i * (dps // 2), dps // 2)
        out = dot_nn(hidden_t[rows, :], gupw_ref[...])
        gup_ref[blocks, 0, :, :] = out.reshape(dps // 2, per, chans).astype(gup_ref.dtype)
        out = dot_nn(gfeed_t[rows, :], act_ref[pl.ds(64, QTOK), :])
        gdown_ref[blocks, 0, :, :] = out.reshape(dps // 2, per, chans).astype(gdown_ref.dtype)
        return carry

    lax.fori_loop(0, 2, weight_loop, 0)

    @pl.when(step == pl.num_programs(0) - 1)
    def _():
        gate_one, scale_two, gate_two = mod(2), 1.0 + mod(4), mod(5)
        sum_ref[...] = jnp.zeros_like(sum_ref)

        def loop(i, carry):
            rows = pl.ds(pl.multiple_of(i * 256, 256), 256)
            wide = pl.ds(pl.multiple_of(128 + i * 256, 128), 256)
            after = after_ref[wide, :]
            feed = feed_ref[rows, :]
            result = (after + by_half(feed, gate_two)).astype(BF16)
            mixed_ref[rows, :] = dot_tn(perm_ref[...], result).astype(BF16)
            cot = dot_nn(perm_ref[...], cot_ref[wide, :])
            sum_ref[3] += half_sums(cot * feed)
            unit, rstd = normalised(after)
            grad = ghid_ref[rows, :]
            sum_ref[1] += half_sums(grad)
            sum_ref[2] += half_sums(grad * unit)
            inner = by_half(grad, scale_two)
            mean = jnp.mean(inner, axis=-1, keepdims=True)
            along = jnp.mean(inner * unit, axis=-1, keepdims=True)
            gafter = cot + rstd * (inner - mean - unit * along)
            sum_ref[0] += half_sums(gafter * att_ref[wide, :])
            gafter_ref[rows, :] = gafter
            gatt = by_half(gafter, gate_one).astype(BF16)
            gupw_ref[rows, :] = gatt
            for g in range(groups):
                gheads_ref[g, rows, :] = dot_nt(gatt, w_out_ref[g]).astype(BF16)
            return carry

        lax.fori_loop(0, 4, loop, 0)
        for g in range(groups):
            out = dot_tn(gupw_ref[...], heads_ref[g, pl.ds(128, QTOK), :])
            gout_ref[:, g, :, :] = out.reshape(dps, per, out.shape[-1]).astype(gout_ref.dtype)
        sums_ref[...] = jnp.sum(sum_ref[...], axis=2)


def feed_stage(info, heads, w_out, tok, cot, mods, w_up, w_down, taps, perm, wire):
    groups, _, hwidth = heads.shape
    dps, chunks, per, chans = w_up.shape
    once = pl.Buffered(1)
    whole = lambda shape: pl.BlockSpec(shape, lambda s: (0,) * len(shape), pipeline_mode=once)
    weights = pl.BlockSpec((dps, 1, per, chans), lambda s: (0, s, 0, 0))
    return pl.pallas_call(
        feed_kernel,
        grid=(chunks,),
        in_specs=[
            pl.BlockSpec(memory_space=pltpu.SMEM),
            whole(heads.shape),
            whole(w_out.shape),
            whole((XTOK, D)),
            whole((XTOK, D)),
            whole((2, 6 * D)),
            weights,
            weights,
            pl.BlockSpec((1, 9, chans), lambda s: (s, 0, 0)),
            whole((256, 256)),
        ],
        out_specs=[
            whole((QTOK, D)),
            whole((groups, QTOK, hwidth)),
            weights,
            weights,
            whole((dps, groups, per, hwidth)),
            pl.BlockSpec((1, 9, chans), lambda s: (s, 0, 0)),
            whole((QTOK, D)),
            whole((4, 2, D)),
        ],
        out_shape=[
            jax.ShapeDtypeStruct((QTOK, D), BF16),
            jax.ShapeDtypeStruct((groups, QTOK, hwidth), BF16),
            jax.ShapeDtypeStruct((dps, chunks, per, chans), wire),
            jax.ShapeDtypeStruct((dps, chunks, per, chans), wire),
            jax.ShapeDtypeStruct((dps, groups, per, hwidth), wire),
            jax.ShapeDtypeStruct((chunks, 9, chans), F32),
            jax.ShapeDtypeStruct((QTOK, D), F32),
            jax.ShapeDtypeStruct((4, 2, D), F32),
        ],
        scratch_shapes=[
            pltpu.VMEM((XTOK, D), F32),
            pltpu.VMEM((XTOK, D), F32),
            pltpu.VMEM((XTOK, D), BF16),
            pltpu.VMEM((D, QTOK), BF16),
            pltpu.VMEM((XTOK, D), BF16),
            pltpu.VMEM((D, QTOK), BF16),
            pltpu.VMEM((QTOK, D), F32),
            pltpu.VMEM((QTOK, D), F32),
            pltpu.VMEM((XTOK, chans), F32),
            pltpu.VMEM((XTOK - 128, chans), F32),
            pltpu.VMEM((XTOK - 128, chans), BF16),
            pltpu.VMEM((QTOK, chans), BF16),
            pltpu.VMEM((4, 2, 16, D), F32),
        ],
        compiler_params=pltpu.CompilerParams(vmem_limit_bytes=VMEM_MAX),
        name="feed_stage",
    )(info, heads, w_out, tok, cot, mods, w_up, w_down, taps, perm)


def conv_back_kernel(tag_ref, grad_ref, proj_ref, taps_ref, out_ref, gtaps_ref):
    tag = tag_ref[0]
    width = grad_ref.shape[1]
    for lane in range(0, width, 128):
        size = min(128, width - lane)
        lanes = slice(lane, lane + size)
        masks = column_masks(tag, size)
        taps = [taps_ref[8 - t : 9 - t, lanes] for t in range(9)]

        def one(row, carry, sums, has_above, has_below):
            start = pl.multiple_of(row * SIDE, SIDE)
            even = grad_ref[pl.ds(start, 32), lanes]
            odd = grad_ref[pl.ds(start + 32, 32), lanes]
            down, up = row_scales(tag, row)
            done, carry, shifted = conv_step(even, odd, masks, taps, down, up, carry)
            for i in range(3):
                if (i == 0 and not has_above) or (i == 2 and not has_below):
                    continue
                at = pl.multiple_of((row + i - 1) * SIDE, SIDE)
                plain = (proj_ref[pl.ds(at, 32), lanes], proj_ref[pl.ds(at + 32, 32), lanes])
                scale = (up, None, down)[i]
                sums = kernel_sums(sums, even, odd, *shifted, plain, scale, 3 * i)
            return done, carry, sums

        def put(row, done):
            for k in range(2):
                start = pl.multiple_of(row * SIDE + 32 * k, 32)
                out_ref[pl.ds(start, 32), lanes] = done[k].astype(BF16)

        def loop(row, state):
            done, carry, sums = one(row, state[0], list(state[1]), True, True)
            put(row - 1, done)
            return carry, tuple(sums)

        zero = jnp.zeros((8, size), F32)
        _, carry, sums = one(0, no_carry(size), [zero] * 9, False, True)
        carry, sums = lax.fori_loop(1, SIDE - 1, loop, (carry, tuple(sums)))
        done, carry, sums = one(SIDE - 1, carry, list(sums), True, False)
        put(SIDE - 2, done)
        put(SIDE - 1, carry[0:2])
        for t in range(9):
            gtaps_ref[t : t + 1, lanes] = jnp.sum(sums[t], axis=0, keepdims=True)


def conv_back_stage(tag, grad, proj, taps):
    width = grad.shape[1]
    space = pl.BlockSpec(memory_space=pltpu.VMEM)
    return pl.pallas_call(
        conv_back_kernel,
        in_specs=[pl.BlockSpec(memory_space=pltpu.SMEM), space, space, space],
        out_specs=[space, space],
        out_shape=[jax.ShapeDtypeStruct((TOK, width), BF16), jax.ShapeDtypeStruct((9, width), F32)],
        compiler_params=pltpu.CompilerParams(vmem_limit_bytes=VMEM_MAX),
        name="conv_back_stage",
    )(tag, grad, proj, taps)


def last_kernel(ghid_ref, tok_ref, gafter_ref, mods_ref, perm_ref, out_ref, sums_ref, sum_ref, turn_ref):
    scale = 1.0 + mods_ref[:, D : 2 * D]
    sum_ref[...] = jnp.zeros_like(sum_ref)

    def loop(i, carry):
        rows = pl.ds(pl.multiple_of(i * 256, 256), 256)
        ordered = dot_nn(perm_ref[...], tok_ref[rows, :])
        unit, rstd = normalised(ordered)
        grad = ghid_ref[rows, :].astype(F32)
        sum_ref[0] += half_sums(grad)
        sum_ref[1] += half_sums(grad * unit)
        inner = by_half(grad, scale)
        mean = jnp.mean(inner, axis=-1, keepdims=True)
        along = jnp.mean(inner * unit, axis=-1, keepdims=True)
        out = gafter_ref[rows, :] + rstd * (inner - mean - unit * along)
        for lane in range(D // 128):
            for r in range(4):
                for parity in range(2):
                    at = r * 64 + parity * 32
                    turn_ref[lane, pl.ds(r * 64 + parity, 32, stride=2), :] = out[
                        at : at + 32, lane * 128 : lane * 128 + 128
                    ]
            out_ref[rows, lane * 128 : lane * 128 + 128] = turn_ref[lane]
        return carry

    lax.fori_loop(0, QTOK // 256, loop, 0)
    sums_ref[...] = jnp.sum(sum_ref[...], axis=2)


def last_stage(ghid, tok, gafter, mods, perm):
    space = pl.BlockSpec(memory_space=pltpu.VMEM)
    return pl.pallas_call(
        last_kernel,
        in_specs=[space] * 5,
        out_specs=[space] * 2,
        out_shape=[jax.ShapeDtypeStruct((QTOK, D), F32), jax.ShapeDtypeStruct((2, 2, D), F32)],
        scratch_shapes=[pltpu.VMEM((2, 2, 16, D), F32), pltpu.VMEM((D // 128, 256, 128), F32)],
        compiler_params=pltpu.CompilerParams(vmem_limit_bytes=VMEM_MAX),
        name="last_stage",
    )(ghid, tok, gafter, mods, perm)


def per_device(
    tokens,
    cotangent,
    size_tags,
    time_index,
    class_index,
    time_table,
    class_table,
    w_mod,
    w_qkv,
    conv_qkv,
    w_out,
    w_up,
    conv_ffn,
    w_down,
):
    tp_count = lax.axis_size("tp")
    dp_count = lax.axis_size("dp")
    tp_rank = lax.axis_index("tp")
    dp_rank = lax.axis_index("dp")
    tag = size_tags[0]
    heads = w_out.shape[0] // HEAD_SIZE
    perm = parity_matrix()
    share = D // dp_count
    fold = 8

    def gather_weights(weight):
        mine = lax.dynamic_slice_in_dim(weight, dp_rank * share, share, 0)
        stacked = lax.all_gather(mine, "tp", axis=0)
        stacked = lax.all_gather(stacked, "dp", axis=0)
        if dp_count == fold:
            return stacked
        inner = stacked.reshape(fold, dp_count // fold, tp_count, share, D)
        return inner.transpose(0, 2, 1, 3, 4).reshape(fold, tp_count, D // fold, D)

    w_up_all = gather_weights(w_up)
    w_down_all = gather_weights(w_down)
    w_out_all = lax.all_gather(w_out, "tp", axis=0)
    conv_ffn_all = lax.all_gather(conv_ffn, "tp", axis=0).astype(F32)

    time_rows = jnp.take(time_table, time_index, axis=0).astype(F32)
    class_rows = jnp.take(class_table, class_index, axis=0).astype(F32)
    condition_all = time_rows + class_rows
    activated_all = jax.nn.silu(condition_all).astype(BF16)
    activated = lax.dynamic_slice_in_dim(activated_all, dp_rank * SLOTS, SLOTS, 0)
    mod_part = jnp.dot(activated, w_mod, preferred_element_type=F32)
    modulation = lax.all_gather(mod_part, "tp", axis=1, tiled=True)
    per_quad = jnp.where(tag == 1, jnp.broadcast_to(modulation[0:1], modulation.shape), modulation)
    quads = per_quad.reshape(2, 2, 6 * D)
    quad_row = tp_rank * QROWS // (SIDE // 2)
    mods = lax.dynamic_index_in_dim(quads, quad_row, 0, keepdims=False)

    tag_word = size_tags.astype(jnp.int32)
    taps_qkv = conv_qkv.astype(F32)
    hidden_one, projected, mixed_qkv = first_stage(
        tag_word, tokens, quads[..., 0:D], quads[..., D : 2 * D], w_qkv, taps_qkv, perm
    )
    heads_out, lse = attend_stage(tag_word, mixed_qkv, heads)

    pad = ((HALO * SIDE, HALO * SIDE), (0, 0))
    flat_heads = jnp.pad(heads_out.reshape(TOK, heads * HEAD_SIZE), pad)
    sends = jnp.stack([flat_heads[k * QTOK : k * QTOK + XTOK] for k in range(tp_count)])
    heads_in = lax.all_to_all(sends, "tp", split_axis=0, concat_axis=0, tiled=True)
    tok_wide = lax.dynamic_slice_in_dim(jnp.pad(tokens, pad), tp_rank * QTOK, XTOK, 0)
    cot_wide = lax.dynamic_slice_in_dim(jnp.pad(cotangent, pad), tp_rank * QTOK, XTOK, 0)
    info = jnp.stack([tag, tp_rank]).astype(jnp.int32)
    wire = BF16
    mixed_q, gheads, g_up, g_down, g_out, g_taps_ffn, g_after, sums_two = feed_stage(
        info, heads_in, w_out_all, tok_wide, cot_wide, mods, w_up_all, w_down_all, conv_ffn_all, perm, wire
    )
    grad_heads = lax.all_to_all(gheads, "tp", split_axis=0, concat_axis=0, tiled=True)
    grad_heads = grad_heads.reshape(TOK, heads * HEAD_SIZE)
    mixed = lax.all_gather(mixed_q, "tp", axis=0, tiled=True)

    grad_mixed = attend_back_stage(tag_word, mixed_qkv, heads_out, grad_heads, lse, heads)
    grad_proj, g_taps_qkv = conv_back_stage(tag_word, grad_mixed, projected, taps_qkv)
    ghid_part = jnp.dot(grad_proj, w_qkv.T, preferred_element_type=F32).astype(BF16)
    ghid_one = lax.psum_scatter(ghid_part, "tp", scatter_dimension=0, tiled=True)
    grad_qkv_w = jnp.einsum("td,tc->dc", hidden_one, grad_proj, preferred_element_type=F32)
    summed_qkv = lax.psum_scatter(grad_qkv_w, "dp", scatter_dimension=0, tiled=True)

    tok_mine = lax.dynamic_slice_in_dim(tokens, tp_rank * QTOK, QTOK, 0)
    grad_tokens, sums_one = last_stage(ghid_one, tok_mine, g_after, mods, perm)

    def reduce_rows(grads):
        if dp_count != fold:
            inner = grads.reshape(fold, tp_count, dp_count // fold, share, grads.shape[-1])
            grads = inner.transpose(0, 2, 1, 3, 4).reshape(dp_count, tp_count, share, grads.shape[-1])
        mine = lax.psum_scatter(grads, "dp", scatter_dimension=0, tiled=True)[0]
        return lax.psum_scatter(mine, "tp", scatter_dimension=0, tiled=True)[0].astype(F32)

    summed_up = reduce_rows(g_up)
    summed_down = reduce_rows(g_down).T
    summed_out = reduce_rows(g_out).T
    mine_taps = lax.psum_scatter(g_taps_ffn, "tp", scatter_dimension=0, tiled=True)[0]
    summed_conv_ffn = lax.psum_scatter(mine_taps, "dp", scatter_dimension=1, tiled=True)
    summed_conv_qkv = lax.psum_scatter(g_taps_qkv, "dp", scatter_dimension=1, tiled=True)

    quad_rows = jnp.concatenate(
        [sums_one[0], sums_one[1], sums_two[0], sums_two[1], sums_two[2], sums_two[3]], axis=-1
    )
    row_pick = (lax.iota(jnp.int32, 2) == quad_row)[:, None, None]
    grad_quads = jnp.where(row_pick, quad_rows[None], 0.0).reshape(4, 6 * D)
    merged = jnp.concatenate(
        [jnp.sum(grad_quads, axis=0, keepdims=True), jnp.zeros((SLOTS - 1, 6 * D), F32)], axis=0
    )
    grad_slots = jnp.where(tag == 1, merged, grad_quads)
    slot_cols = lax.psum_scatter(grad_slots, "tp", scatter_dimension=1, tiled=True)
    mod_cols = lax.all_gather(slot_cols, "dp", axis=0, tiled=True)
    my_act = lax.dynamic_slice_in_dim(activated_all, dp_rank * share, share, 1).astype(F32)
    my_cond = lax.dynamic_slice_in_dim(condition_all, dp_rank * share, share, 1)
    my_w_mod = lax.dynamic_slice_in_dim(w_mod, dp_rank * share, share, 0).astype(F32)
    summed_mod = jnp.dot(my_act.T, mod_cols, precision=lax.Precision.HIGHEST)
    part_act = jnp.dot(mod_cols, my_w_mod.T, precision=lax.Precision.HIGHEST)
    grad_act = lax.psum(part_act, "tp")
    _, silu_pull = jax.vjp(jax.nn.silu, my_cond)
    grad_cols = silu_pull(grad_act)[0]
    time_iota = lax.broadcasted_iota(jnp.int32, (time_index.shape[0], time_table.shape[0]), 1)
    time_hits = (time_index[:, None] == time_iota).astype(F32)
    grad_time = jnp.dot(time_hits.T, grad_cols, precision=lax.Precision.HIGHEST)
    class_iota = lax.broadcasted_iota(jnp.int32, (class_index.shape[0], class_table.shape[0]), 1)
    class_hits = (class_index[:, None] == class_iota).astype(F32)
    grad_class = jnp.dot(class_hits.T, grad_cols, precision=lax.Precision.HIGHEST)
    return (
        mixed,
        grad_tokens,
        grad_time,
        grad_class,
        summed_mod,
        summed_qkv,
        summed_conv_qkv,
        summed_out,
        summed_up,
        summed_conv_ffn,
        summed_down,
    )


def solution(mesh):
    in_specs = (
        P("dp", None),
        P("dp", None),
        P("dp"),
        P(),
        P(),
        P(),
        P(),
        P(None, "tp"),
        P(None, "tp"),
        P(None, "tp"),
        P("tp", None),
        P(None, "tp"),
        P(None, "tp"),
        P("tp", None),
    )
    out_specs = (
        P("dp", None),
        P(("dp", "tp"), None),
        P(None, "dp"),
        P(None, "dp"),
        P("dp", "tp"),
        P("dp", "tp"),
        P(None, ("tp", "dp")),
        P("tp", "dp"),
        P("dp", "tp"),
        P(None, ("tp", "dp")),
        P("tp", "dp"),
    )
    return jax.shard_map(
        per_device, mesh=mesh, in_specs=in_specs, out_specs=out_specs, check_vma=False
    )
```

```python
from functools import partial

import jax
import jax.numpy as jnp
import numpy as np
from jax import lax
from jax.experimental import pallas as pl
from jax.experimental.pallas import tpu as pltpu
from jax.sharding import PartitionSpec as P

D = 768
HEAD_SIZE = 64
SIDE = 64
SLOTS = 4
TOK = SIDE * SIDE
HALO = 2
QROWS = 16
QTOK = QROWS * SIDE
XTOK = (QROWS + 2 * HALO) * SIDE
F32 = jnp.float32
BF16 = jnp.bfloat16
VMEM_MAX = 66_000_000


def dot_nn(a, b):
    return lax.dot_general(a, b, (((1,), (0,)), ((), ())), preferred_element_type=F32)


def dot_nt(a, b):
    return lax.dot_general(a, b, (((1,), (1,)), ((), ())), preferred_element_type=F32)


def dot_tn(a, b):
    return lax.dot_general(a, b, (((0,), (0,)), ((), ())), preferred_element_type=F32)


def parity_matrix():
    one = np.zeros((SIDE, SIDE), np.float32)
    for parity in range(2):
        for j in range(SIDE // 2):
            one[parity * 32 + j, 2 * j + parity] = 1.0
    return jnp.asarray(np.kron(np.eye(4, dtype=np.float32), one), BF16)


def normalised(values):
    mean = jnp.mean(values, axis=-1, keepdims=True)
    centred = values - mean
    variance = jnp.mean(centred * centred, axis=-1, keepdims=True)
    rstd = lax.rsqrt(variance + 1e-06)
    return centred * rstd, rstd


def by_half(values, part):
    rows = values.shape[0]
    shaped = values.reshape(rows // 32, 2, 16, values.shape[-1])
    return (shaped * part[None, :, None, :]).reshape(values.shape)


def spread(part, rows):
    width = part.shape[-1]
    full = jnp.broadcast_to(part[None, :, None, :], (rows // 32, 2, 16, width))
    return full.reshape(rows, width)


def half_sums(values):
    return jnp.sum(values.reshape(values.shape[0] // 32, 2, 16, values.shape[-1]), axis=0)


def column_masks(tag, width):
    j = lax.broadcasted_iota(jnp.int32, (32, width), 0)
    split = tag == 0
    left = jnp.where((j == 0) | ((j == 16) & split), 0.0, 1.0)
    right = jnp.where((j == 31) | ((j == 15) & split), 0.0, 1.0)
    return left, right


def row_scales(tag, row):
    inside = (row >= 0) & (row < SIDE)
    down = jnp.where(inside & jnp.logical_not((tag == 0) & (row == 31)), 1.0, 0.0)
    up = jnp.where(inside & jnp.logical_not((tag == 0) & (row == 32)), 1.0, 0.0)
    return down, up


def conv_step(even, odd, masks, taps, down, up, carry):
    left, right = masks
    odd_left = pltpu.roll(odd, 1, 0) * left
    even_right = pltpu.roll(even, 31, 0) * right
    before_e, before_o, here_e, here_o = carry

    def terms(k):
        return (
            k[0] * odd_left + k[1] * even + k[2] * odd,
            k[0] * even + k[1] * odd + k[2] * even_right,
        )

    last = [t * up for t in taps[6:9]]
    middle = taps[3:6]
    first = [t * down for t in taps[0:3]]
    last_e, last_o = terms(last)
    mid_e, mid_o = terms(middle)
    first_e, first_o = terms(first)
    done = (before_e + last_e, before_o + last_o)
    return done, (here_e + mid_e, here_o + mid_o, first_e, first_o), (odd_left, even_right)


def no_carry(width):
    zero = jnp.zeros((32, width), F32)
    return (zero, zero, zero, zero)


def first_kernel(tag_ref, tok_ref, shift_ref, scale_ref, w_ref, taps_ref, perm_ref, hid_ref, proj_ref, mix_ref, field):
    step = pl.program_id(0)
    tag = tag_ref[0]
    width = w_ref.shape[1]

    @pl.when(step == 0)
    def _():
        field[pl.ds(0, SIDE), :] = jnp.zeros((SIDE, width), F32)
        field[pl.ds((SIDE + 1) * SIDE, SIDE), :] = jnp.zeros((SIDE, width), F32)

    @pl.when(step < 4)
    def _():
        half = step // 2
        shift = shift_ref[half]
        scale = 1.0 + scale_ref[half]

        def chunk(i, carry):
            rows = pl.ds(pl.multiple_of(i * 256, 256), 256)
            ordered = dot_nn(perm_ref[...], tok_ref[rows, :])
            unit, _ = normalised(ordered)
            hidden = (by_half(unit, scale) + spread(shift, 256)).astype(BF16)
            hid_ref[rows, :] = hidden
            out = dot_nn(hidden, w_ref[...])
            for head in range(proj_ref.shape[0]):
                proj_ref[head, rows, :] = out[:, head * 192 : head * 192 + 192]
            field[pl.ds(pl.multiple_of((step * 16 + 1) * SIDE + i * 256, 64), 256), :] = out
            return carry

        lax.fori_loop(0, 4, chunk, 0)

    @pl.when(step > 0)
    def _():
        base = (step - 1) * 16 - 1
        for lane in range(0, width, 128):
            size = min(128, width - lane)
            lanes = slice(lane, lane + size)
            masks = column_masks(tag, size)
            taps = [taps_ref[t : t + 1, lanes] for t in range(9)]

            def one(n, carry):
                row = base + n
                start = pl.multiple_of((row + 1) * SIDE, SIDE)
                even = field[pl.ds(start, 32), lanes]
                odd = field[pl.ds(start + 32, 32), lanes]
                down, up = row_scales(tag, row)
                done, carry, _ = conv_step(even, odd, masks, taps, down, up, carry)
                return done, carry

            def loop(n, carry):
                done, carry = one(n, carry)
                start = pl.multiple_of((n - 2) * SIDE, SIDE)
                for k in range(2):
                    out = done[k].astype(BF16)
                    mix_ref[pl.ds(start + 32 * k, 32), lanes] = out
                return carry

            _, carry = one(0, no_carry(size))
            _, carry = one(1, carry)
            lax.fori_loop(2, 18, loop, carry)


def first_stage(tag, tokens, shift, scale, w_qkv, taps, perm):
    width = w_qkv.shape[1]
    heads = width // 192
    whole = lambda shape: pl.BlockSpec(shape, lambda s: (0,) * len(shape))
    ahead = lambda w: pl.BlockSpec((1024, w), lambda s: (jnp.minimum(s, 3), 0))
    return pl.pallas_call(
        first_kernel,
        grid=(5,),
        in_specs=[
            pl.BlockSpec(memory_space=pltpu.SMEM),
            ahead(D),
            whole((2, 2, D)),
            whole((2, 2, D)),
            whole((D, width)),
            whole((9, width)),
            whole((256, 256)),
        ],
        out_specs=[
            ahead(D),
            pl.BlockSpec((heads, 1024, 192), lambda s: (0, jnp.minimum(s, 3), 0)),
            pl.BlockSpec((1024, width), lambda s: (jnp.maximum(s - 1, 0), 0)),
        ],
        out_shape=[
            jax.ShapeDtypeStruct((TOK, D), BF16),
            jax.ShapeDtypeStruct((heads, TOK, 192), F32),
            jax.ShapeDtypeStruct((TOK, width), BF16),
        ],
        scratch_shapes=[pltpu.VMEM(((SIDE + 2) * SIDE, width), F32)],
        compiler_params=pltpu.CompilerParams(vmem_limit_bytes=VMEM_MAX),
        name="first_stage",
    )(tag, tokens, shift, scale, w_qkv, taps, perm)


def to_row(column, count):
    return jnp.transpose(jnp.broadcast_to(column, (count, 128)))[0:1, :]


def attend_kernel(tag_ref, x_ref, o_ref, lse_ref, *, base):
    tag = tag_ref[0]
    parity = pl.program_id(0) % 2

    def run(split):
        def chunk(c, carry):
            query = x_ref[pl.ds(c * 8, 8), 0, 0, :, base : base + 64].reshape(256, 64)
            query = query * jnp.asarray(0.125, BF16)
            if split:
                rows = pl.ds((c // 2) * 16, 16)
                count = 512
            else:
                rows = pl.ds(0, 32)
                count = 1024
            keys = x_ref[rows, 0, 0, :, base + 64 : base + 128].reshape(count, 64)
            values = x_ref[rows, 0, 0, :, base + 128 : base + 192].reshape(count, 64)
            scores = dot_nt(query, keys)
            if split:
                qj = lax.broadcasted_iota(jnp.int32, (256, count), 0) & 16
                kj = lax.broadcasted_iota(jnp.int32, (256, count), 1) & 16
                scores = jnp.where(qj == kj, scores, -1e30)
            top = jnp.max(scores, axis=-1, keepdims=True)
            expo = jnp.exp(scores - top)
            total = jnp.sum(expo, axis=-1, keepdims=True)
            out = dot_nn(expo.astype(BF16), values) / total
            out = out.astype(BF16).reshape(8, 32, 64)
            for b in range(2):

                @pl.when(parity == b)
                def _():
                    o_ref[pl.ds(c * 8, 8), 0, :, b * 64 : b * 64 + 64] = out

            lse_ref[0, 0:1, pl.ds(pl.multiple_of(c * 256, 256), 256)] = to_row(top + jnp.log(total), 256)
            return carry

        lax.fori_loop(0, 4, chunk, 0)

    pl.when(tag == 1)(lambda: run(False))
    pl.when(tag != 1)(lambda: run(True))


def group_block(width):
    at = lambda g: jnp.minimum(g, 3)
    return pl.BlockSpec((32, 1, 1, 32, width), lambda g: (0, at(g) // 2, at(g) % 2, 0, 0))


def pair_block():
    return pl.BlockSpec((32, 1, 32, 128), lambda g: (0, jnp.minimum(g, 3) // 2, 0, 0))


def lse_block():
    return pl.BlockSpec((1, 8, 1024), lambda g: (jnp.minimum(g, 3), 0, 0))


def attend_stage(tag, mixed_qkv, head):
    out, lse = pl.pallas_call(
        partial(attend_kernel, base=head * 192),
        grid=(4,),
        in_specs=[pl.BlockSpec(memory_space=pltpu.SMEM), group_block(mixed_qkv.shape[-1])],
        out_specs=[pair_block(), lse_block()],
        out_shape=[
            jax.ShapeDtypeStruct((32, 2, 32, 128), BF16),
            jax.ShapeDtypeStruct((4, 8, 1024), F32),
        ],
        compiler_params=pltpu.CompilerParams(vmem_limit_bytes=VMEM_MAX),
        cost_estimate=pl.CostEstimate(flops=2_000_000_000, transcendentals=4_000_000, bytes_accessed=4_000_000),
        name="attend_stage",
    )(tag, mixed_qkv)
    return out, lse


def kernel_sums(acc, even, odd, odd_left, even_right, plain, scale, first):
    plain_e, plain_o = plain

    def fold(values):
        return jnp.sum(values.reshape(4, 8, values.shape[-1]), axis=0)

    terms = [
        fold(odd * plain_e) + fold(even_right * plain_o),
        fold(even * plain_e) + fold(odd * plain_o),
        fold(odd_left * plain_e) + fold(even * plain_o),
    ]
    out = list(acc)
    for t in range(3):
        term = terms[t] if scale is None else terms[t] * scale
        out[first + t] = acc[first + t] + term
    return out


POLY = (
    0.13241715506535054,
    0.12108811680396304,
    0.17555028579228482,
    -0.0796444980816301,
    0.3217932733518851,
    -0.21571441684424994,
    0.04451008654080756,
)


def gelu_parts(z):
    size = jnp.abs(z)
    t = 1.0 / (1.0 + 0.33 * size)
    expo = jnp.exp(z * z * -0.5)
    poly = POLY[6]
    for c in POLY[5::-1]:
        poly = poly * t + c
    tail = poly * t * expo
    cdf = jnp.where(z >= 0.0, 1.0 - tail, tail)
    value = z * cdf
    slope = cdf + z * (expo * 0.3989422804014327)
    return value, slope


def mod_part(mods_ref, i):
    return mods_ref[:, i * D : (i + 1) * D]


def feed_kernel(
    info_ref,
    *refs,
):
    heads_refs, refs = refs[0:12], refs[12:]
    feed_body(info_ref, heads_refs, *refs)


def feed_body(
    info_ref,
    heads_refs,
    w_out_ref,
    tok_ref,
    cot_ref,
    mods_ref,
    w_up_ref,
    w_down_ref,
    taps_ref,
    perm_ref,
    mixed_ref,
    up_ref,
    slope_ref,
    act_ref,
    after_ref,
    att_ref,
    hidden_out,
    heads_out,
    sums_ref,
    hidden_ref,
    hcat_ref,
    feed_ref,
    sum_ref,
):
    step = pl.program_id(0)
    tag = info_ref[0]
    first_row = info_ref[1] * QROWS - HALO
    chans = up_ref.shape[2]
    groups = w_out_ref.shape[0]
    heads = len(heads_refs) // groups
    rank = info_ref[1]

    @pl.when(step == 0)
    def _():
        gate_one, shift_two, scale_two = mod_part(mods_ref, 2), mod_part(mods_ref, 3), 1.0 + mod_part(mods_ref, 4)

        def unpack(i, carry):
            for g in range(groups):
                for head in range(heads):
                    ref = heads_refs[head * groups + g]
                    for b in range(2):
                        rows = pl.ds(pl.multiple_of(i * SIDE + b * 32, 32), 32)
                        lane = (g * heads + head) * 64
                        hcat_ref[rows, lane : lane + 64] = ref[i, :, b * 64 : b * 64 + 64]
            return carry

        lax.fori_loop(0, XTOK // SIDE, unpack, 0)

        def part(start, size):
            rows = pl.ds(start, size)
            perm = perm_ref[0:size, 0:size]
            ordered = dot_nn(perm, tok_ref[rows, :])
            attention = jnp.zeros((size, D), F32)
            width = heads * HEAD_SIZE
            for g in range(groups):
                source = lax.rem(rank - g + groups, groups)
                term = dot_nn(hcat_ref[rows, g * width : g * width + width], w_out_ref[source])
                attention = attention + term.astype(BF16).astype(F32)
            after = ordered + by_half(attention, gate_one)
            unit, _ = normalised(after)
            hidden = (by_half(unit, scale_two) + spread(shift_two, size)).astype(BF16)
            hidden_ref[rows, :] = hidden
            if size == 256:
                mine = pl.ds(pl.multiple_of(start - 128, 256), 256)
                att_ref[mine, :] = attention.astype(BF16)
                after_ref[mine, :] = after
                hidden_out[mine, :] = hidden
                heads_out[mine, :] = hcat_ref[rows, :]

        part(0, 128)
        part(XTOK - 128, 128)

        def loop(i, carry):
            part(pl.multiple_of(128 + i * 256, 128), 256)
            return carry

        lax.fori_loop(0, 4, loop, 0)
        feed_ref[...] = jnp.zeros_like(feed_ref)

    w_up = w_up_ref[...].reshape(D, chans)
    w_down = w_down_ref[...].reshape(chans, D)

    def up_loop(i, carry):
        rows = pl.ds(pl.multiple_of(i * 640, 128), 640)
        up_ref[0, rows, :] = dot_nn(hidden_ref[rows, :], w_up)
        return carry

    lax.fori_loop(0, 2, up_loop, 0)

    for lane in range(0, chans, 128):
        lanes = slice(lane, lane + 128)
        masks = column_masks(tag, 128)
        taps = [taps_ref[0, t : t + 1, lanes] for t in range(9)]

        def one(n, carry):
            start = pl.multiple_of(n * SIDE, SIDE)
            even = up_ref[0, pl.ds(start, 32), lanes]
            odd = up_ref[0, pl.ds(start + 32, 32), lanes]
            down, up = row_scales(tag, first_row + n)
            done, carry, _ = conv_step(even, odd, masks, taps, down, up, carry)
            return done, carry

        def loop(n, carry):
            done, carry = one(n, carry)
            for k in range(2):
                start = pl.multiple_of((n - 2) * SIDE + 32 * k, 32)
                value, slope = gelu_parts(done[k])
                act_ref[0, pl.ds(start, 32), lanes] = value.astype(BF16)
                slope_ref[0, pl.ds(start, 32), lanes] = slope
            return carry

        _, carry = one(0, no_carry(128))
        _, carry = one(1, carry)
        lax.fori_loop(2, QROWS + 2 * HALO, loop, carry)

    def token_loop(i, carry):
        rows = pl.ds(pl.multiple_of(i * 512, 512), 512)
        feed_ref[rows, :] += dot_nn(act_ref[0, pl.ds(pl.multiple_of(64 + i * 512, 64), 512), :], w_down)
        return carry

    lax.fori_loop(0, 2, token_loop, 0)

    @pl.when(step == pl.num_programs(0) - 1)
    def _():
        gate_two = mod_part(mods_ref, 5)
        sum_ref[...] = jnp.zeros_like(sum_ref)

        def loop(i, carry):
            rows = pl.ds(pl.multiple_of(i * 256, 256), 256)
            wide = pl.ds(pl.multiple_of(128 + i * 256, 128), 256)
            feed = feed_ref[rows, :]
            result = (after_ref[rows, :] + by_half(feed, gate_two)).astype(BF16)
            mixed_ref[rows, :] = dot_tn(perm_ref[...], result).astype(BF16)
            sum_ref[...] += half_sums(dot_nn(perm_ref[...], cot_ref[wide, :]) * feed)
            return carry

        lax.fori_loop(0, 4, loop, 0)
        sums_ref[...] = jnp.sum(sum_ref[...], axis=1)


def feed_stage(info, heads, w_out, tok, cot, mods, w_rows, taps, perm):
    dps, chunks, tall, chans = w_rows.shape
    per = D // dps
    once = pl.Buffered(1)
    whole = lambda shape: pl.BlockSpec(shape, lambda s: (0,) * len(shape), pipeline_mode=once)
    chunk = lambda rows: pl.BlockSpec((1, rows, chans), lambda s: (s, 0, 0))
    return pl.pallas_call(
        feed_kernel,
        grid=(chunks,),
        in_specs=[
            pl.BlockSpec(memory_space=pltpu.SMEM),
            *[whole(h.shape) for h in heads],
            whole(w_out.shape),
            whole((XTOK, D)),
            whole((XTOK, D)),
            whole((2, 6 * D)),
            pl.BlockSpec((dps, 1, per, chans), lambda s: (0, s, 0, 0)),
            pl.BlockSpec((dps, 1, per, chans), lambda s: (0, s, 1, 0)),
            chunk(9),
            whole((256, 256)),
        ],
        out_specs=[
            whole((QTOK, D)),
            chunk(XTOK),
            chunk(XTOK - 128),
            chunk(XTOK - 128),
            whole((QTOK, D)),
            whole((QTOK, D)),
            whole((QTOK, D)),
            whole((QTOK, D)),
            whole((2, D)),
        ],
        out_shape=[
            jax.ShapeDtypeStruct((QTOK, D), BF16),
            jax.ShapeDtypeStruct((chunks, XTOK, chans), F32),
            jax.ShapeDtypeStruct((chunks, XTOK - 128, chans), F32),
            jax.ShapeDtypeStruct((chunks, XTOK - 128, chans), BF16),
            jax.ShapeDtypeStruct((QTOK, D), F32),
            jax.ShapeDtypeStruct((QTOK, D), BF16),
            jax.ShapeDtypeStruct((QTOK, D), BF16),
            jax.ShapeDtypeStruct((QTOK, D), BF16),
            jax.ShapeDtypeStruct((2, D), F32),
        ],
        scratch_shapes=[
            pltpu.VMEM((XTOK, D), BF16),
            pltpu.VMEM((XTOK, D), BF16),
            pltpu.VMEM((QTOK, D), F32),
            pltpu.VMEM((2, 16, D), F32),
        ],
        compiler_params=pltpu.CompilerParams(vmem_limit_bytes=VMEM_MAX),
        cost_estimate=pl.CostEstimate(flops=20_000_000_000, transcendentals=8_000_000, bytes_accessed=80_000_000),
        name="feed_stage",
    )(info, *heads, w_out, tok, cot, mods, w_rows, w_rows, taps, perm)


def feed_back_kernel(
    info_ref,
    up_ref,
    slope_ref,
    act_ref,
    w_up_ref,
    w_down_ref,
    taps_ref,
    cot_ref,
    hidden_ref,
    after_ref,
    att_ref,
    heads_ref,
    w_out_ref,
    mods_ref,
    perm_ref,
    gcat_ref,
    g0_ref,
    g1_ref,
    g2_ref,
    gafter_ref,
    sums_ref,
    hidden_t,
    gfeed_ref,
    gfeed_t,
    ghid_ref,
    gact_ref,
    gup_ref,
    sum_ref,
    gtaps_ref,
):
    step = pl.program_id(0)
    tag = info_ref[0]
    first_row = info_ref[1] * QROWS - HALO
    chans = up_ref.shape[2]
    dps, per = w_up_ref.shape[0], w_up_ref.shape[2]

    @pl.when(step == 0)
    def _():
        gate_two = mod_part(mods_ref, 5)

        def part(start, size):
            rows = pl.ds(start, size)
            perm = perm_ref[0:size, 0:size]
            gfeed_ref[rows, :] = by_half(dot_nn(perm, cot_ref[rows, :]), gate_two).astype(BF16)

        def loop(i, carry):
            part(pl.multiple_of(i * 256, 256), 256)
            return carry

        lax.fori_loop(0, XTOK // 256, loop, 0)
        hidden_t[...] = jnp.transpose(hidden_ref[...])
        gfeed_t[...] = jnp.transpose(gfeed_ref[pl.ds(128, QTOK), :])
        ghid_ref[...] = jnp.zeros_like(ghid_ref)

    @pl.when(step < pl.num_programs(0) - 1)
    def _():
        w_up = w_up_ref[...].reshape(D, chans)
        w_down = w_down_ref[...].reshape(chans, D)

        def gact_loop(i, carry):
            rows = pl.ds(pl.multiple_of(i * 576, 64), 576)
            out = dot_nt(gfeed_ref[pl.ds(pl.multiple_of(64 + i * 576, 64), 576), :], w_down)
            gact_ref[rows, :] = out * slope_ref[0, rows, :]
            return carry

        lax.fori_loop(0, 2, gact_loop, 0)

        for lane in range(0, chans, 128):
            lanes = slice(lane, lane + 128)
            masks = column_masks(tag, 128)
            taps = [taps_ref[0, 8 - t : 9 - t, lanes] for t in range(9)]

            def one(n, carry, sums):
                start = pl.multiple_of(n * SIDE, SIDE)
                low, high = pl.ds(start, 32), pl.ds(start + 32, 32)
                even, odd = gact_ref[low, lanes], gact_ref[high, lanes]
                row = first_row + 1 + n
                down, up = row_scales(tag, row)
                done, carry, shifted = conv_step(even, odd, masks, taps, down, up, carry)
                if sums is not None:
                    above = jnp.where((row == 0) | ((tag == 0) & (row == 32)), 0.0, 1.0)
                    below = jnp.where((row == SIDE - 1) | ((tag == 0) & (row == 31)), 0.0, 1.0)
                    for i, scale in ((0, above), (1, None), (2, below)):
                        at = pl.multiple_of((n + i) * SIDE, SIDE)
                        plain = (up_ref[0, pl.ds(at, 32), lanes], up_ref[0, pl.ds(at + 32, 32), lanes])
                        sums = kernel_sums(sums, even, odd, *shifted, plain, scale, 3 * i)
                return done, carry, sums

            def put(n, done):
                for k in range(2):
                    start = pl.multiple_of((n - 2) * SIDE + 32 * k, 32)
                    gup_ref[pl.ds(start, 32), lanes] = done[k].astype(BF16)

            def loop(n, state):
                done, carry, sums = one(n, state[0], list(state[1]))
                put(n, done)
                return carry, tuple(sums)

            zero = jnp.zeros((8, 128), F32)
            _, carry, _ = one(0, no_carry(128), None)
            _, carry, sums = one(1, carry, [zero] * 9)
            carry, sums = lax.fori_loop(2, QROWS + 1, loop, (carry, tuple(sums)))
            done, carry, _ = one(QROWS + 1, carry, None)
            put(QROWS + 1, done)
            for t in range(9):
                gtaps_ref[t : t + 1, lanes] = jnp.sum(sums[t], axis=0, keepdims=True)

        def token_loop(i, carry):
            rows = pl.ds(pl.multiple_of(i * 512, 512), 512)
            ghid_ref[rows, :] += dot_nt(gup_ref[rows, :], w_up)
            return carry

        lax.fori_loop(0, 2, token_loop, 0)

        def weight_loop(i, carry):
            rows = pl.ds(pl.multiple_of(i * 384, 128), 384)
            blocks = pl.ds(i * (dps // 2), dps // 2)
            out = dot_nn(hidden_t[rows, :], gup_ref[...])
            gcat_ref[blocks, 0, 0:per, :] = out.reshape(dps // 2, per, chans).astype(BF16)
            out = dot_nn(gfeed_t[rows, :], act_ref[0, pl.ds(64, QTOK), :])
            gcat_ref[blocks, 0, per : 2 * per, :] = out.reshape(dps // 2, per, chans).astype(BF16)
            return carry

        lax.fori_loop(0, 2, weight_loop, 0)
        sums = jnp.concatenate([gtaps_ref[0:9, :], jnp.zeros((7, chans), F32)], axis=0)
        for d in range(dps):
            part_sums = jnp.concatenate([sums[:, d * per : d * per + per], jnp.zeros((16, chans - per), F32)], axis=1)
            gcat_ref[d, 0, 2 * per : 2 * per + 16, :] = part_sums.astype(BF16)

    @pl.when(step == pl.num_programs(0) - 1)
    def _():
        gate_one, scale_two = mod_part(mods_ref, 2), 1.0 + mod_part(mods_ref, 4)
        groups = w_out_ref.shape[0]
        sum_ref[...] = jnp.zeros_like(sum_ref)

        def loop(i, carry):
            rows = pl.ds(pl.multiple_of(i * 256, 256), 256)
            wide = pl.ds(pl.multiple_of(128 + i * 256, 128), 256)
            cot = dot_nn(perm_ref[...], cot_ref[wide, :])
            unit, rstd = normalised(after_ref[rows, :])
            grad = ghid_ref[rows, :]
            sum_ref[1] += half_sums(grad)
            sum_ref[2] += half_sums(grad * unit)
            inner = by_half(grad, scale_two)
            mean = jnp.mean(inner, axis=-1, keepdims=True)
            along = jnp.mean(inner * unit, axis=-1, keepdims=True)
            gafter = cot + rstd * (inner - mean - unit * along)
            sum_ref[0] += half_sums(gafter * att_ref[rows, :].astype(F32))
            gafter_ref[rows, :] = gafter
            gatt = by_half(gafter, gate_one).astype(BF16)
            gup_ref[rows, :] = gatt
            for g in range(groups):
                target = lax.rem(info_ref[1] + g, groups)
                out = dot_nt(gatt, w_out_ref[target]).astype(BF16).reshape(4, 2, 32, w_out_ref.shape[1])
                for head, ref in enumerate((g0_ref, g1_ref, g2_ref)):
                    for b in range(2):
                        ref[g, pl.ds(i * 4, 4), :, b * 64 : b * 64 + 64] = out[:, b, :, head * 64 : head * 64 + 64]
            return carry

        lax.fori_loop(0, 4, loop, 0)
        out = dot_tn(gup_ref[...], heads_ref[...])
        gcat_ref[:, 0, 0:per, :] = out.reshape(dps, per, D).astype(BF16)
        gcat_ref[:, 0, per:, :] = jnp.zeros((dps, per + 16, D), BF16)
        sums_ref[...] = jnp.sum(sum_ref[...], axis=2)


def feed_back_stage(info, up, slope, act, w_rows, taps, cot, hidden, after, att, heads, w_out, mods, perm):
    dps, chunks, tall, chans = w_rows.shape
    groups = w_out.shape[0]
    per = D // dps
    once = pl.Buffered(1)
    whole = lambda shape: pl.BlockSpec(shape, lambda s: (0,) * len(shape), pipeline_mode=once)
    at = lambda s: jnp.minimum(s, chunks - 1)
    chunk = lambda rows: pl.BlockSpec((1, rows, chans), lambda s: (at(s), 0, 0))
    sent = (groups, QROWS, 32, 128)
    return pl.pallas_call(
        feed_back_kernel,
        grid=(chunks + 1,),
        in_specs=[
            pl.BlockSpec(memory_space=pltpu.SMEM),
            chunk(XTOK),
            chunk(XTOK - 128),
            chunk(XTOK - 128),
            pl.BlockSpec((dps, 1, per, chans), lambda s: (0, at(s), 0, 0)),
            pl.BlockSpec((dps, 1, per, chans), lambda s: (0, at(s), 1, 0)),
            chunk(9),
            whole((XTOK, D)),
            whole((QTOK, D)),
            whole((QTOK, D)),
            whole((QTOK, D)),
            whole((QTOK, D)),
            whole(w_out.shape),
            whole((2, 6 * D)),
            whole((256, 256)),
        ],
        out_specs=[
            pl.BlockSpec((dps, 1, 2 * per + 16, chans), lambda s: (0, s, 0, 0)),
            whole(sent),
            whole(sent),
            whole(sent),
            whole((QTOK, D)),
            whole((3, 2, D)),
        ],
        out_shape=[
            jax.ShapeDtypeStruct((dps, chunks + 1, 2 * per + 16, chans), BF16),
            jax.ShapeDtypeStruct(sent, BF16),
            jax.ShapeDtypeStruct(sent, BF16),
            jax.ShapeDtypeStruct(sent, BF16),
            jax.ShapeDtypeStruct((QTOK, D), F32),
            jax.ShapeDtypeStruct((3, 2, D), F32),
        ],
        scratch_shapes=[
            pltpu.VMEM((D, QTOK), BF16),
            pltpu.VMEM((XTOK, D), BF16),
            pltpu.VMEM((D, QTOK), BF16),
            pltpu.VMEM((QTOK, D), F32),
            pltpu.VMEM((XTOK - 128, chans), F32),
            pltpu.VMEM((QTOK, chans), BF16),
            pltpu.VMEM((3, 2, 16, D), F32),
            pltpu.VMEM((16, chans), F32),
        ],
        compiler_params=pltpu.CompilerParams(vmem_limit_bytes=VMEM_MAX),
        cost_estimate=pl.CostEstimate(flops=30_000_000_000, transcendentals=8_000_000, bytes_accessed=80_000_000),
        name="feed_back_stage",
    )(info, up, slope, act, w_rows, w_rows, taps, cot, hidden, after, att, heads, w_out, mods, perm)


def head_back_kernel(
    info_ref, x_ref, o_ref, do0_ref, do1_ref, do2_ref, do3_ref, lse_ref, proj_ref, taps_ref, hid_ref, g_ref, gw_ref, gtaps_ref, acc_ref, field, flat, *, base
):
    tag = info_ref[0]
    rank = info_ref[1]
    step = pl.program_id(0)
    parity = step % 2
    odd_row = jnp.minimum(step, 3) // 2

    def run(split):
        acc_ref[...] = jnp.zeros_like(acc_ref)

        def chunk(c, carry):
            mine = pl.ds(c * 8, 8)

            def pick(ref, rows):
                both = [ref[rows, 0, :, 64 * b : 64 * b + 64] for b in range(2)]
                return jnp.where(parity == 0, both[0], both[1]).reshape(256, 64)

            query = x_ref[mine, 0, 0, :, base : base + 64].reshape(256, 64)
            query = query * jnp.asarray(0.125, BF16)
            slot = lax.rem(rank - c + 4, 4)
            grad = pick(do0_ref, pl.ds(0, 8))
            for i, ref in enumerate((do1_ref, do2_ref, do3_ref)):
                grad = jnp.where(slot == i + 1, pick(ref, pl.ds(0, 8)), grad)
            out = pick(o_ref, mine)
            if split:
                first = (c // 2) * 16
                count = 512
            else:
                first = 0
                count = 1024
            rows = pl.ds(first, count // 32)
            keys = x_ref[rows, 0, 0, :, base + 64 : base + 128].reshape(count, 64)
            values = x_ref[rows, 0, 0, :, base + 128 : base + 192].reshape(count, 64)
            lse = lse_ref[0, 0:1, pl.ds(pl.multiple_of(c * 256, 256), 256)]
            delta = jnp.sum(grad.astype(F32) * out.astype(F32), axis=-1, keepdims=True)
            delta = to_row(delta, 256)
            probs = jnp.exp(dot_nt(keys, query) - lse)
            if split:
                qj = lax.broadcasted_iota(jnp.int32, (count, 256), 1) & 16
                kj = lax.broadcasted_iota(jnp.int32, (count, 256), 0) & 16
                probs = jnp.where(qj == kj, probs, 0.0)
            scores = (probs * (dot_nt(values, grad) - delta)).astype(BF16)
            zero = jnp.zeros((256, 64), BF16)
            part = dot_nn(scores, jnp.concatenate([query, zero], axis=1))
            part += dot_nn(probs.astype(BF16), jnp.concatenate([zero, grad], axis=1))
            target = pl.ds(pl.multiple_of(first * 32, 256), count)
            acc_ref[target, :] += part
            grad_query = dot_tn(scores, keys) * 0.125
            field[mine, odd_row, parity, :, 0:64] = grad_query.reshape(8, 32, 64)
            return carry

        lax.fori_loop(0, 4, chunk, 0)
        field[:, odd_row, parity, :, 64:192] = acc_ref[...].reshape(32, 32, 128)

    pl.when((step < 4) & (tag == 1))(lambda: run(False))
    pl.when((step < 4) & (tag != 1))(lambda: run(True))

    @pl.when(step == 4)
    def _():
        for start_lane, size in ((0, 128), (128, 64)):
            lanes = slice(start_lane, start_lane + size)
            masks = column_masks(tag, size)
            taps = [taps_ref[8 - t : 9 - t, base + start_lane : base + start_lane + size] for t in range(9)]

            def one(row, carry, sums, has_above, has_below):
                even = field[row // 2, row % 2, 0, :, lanes]
                odd = field[row // 2, row % 2, 1, :, lanes]
                down, up = row_scales(tag, row)
                done, carry, shifted = conv_step(even, odd, masks, taps, down, up, carry)
                for i in range(3):
                    if (i == 0 and not has_above) or (i == 2 and not has_below):
                        continue
                    at = pl.multiple_of((row + i - 1) * SIDE, SIDE)
                    plain = (proj_ref[0, pl.ds(at, 32), lanes], proj_ref[0, pl.ds(at + 32, 32), lanes])
                    scale = (up, None, down)[i]
                    sums = kernel_sums(sums, even, odd, *shifted, plain, scale, 3 * i)
                return done, carry, sums

            def put(row, done):
                for k in range(2):
                    out = done[k].astype(BF16)
                    at = k * 192 + start_lane
                    quarter = row // QROWS if isinstance(row, int) else lax.div(row, QROWS)
                    slot = lax.rem(quarter - rank + 4, 4)
                    g_ref[slot, row - quarter * QROWS, :, at : at + size] = out
                    flat[pl.ds(pl.multiple_of(row * SIDE + 32 * k, 32), 32), lanes] = out

            def loop(row, state):
                done, carry, sums = one(row, state[0], list(state[1]), True, True)
                put(row - 1, done)
                return carry, tuple(sums)

            zero = jnp.zeros((8, size), F32)
            _, carry, sums = one(0, no_carry(size), [zero] * 9, False, True)
            carry, sums = lax.fori_loop(1, SIDE - 1, loop, (carry, tuple(sums)))
            done, carry, sums = one(SIDE - 1, carry, list(sums), True, False)
            put(SIDE - 2, done)
            put(SIDE - 1, carry[0:2])
            for t in range(9):
                gtaps_ref[t : t + 1, lanes] = jnp.sum(sums[t], axis=0, keepdims=True)
        gw_ref[...] = jnp.zeros_like(gw_ref)

    @pl.when(step >= 4)
    def _():
        rows = pl.ds(pl.multiple_of((step - 4) * 1024, 1024), 1024)
        gw_ref[...] += dot_tn(flat[rows, :], hid_ref[...])


def head_back_stage(tag, mixed_qkv, heads_out, grad_heads, lse, proj, taps, hidden, head):
    whole = lambda shape, at: pl.BlockSpec(shape, lambda s: at)
    return pl.pallas_call(
        partial(head_back_kernel, base=head * 192),
        grid=(8,),
        in_specs=[
            pl.BlockSpec(memory_space=pltpu.SMEM),
            group_block(mixed_qkv.shape[-1]),
            pair_block(),
            *[pl.BlockSpec((8, 1, 32, 128), lambda g: (0, jnp.minimum(g, 3) // 2, 0, 0))] * 4,
            lse_block(),
            whole((1, TOK, 192), (head, 0, 0)),
            whole(taps.shape, (0, 0)),
            pl.BlockSpec((1024, D), lambda s: (jnp.maximum(s - 4, 0), 0)),
        ],
        out_specs=[
            whole((4, QROWS, 32, 384), (0, 0, 0, 0)),
            whole((192, D), (0, 0)),
            whole((9, 192), (0, 0)),
        ],
        out_shape=[
            jax.ShapeDtypeStruct((4, QROWS, 32, 384), BF16),
            jax.ShapeDtypeStruct((192, D), F32),
            jax.ShapeDtypeStruct((9, 192), F32),
        ],
        scratch_shapes=[
            pltpu.VMEM((1024, 128), F32),
            pltpu.VMEM((32, 2, 2, 32, 192), F32),
            pltpu.VMEM((TOK, 192), BF16),
        ],
        compiler_params=pltpu.CompilerParams(vmem_limit_bytes=VMEM_MAX),
        cost_estimate=pl.CostEstimate(flops=8_000_000_000, transcendentals=4_000_000, bytes_accessed=20_000_000),
        name=f"head_back_{head}",
    )(tag, mixed_qkv, heads_out, *grad_heads, lse, proj, taps, hidden)


def last_kernel(info_ref, *refs):
    last_body(info_ref, refs[0:12], *refs[12:])


def last_body(info_ref, grad_refs, w_ref, tok_ref, gafter_ref, mods_ref, perm_ref, out_ref, sums_ref, sum_ref, turn_ref, ghid_ref):
    scale = 1.0 + mods_ref[:, D : 2 * D]
    sum_ref[...] = jnp.zeros_like(sum_ref)
    for b in range(2):
        total = jnp.zeros((QROWS * 32, D), F32)
        groups = w_ref.shape[1]
        for slot in range(groups):
            source = lax.rem(info_ref[1] - slot + groups, groups)
            weight = w_ref[:, source].reshape(D, w_ref.shape[-1])
            for head in range(len(grad_refs) // groups):
                ref = grad_refs[head * groups + slot]
                part = ref[:, :, b * 192 : b * 192 + 192].reshape(QROWS * 32, 192)
                total += dot_nt(part, weight[:, head * 192 : head * 192 + 192])
        ghid_ref[:, b] = total.reshape(QROWS, 32, D)

    def loop(i, carry):
        rows = pl.ds(pl.multiple_of(i * 256, 256), 256)
        ordered = dot_nn(perm_ref[...], tok_ref[rows, :])
        unit, rstd = normalised(ordered)
        grad = ghid_ref[pl.ds(i * 4, 4)].reshape(256, D)
        sum_ref[0] += half_sums(grad)
        sum_ref[1] += half_sums(grad * unit)
        inner = by_half(grad, scale)
        mean = jnp.mean(inner, axis=-1, keepdims=True)
        along = jnp.mean(inner * unit, axis=-1, keepdims=True)
        out = gafter_ref[rows, :] + rstd * (inner - mean - unit * along)
        for lane in range(D // 128):
            for r in range(4):
                for parity in range(2):
                    at = r * 64 + parity * 32
                    turn_ref[lane, pl.ds(r * 64 + parity, 32, stride=2), :] = out[
                        at : at + 32, lane * 128 : lane * 128 + 128
                    ]
            out_ref[rows, lane * 128 : lane * 128 + 128] = turn_ref[lane]
        return carry

    lax.fori_loop(0, QTOK // 256, loop, 0)
    sums_ref[...] = jnp.sum(sum_ref[...], axis=2)


def last_stage(info, grads, w_qkv, tok, gafter, mods, perm):
    space = pl.BlockSpec(memory_space=pltpu.VMEM)
    return pl.pallas_call(
        last_kernel,
        in_specs=[pl.BlockSpec(memory_space=pltpu.SMEM)] + [space] * (len(grads) + 5),
        out_specs=[space] * 2,
        out_shape=[jax.ShapeDtypeStruct((QTOK, D), F32), jax.ShapeDtypeStruct((2, 2, D), F32)],
        scratch_shapes=[pltpu.VMEM((2, 2, 16, D), F32), pltpu.VMEM((D // 128, 256, 128), F32), pltpu.VMEM((QROWS, 2, 32, D), F32)],
        compiler_params=pltpu.CompilerParams(vmem_limit_bytes=VMEM_MAX),
        name="last_stage",
    )(info, *grads, w_qkv, tok, gafter, mods, perm)


def per_device(
    tokens,
    cotangent,
    size_tags,
    time_index,
    class_index,
    time_table,
    class_table,
    w_mod,
    w_qkv,
    conv_qkv,
    w_out,
    w_up,
    conv_ffn,
    w_down,
):
    tp_count = lax.axis_size("tp")
    dp_count = lax.axis_size("dp")
    tp_rank = lax.axis_index("tp")
    dp_rank = lax.axis_index("dp")
    tag = size_tags[0]
    heads = w_out.shape[0] // HEAD_SIZE
    perm = parity_matrix()
    share = D // dp_count
    fold = 8

    def slice_rows(weight):
        size = weight.shape[0] // dp_count
        return lax.dynamic_slice_in_dim(weight, dp_rank * size, size, 0)

    def eight(stacked):
        if dp_count == fold:
            return stacked
        rows, width = stacked.shape[2:]
        inner = stacked.reshape(fold, dp_count // fold, tp_count, rows, width)
        return inner.transpose(0, 2, 1, 3, 4).reshape(fold, tp_count, rows * dp_count // fold, width)

    def gather_all(rows):
        stacked = lax.all_gather(rows, ("dp", "tp"), axis=0)
        return stacked.reshape((dp_count, tp_count) + rows.shape)

    packed = jnp.concatenate([slice_rows(w_up), slice_rows(w_down), slice_rows(w_out)], axis=0)
    packed = gather_all(packed)
    w_rows = jnp.concatenate([eight(packed[:, :, 0:share]), eight(packed[:, :, share : 2 * share])], axis=2)
    if dp_count == fold:
        w_rows = packed
    else:
        w_rows = jnp.concatenate([w_rows, jnp.zeros((fold, tp_count, 24, D), BF16)], axis=2)
    w_out_all = packed[:, :, 2 * share :].transpose(1, 0, 2, 3).reshape(tp_count, D // tp_count, D)
    w_qkv_all = eight(gather_all(slice_rows(w_qkv)))
    turn = [[(i, (i + s) % tp_count) for i in range(tp_count)] for s in range(tp_count)]
    w_mod_mine = slice_rows(w_mod)
    w_mod_slots = [w_mod_mine] + [lax.ppermute(w_mod_mine, "tp", turn[s]) for s in range(1, tp_count)]

    time_rows = jnp.take(time_table, time_index, axis=0).astype(F32)
    class_rows = jnp.take(class_table, class_index, axis=0).astype(F32)
    condition_all = time_rows + class_rows
    activated_all = jax.nn.silu(condition_all).astype(BF16)
    activated = lax.dynamic_slice_in_dim(activated_all, dp_rank * SLOTS, SLOTS, 0)
    mod_part = jnp.dot(activated, w_mod, preferred_element_type=F32)
    small = jnp.concatenate([mod_part.reshape(-1), conv_ffn.astype(F32).reshape(-1)])
    small = lax.all_gather(small.reshape(-1, 128), "tp", axis=0).reshape(tp_count, -1)
    modulation = small[:, : mod_part.size].reshape(tp_count, SLOTS, -1).transpose(1, 0, 2).reshape(SLOTS, 6 * D)
    conv_ffn_all = small[:, mod_part.size :].reshape(tp_count, 9, -1)
    per_quad = jnp.where(tag == 1, jnp.broadcast_to(modulation[0:1], modulation.shape), modulation)
    quads = per_quad.reshape(2, 2, 6 * D)
    quad_row = tp_rank * QROWS // (SIDE // 2)
    mods = lax.dynamic_index_in_dim(quads, quad_row, 0, keepdims=False)

    tag_word = size_tags.astype(jnp.int32)
    taps_qkv = conv_qkv.astype(F32)
    hidden_one, projected, mixed_qkv = first_stage(
        tag_word, tokens, quads[..., 0:D], quads[..., D : 2 * D], w_qkv, taps_qkv, perm
    )
    mixed_qkv = mixed_qkv.reshape(32, 2, 2, 32, 192 * heads)

    def exchange(slots):
        return [slots[0]] + [lax.ppermute(slots[s], "tp", turn[s]) for s in range(1, tp_count)]

    heads_out, lse, heads_in = [], [], []
    for head in range(heads):
        out, sums = attend_stage(tag_word, mixed_qkv, head)
        heads_out.append(out)
        lse.append(sums)
        wide = jnp.pad(out.reshape(SIDE, 32, 128), ((HALO, HALO), (0, 0), (0, 0)))
        places = [lax.rem(tp_rank + s, tp_count) * QROWS for s in range(tp_count)]
        heads_in += exchange([lax.dynamic_slice_in_dim(wide, p, XTOK // SIDE, 0) for p in places])
    pad = ((HALO * SIDE, HALO * SIDE), (0, 0))
    tok_wide = lax.dynamic_slice_in_dim(jnp.pad(tokens, pad), tp_rank * QTOK, XTOK, 0)
    cot_wide = lax.dynamic_slice_in_dim(jnp.pad(cotangent, pad), tp_rank * QTOK, XTOK, 0)
    info = jnp.stack([tag, tp_rank]).astype(jnp.int32)
    mixed_q, up, slope, act, after, att, hidden_two, heads_rows, sums_gate = feed_stage(
        info, heads_in, w_out_all, tok_wide, cot_wide, mods, w_rows, conv_ffn_all, perm
    )
    mixed = lax.all_gather(mixed_q, "tp", axis=0, tiled=True)
    g_cat, *gheads, g_after, sums_two = feed_back_stage(
        info, up, slope, act, w_rows, conv_ffn_all, cot_wide, hidden_two, after, att, heads_rows, w_out_all, mods, perm
    )
    grads, grad_w, grad_taps = [], [], []
    for head in range(heads):
        grad_heads = [g.reshape(8, 2, 32, 128) for g in exchange(gheads[head])]
        g_proj, g_w, g_taps = head_back_stage(
            info, mixed_qkv, heads_out[head], grad_heads, lse[head], projected, taps_qkv, hidden_one, head
        )
        grads += exchange(g_proj)
        grad_w.append(g_w)
        grad_taps.append(g_taps)
    tok_mine = lax.dynamic_slice_in_dim(tokens, tp_rank * QTOK, QTOK, 0)
    grad_tokens, sums_one = last_stage(info, grads, w_qkv_all, tok_mine, g_after, mods, perm)

    def regroup(values):
        rows, width = values.shape[-2:]
        if dp_count == fold:
            return values
        inner = values.reshape(fold, -1, dp_count // fold, rows * fold // dp_count, width)
        return inner.transpose(0, 2, 1, 3, 4).reshape(dp_count, -1, rows * fold // dp_count, width)

    def scatter(values, axis, dim=0):
        return lax.psum_scatter(values, axis, scatter_dimension=dim, tiled=True)

    def out_rows(values):
        return values.reshape(values.shape[0], tp_count, -1)[:, np.array([0, 3, 2, 1])].transpose(1, 2, 0)

    def sum_slots(slots):
        return sum(part.astype(F32) for part in exchange(slots))

    width = w_qkv.shape[1]
    w_cols = jnp.concatenate(grad_w, axis=0).T.reshape(dp_count, share, width)
    taps_rows = jnp.concatenate(grad_taps, axis=1).reshape(9, dp_count, width // dp_count).transpose(1, 0, 2)
    if dp_count == fold:
        mine = scatter(g_cat, "dp")[0]
        rows_out = out_rows(mine[tp_count, 0:share]).reshape(tp_count, -1, D)
        slots = []
        for s in range(tp_count):
            part = lax.dynamic_index_in_dim(mine, lax.rem(tp_rank + s, tp_count), 0, keepdims=False)
            slots.append(jnp.concatenate([part, rows_out[s]], axis=0))
        mine = sum_slots(slots)
        summed_up, summed_down = mine[0:share], mine[share : 2 * share].T
        summed_conv_ffn = mine[2 * share : 2 * share + 9, 0:share]
        summed_out = mine[2 * share + 16 :].reshape(-1, share)
        taps_rows = jnp.pad(taps_rows, ((0, 0), (0, 7), (0, width - taps_rows.shape[2])))
        both = jnp.concatenate([w_cols, taps_rows], axis=1)
        mine = jnp.sum(lax.all_to_all(both, "dp", split_axis=0, concat_axis=0, tiled=True), axis=0)
        summed_qkv, summed_conv_qkv = mine[0:share], mine[share : share + 9, 0 : width // dp_count]
    else:
        per = D // fold
        body = g_cat[:, 0:tp_count]
        summed_up = scatter(scatter(regroup(body[:, :, 0:per]), "dp")[0], "tp")[0].astype(F32)
        summed_down = scatter(scatter(regroup(body[:, :, per : 2 * per]), "dp")[0], "tp")[0].astype(F32).T
        taps_part = body[:, :, 2 * per : 2 * per + 9, 0:per].transpose(1, 2, 0, 3).reshape(tp_count, 9, D)
        taps_part = scatter(taps_part.astype(F32), "tp")[0]
        summed_conv_ffn = scatter(taps_part, "dp", 1)
        g_out = scatter(regroup(g_cat[:, tp_count:, 0:per]), "dp")[0, 0]
        rows_out = out_rows(g_out)
        summed_out = sum_slots([rows_out[s] for s in range(tp_count)])
        summed_qkv = scatter(w_cols, "dp")[0]
        summed_conv_qkv = scatter(taps_rows, "dp")[0]

    quad_rows = jnp.concatenate(
        [sums_one[0], sums_one[1], sums_two[0], sums_two[1], sums_two[2], sums_gate], axis=-1
    )
    by_rank = lax.all_gather(quad_rows, "tp", axis=0)
    grad_quads = jnp.sum(by_rank.reshape(2, tp_count // 2, 2, 6 * D), axis=1).reshape(4, 6 * D)
    merged = jnp.concatenate(
        [jnp.sum(grad_quads, axis=0, keepdims=True), jnp.zeros((SLOTS - 1, 6 * D), F32)], axis=0
    )
    grad_slots = jnp.where(tag == 1, merged, grad_quads)
    mod_all = lax.all_gather(grad_slots, "dp", axis=0, tiled=True)
    my_act = lax.dynamic_slice_in_dim(activated_all, dp_rank * share, share, 1).astype(F32)
    my_cond = lax.dynamic_slice_in_dim(condition_all, dp_rank * share, share, 1)
    mod_cols = lax.dynamic_slice_in_dim(mod_all, tp_rank * w_mod.shape[1], w_mod.shape[1], 1)
    summed_mod = jnp.dot(my_act.T, mod_cols, precision=lax.Precision.HIGHEST)
    by_group = mod_all.reshape(mod_all.shape[0], tp_count, -1)
    grad_act = jnp.zeros((mod_all.shape[0], share), F32)
    for s in range(tp_count):
        cols = lax.dynamic_index_in_dim(by_group, lax.rem(tp_rank - s + tp_count, tp_count), 1, keepdims=False)
        grad_act += jnp.dot(cols, w_mod_slots[s].astype(F32).T, precision=lax.Precision.HIGHEST)
    _, silu_pull = jax.vjp(jax.nn.silu, my_cond)
    grad_cols = silu_pull(grad_act)[0]
    time_iota = lax.broadcasted_iota(jnp.int32, (time_index.shape[0], time_table.shape[0]), 1)
    time_hits = (time_index[:, None] == time_iota).astype(F32)
    grad_time = jnp.dot(time_hits.T, grad_cols, precision=lax.Precision.HIGHEST)
    class_iota = lax.broadcasted_iota(jnp.int32, (class_index.shape[0], class_table.shape[0]), 1)
    class_hits = (class_index[:, None] == class_iota).astype(F32)
    grad_class = jnp.dot(class_hits.T, grad_cols, precision=lax.Precision.HIGHEST)
    return (
        mixed,
        grad_tokens,
        grad_time,
        grad_class,
        summed_mod,
        summed_qkv,
        summed_conv_qkv,
        summed_out,
        summed_up,
        summed_conv_ffn,
        summed_down,
    )


def solution(mesh):
    in_specs = (
        P("dp", None),
        P("dp", None),
        P("dp"),
        P(),
        P(),
        P(),
        P(),
        P(None, "tp"),
        P(None, "tp"),
        P(None, "tp"),
        P("tp", None),
        P(None, "tp"),
        P(None, "tp"),
        P("tp", None),
    )
    out_specs = (
        P("dp", None),
        P(("dp", "tp"), None),
        P(None, "dp"),
        P(None, "dp"),
        P("dp", "tp"),
        P("dp", "tp"),
        P(None, ("tp", "dp")),
        P("tp", "dp"),
        P("dp", "tp"),
        P(None, ("tp", "dp")),
        P("tp", "dp"),
    )
    return jax.shard_map(
        per_device, mesh=mesh, in_specs=in_specs, out_specs=out_specs, check_vma=False
    )
```

```python
from functools import partial

import jax
import jax.numpy as jnp
import numpy as np
from jax import lax
from jax.experimental import pallas as pl
from jax.experimental.pallas import tpu as pltpu
from jax.sharding import PartitionSpec as P

D = 768
HEAD_SIZE = 64
SIDE = 64
SLOTS = 4
TOK = SIDE * SIDE
HALO = 2
QROWS = 16
QTOK = QROWS * SIDE
XTOK = (QROWS + 2 * HALO) * SIDE
F32 = jnp.float32
BF16 = jnp.bfloat16
VMEM_MAX = 66_000_000


def dot_nn(a, b):
    return lax.dot_general(a, b, (((1,), (0,)), ((), ())), preferred_element_type=F32)


def dot_nt(a, b):
    return lax.dot_general(a, b, (((1,), (1,)), ((), ())), preferred_element_type=F32)


def dot_tn(a, b):
    return lax.dot_general(a, b, (((0,), (0,)), ((), ())), preferred_element_type=F32)


def parity_matrix():
    one = np.zeros((SIDE, SIDE), np.float32)
    for parity in range(2):
        for j in range(SIDE // 2):
            one[parity * 32 + j, 2 * j + parity] = 1.0
    return jnp.asarray(np.kron(np.eye(4, dtype=np.float32), one), BF16)


def normalised(values):
    mean = jnp.mean(values, axis=-1, keepdims=True)
    centred = values - mean
    variance = jnp.mean(centred * centred, axis=-1, keepdims=True)
    rstd = lax.rsqrt(variance + 1e-06)
    return centred * rstd, rstd


def by_half(values, part):
    rows = values.shape[0]
    shaped = values.reshape(rows // 32, 2, 16, values.shape[-1])
    return (shaped * part[None, :, None, :]).reshape(values.shape)


def spread(part, rows):
    width = part.shape[-1]
    full = jnp.broadcast_to(part[None, :, None, :], (rows // 32, 2, 16, width))
    return full.reshape(rows, width)


def half_sums(values):
    return jnp.sum(values.reshape(values.shape[0] // 32, 2, 16, values.shape[-1]), axis=0)


def column_masks(tag, width):
    j = lax.broadcasted_iota(jnp.int32, (32, width), 0)
    split = tag == 0
    left = jnp.where((j == 0) | ((j == 16) & split), 0.0, 1.0)
    right = jnp.where((j == 31) | ((j == 15) & split), 0.0, 1.0)
    return left, right


def row_scales(tag, row):
    inside = (row >= 0) & (row < SIDE)
    down = jnp.where(inside & jnp.logical_not((tag == 0) & (row == 31)), 1.0, 0.0)
    up = jnp.where(inside & jnp.logical_not((tag == 0) & (row == 32)), 1.0, 0.0)
    return down, up


def conv_step(even, odd, masks, taps, down, up, carry):
    left, right = masks
    odd_left = pltpu.roll(odd, 1, 0) * left
    even_right = pltpu.roll(even, 31, 0) * right
    before_e, before_o, here_e, here_o = carry

    def terms(k):
        return (
            k[0] * odd_left + k[1] * even + k[2] * odd,
            k[0] * even + k[1] * odd + k[2] * even_right,
        )

    last = [t * up for t in taps[6:9]]
    middle = taps[3:6]
    first = [t * down for t in taps[0:3]]
    last_e, last_o = terms(last)
    mid_e, mid_o = terms(middle)
    first_e, first_o = terms(first)
    done = (before_e + last_e, before_o + last_o)
    return done, (here_e + mid_e, here_o + mid_o, first_e, first_o), (odd_left, even_right)


def no_carry(width):
    zero = jnp.zeros((32, width), F32)
    return (zero, zero, zero, zero)


def first_kernel(tag_ref, tok_ref, shift_ref, scale_ref, w_ref, taps_ref, perm_ref, hid_ref, proj_ref, mix_ref, field):
    step = pl.program_id(0)
    tag = tag_ref[0]
    width = w_ref.shape[1]

    @pl.when(step == 0)
    def _():
        field[pl.ds(0, SIDE), :] = jnp.zeros((SIDE, width), F32)
        field[pl.ds((SIDE + 1) * SIDE, SIDE), :] = jnp.zeros((SIDE, width), F32)

    @pl.when(step < 4)
    def _():
        half = step // 2
        shift = shift_ref[half]
        scale = 1.0 + scale_ref[half]

        def chunk(i, carry):
            rows = pl.ds(pl.multiple_of(i * 256, 256), 256)
            ordered = dot_nn(perm_ref[...], tok_ref[rows, :])
            unit, _ = normalised(ordered)
            hidden = (by_half(unit, scale) + spread(shift, 256)).astype(BF16)
            hid_ref[rows, :] = hidden
            out = dot_nn(hidden, w_ref[...])
            for head in range(proj_ref.shape[0]):
                proj_ref[head, rows, :] = out[:, head * 192 : head * 192 + 192]
            field[pl.ds(pl.multiple_of((step * 16 + 1) * SIDE + i * 256, 64), 256), :] = out
            return carry

        lax.fori_loop(0, 4, chunk, 0)

    @pl.when(step > 0)
    def _():
        base = (step - 1) * 16 - 1
        for lane in range(0, width, 128):
            size = min(128, width - lane)
            lanes = slice(lane, lane + size)
            masks = column_masks(tag, size)
            taps = [taps_ref[t : t + 1, lanes] for t in range(9)]

            def one(n, carry):
                row = base + n
                start = pl.multiple_of((row + 1) * SIDE, SIDE)
                even = field[pl.ds(start, 32), lanes]
                odd = field[pl.ds(start + 32, 32), lanes]
                down, up = row_scales(tag, row)
                done, carry, _ = conv_step(even, odd, masks, taps, down, up, carry)
                return done, carry

            def loop(n, carry):
                done, carry = one(n, carry)
                start = pl.multiple_of((n - 2) * SIDE, SIDE)
                for k in range(2):
                    out = done[k].astype(BF16)
                    mix_ref[pl.ds(start + 32 * k, 32), lanes] = out
                return carry

            _, carry = one(0, no_carry(size))
            _, carry = one(1, carry)
            lax.fori_loop(2, 18, loop, carry)


def first_stage(tag, tokens, shift, scale, w_qkv, taps, perm):
    width = w_qkv.shape[1]
    heads = width // 192
    whole = lambda shape: pl.BlockSpec(shape, lambda s: (0,) * len(shape))
    ahead = lambda w: pl.BlockSpec((1024, w), lambda s: (jnp.minimum(s, 3), 0))
    return pl.pallas_call(
        first_kernel,
        grid=(5,),
        in_specs=[
            pl.BlockSpec(memory_space=pltpu.SMEM),
            ahead(D),
            whole((2, 2, D)),
            whole((2, 2, D)),
            whole((D, width)),
            whole((9, width)),
            whole((256, 256)),
        ],
        out_specs=[
            ahead(D),
            pl.BlockSpec((heads, 1024, 192), lambda s: (0, jnp.minimum(s, 3), 0)),
            pl.BlockSpec((1024, width), lambda s: (jnp.maximum(s - 1, 0), 0)),
        ],
        out_shape=[
            jax.ShapeDtypeStruct((TOK, D), BF16),
            jax.ShapeDtypeStruct((heads, TOK, 192), F32),
            jax.ShapeDtypeStruct((TOK, width), BF16),
        ],
        scratch_shapes=[pltpu.VMEM(((SIDE + 2) * SIDE, width), F32)],
        compiler_params=pltpu.CompilerParams(vmem_limit_bytes=VMEM_MAX),
        name="first_stage",
    )(tag, tokens, shift, scale, w_qkv, taps, perm)


def to_row(column, count):
    return jnp.transpose(jnp.broadcast_to(column, (count, 128)))[0:1, :]


def attend_kernel(tag_ref, x_ref, o_ref, lse_ref, *, base):
    tag = tag_ref[0]
    parity = pl.program_id(0) % 2

    def run(split):
        def chunk(c, carry):
            query = x_ref[pl.ds(c * 8, 8), 0, 0, :, base : base + 64].reshape(256, 64)
            query = query * jnp.asarray(0.125, BF16)
            if split:
                rows = pl.ds((c // 2) * 16, 16)
                count = 512
            else:
                rows = pl.ds(0, 32)
                count = 1024
            keys = x_ref[rows, 0, 0, :, base + 64 : base + 128].reshape(count, 64)
            values = x_ref[rows, 0, 0, :, base + 128 : base + 192].reshape(count, 64)
            scores = dot_nt(query, keys)
            if split:
                qj = lax.broadcasted_iota(jnp.int32, (256, count), 0) & 16
                kj = lax.broadcasted_iota(jnp.int32, (256, count), 1) & 16
                scores = jnp.where(qj == kj, scores, -1e30)
            top = jnp.max(scores, axis=-1, keepdims=True)
            expo = jnp.exp(scores - top)
            total = jnp.sum(expo, axis=-1, keepdims=True)
            out = dot_nn(expo.astype(BF16), values) / total
            out = out.astype(BF16).reshape(8, 32, 64)
            for b in range(2):

                @pl.when(parity == b)
                def _():
                    o_ref[pl.ds(c * 8, 8), 0, :, b * 64 : b * 64 + 64] = out

            lse_ref[0, 0:1, pl.ds(pl.multiple_of(c * 256, 256), 256)] = to_row(top + jnp.log(total), 256)
            return carry

        lax.fori_loop(0, 4, chunk, 0)

    pl.when(tag == 1)(lambda: run(False))
    pl.when(tag != 1)(lambda: run(True))


def group_block(width):
    at = lambda g: jnp.minimum(g, 3)
    return pl.BlockSpec((32, 1, 1, 32, width), lambda g: (0, at(g) // 2, at(g) % 2, 0, 0))


def pair_block():
    return pl.BlockSpec((32, 1, 32, 128), lambda g: (0, jnp.minimum(g, 3) // 2, 0, 0))


def lse_block():
    return pl.BlockSpec((1, 8, 1024), lambda g: (jnp.minimum(g, 3), 0, 0))


def attend_stage(tag, mixed_qkv, head):
    out, lse = pl.pallas_call(
        partial(attend_kernel, base=head * 192),
        grid=(4,),
        in_specs=[pl.BlockSpec(memory_space=pltpu.SMEM), group_block(mixed_qkv.shape[-1])],
        out_specs=[pair_block(), lse_block()],
        out_shape=[
            jax.ShapeDtypeStruct((32, 2, 32, 128), BF16),
            jax.ShapeDtypeStruct((4, 8, 1024), F32),
        ],
        compiler_params=pltpu.CompilerParams(vmem_limit_bytes=VMEM_MAX),
        cost_estimate=pl.CostEstimate(flops=2_000_000_000, transcendentals=4_000_000, bytes_accessed=4_000_000),
        name="attend_stage",
    )(tag, mixed_qkv)
    return out, lse


def kernel_sums(acc, even, odd, odd_left, even_right, plain, scale, first):
    plain_e, plain_o = plain

    def fold(values):
        return jnp.sum(values.reshape(4, 8, values.shape[-1]), axis=0)

    terms = [
        fold(odd * plain_e) + fold(even_right * plain_o),
        fold(even * plain_e) + fold(odd * plain_o),
        fold(odd_left * plain_e) + fold(even * plain_o),
    ]
    out = list(acc)
    for t in range(3):
        term = terms[t] if scale is None else terms[t] * scale
        out[first + t] = acc[first + t] + term
    return out


POLY = (
    0.13241715506535054,
    0.12108811680396304,
    0.17555028579228482,
    -0.0796444980816301,
    0.3217932733518851,
    -0.21571441684424994,
    0.04451008654080756,
)


def gelu_parts(z):
    size = jnp.abs(z)
    t = 1.0 / (1.0 + 0.33 * size)
    expo = jnp.exp(z * z * -0.5)
    poly = POLY[6]
    for c in POLY[5::-1]:
        poly = poly * t + c
    tail = poly * t * expo
    cdf = jnp.where(z >= 0.0, 1.0 - tail, tail)
    value = z * cdf
    slope = cdf + z * (expo * 0.3989422804014327)
    return value, slope


def mod_part(mods_ref, i):
    return mods_ref[:, i * D : (i + 1) * D]


def feed_kernel(
    info_ref,
    *refs,
):
    heads_refs, refs = refs[0:12], refs[12:]
    feed_body(info_ref, heads_refs, *refs)


def feed_body(
    info_ref,
    heads_refs,
    w_out_ref,
    tok_ref,
    cot_ref,
    mods_ref,
    w_up_ref,
    w_down_ref,
    taps_ref,
    perm_ref,
    mixed_ref,
    up_ref,
    slope_ref,
    act_ref,
    after_ref,
    att_ref,
    hidden_out,
    heads_out,
    sums_ref,
    hidden_ref,
    hcat_ref,
    feed_ref,
    sum_ref,
):
    step = pl.program_id(0)
    tag = info_ref[0]
    first_row = info_ref[1] * QROWS - HALO
    chans = up_ref.shape[2]
    groups = w_out_ref.shape[0]
    heads = len(heads_refs) // groups
    rank = info_ref[1]

    @pl.when(step == 0)
    def _():
        gate_one, shift_two, scale_two = mod_part(mods_ref, 2), mod_part(mods_ref, 3), 1.0 + mod_part(mods_ref, 4)

        def unpack(i, carry):
            for g in range(groups):
                for head in range(heads):
                    ref = heads_refs[head * groups + g]
                    for b in range(2):
                        rows = pl.ds(pl.multiple_of(i * SIDE + b * 32, 32), 32)
                        lane = (g * heads + head) * 64
                        hcat_ref[rows, lane : lane + 64] = ref[i, :, b * 64 : b * 64 + 64]
            return carry

        lax.fori_loop(0, XTOK // SIDE, unpack, 0)

        def part(start, size):
            rows = pl.ds(start, size)
            perm = perm_ref[0:size, 0:size]
            ordered = dot_nn(perm, tok_ref[rows, :])
            attention = jnp.zeros((size, D), F32)
            width = heads * HEAD_SIZE
            for g in range(groups):
                source = lax.rem(rank - g + groups, groups)
                term = dot_nn(hcat_ref[rows, g * width : g * width + width], w_out_ref[source])
                attention = attention + term.astype(BF16).astype(F32)
            after = ordered + by_half(attention, gate_one)
            unit, _ = normalised(after)
            hidden = (by_half(unit, scale_two) + spread(shift_two, size)).astype(BF16)
            hidden_ref[rows, :] = hidden
            if size == 256:
                mine = pl.ds(pl.multiple_of(start - 128, 256), 256)
                att_ref[mine, :] = attention.astype(BF16)
                after_ref[mine, :] = after
                hidden_out[mine, :] = hidden
                heads_out[mine, :] = hcat_ref[rows, :]

        part(0, 128)
        part(XTOK - 128, 128)

        def loop(i, carry):
            part(pl.multiple_of(128 + i * 256, 128), 256)
            return carry

        lax.fori_loop(0, 4, loop, 0)
        feed_ref[...] = jnp.zeros_like(feed_ref)

    w_up = w_up_ref[...].reshape(D, chans)
    w_down = w_down_ref[...].reshape(chans, D)

    def up_loop(i, carry):
        rows = pl.ds(pl.multiple_of(i * 640, 128), 640)
        up_ref[0, rows, :] = dot_nn(hidden_ref[rows, :], w_up)
        return carry

    lax.fori_loop(0, 2, up_loop, 0)

    for lane in range(0, chans, 128):
        lanes = slice(lane, lane + 128)
        masks = column_masks(tag, 128)
        taps = [taps_ref[0, t : t + 1, lanes] for t in range(9)]

        def one(n, carry):
            start = pl.multiple_of(n * SIDE, SIDE)
            even = up_ref[0, pl.ds(start, 32), lanes]
            odd = up_ref[0, pl.ds(start + 32, 32), lanes]
            down, up = row_scales(tag, first_row + n)
            done, carry, _ = conv_step(even, odd, masks, taps, down, up, carry)
            return done, carry

        def loop(n, carry):
            done, carry = one(n, carry)
            for k in range(2):
                start = pl.multiple_of((n - 2) * SIDE + 32 * k, 32)
                value, slope = gelu_parts(done[k])
                act_ref[0, pl.ds(start, 32), lanes] = value.astype(BF16)
                slope_ref[0, pl.ds(start, 32), lanes] = slope
            return carry

        _, carry = one(0, no_carry(128))
        _, carry = one(1, carry)
        lax.fori_loop(2, QROWS + 2 * HALO, loop, carry)

    def token_loop(i, carry):
        rows = pl.ds(pl.multiple_of(i * 512, 512), 512)
        feed_ref[rows, :] += dot_nn(act_ref[0, pl.ds(pl.multiple_of(64 + i * 512, 64), 512), :], w_down)
        return carry

    lax.fori_loop(0, 2, token_loop, 0)

    @pl.when(step == pl.num_programs(0) - 1)
    def _():
        gate_two = mod_part(mods_ref, 5)
        sum_ref[...] = jnp.zeros_like(sum_ref)

        def loop(i, carry):
            rows = pl.ds(pl.multiple_of(i * 256, 256), 256)
            wide = pl.ds(pl.multiple_of(128 + i * 256, 128), 256)
            feed = feed_ref[rows, :]
            result = (after_ref[rows, :] + by_half(feed, gate_two)).astype(BF16)
            mixed_ref[rows, :] = dot_tn(perm_ref[...], result).astype(BF16)
            sum_ref[...] += half_sums(dot_nn(perm_ref[...], cot_ref[wide, :]) * feed)
            return carry

        lax.fori_loop(0, 4, loop, 0)
        sums_ref[...] = jnp.sum(sum_ref[...], axis=1)


def feed_stage(info, heads, w_out, tok, cot, mods, w_rows, taps, perm):
    dps, chunks, tall, chans = w_rows.shape
    per = D // dps
    once = pl.Buffered(1)
    whole = lambda shape: pl.BlockSpec(shape, lambda s: (0,) * len(shape), pipeline_mode=once)
    chunk = lambda rows: pl.BlockSpec((1, rows, chans), lambda s: (s, 0, 0))
    return pl.pallas_call(
        feed_kernel,
        grid=(chunks,),
        in_specs=[
            pl.BlockSpec(memory_space=pltpu.SMEM),
            *[whole(h.shape) for h in heads],
            whole(w_out.shape),
            whole((XTOK, D)),
            whole((XTOK, D)),
            whole((2, 6 * D)),
            pl.BlockSpec((dps, 1, per, chans), lambda s: (0, s, 0, 0)),
            pl.BlockSpec((dps, 1, per, chans), lambda s: (0, s, 1, 0)),
            chunk(9),
            whole((256, 256)),
        ],
        out_specs=[
            whole((QTOK, D)),
            chunk(XTOK),
            chunk(XTOK - 128),
            chunk(XTOK - 128),
            whole((QTOK, D)),
            whole((QTOK, D)),
            whole((QTOK, D)),
            whole((QTOK, D)),
            whole((2, D)),
        ],
        out_shape=[
            jax.ShapeDtypeStruct((QTOK, D), BF16),
            jax.ShapeDtypeStruct((chunks, XTOK, chans), F32),
            jax.ShapeDtypeStruct((chunks, XTOK - 128, chans), F32),
            jax.ShapeDtypeStruct((chunks, XTOK - 128, chans), BF16),
            jax.ShapeDtypeStruct((QTOK, D), F32),
            jax.ShapeDtypeStruct((QTOK, D), BF16),
            jax.ShapeDtypeStruct((QTOK, D), BF16),
            jax.ShapeDtypeStruct((QTOK, D), BF16),
            jax.ShapeDtypeStruct((2, D), F32),
        ],
        scratch_shapes=[
            pltpu.VMEM((XTOK, D), BF16),
            pltpu.VMEM((XTOK, D), BF16),
            pltpu.VMEM((QTOK, D), F32),
            pltpu.VMEM((2, 16, D), F32),
        ],
        compiler_params=pltpu.CompilerParams(vmem_limit_bytes=VMEM_MAX),
        cost_estimate=pl.CostEstimate(flops=20_000_000_000, transcendentals=8_000_000, bytes_accessed=80_000_000),
        name="feed_stage",
    )(info, *heads, w_out, tok, cot, mods, w_rows, w_rows, taps, perm)


def feed_back_kernel(
    info_ref,
    up_ref,
    slope_ref,
    act_ref,
    w_up_ref,
    w_down_ref,
    taps_ref,
    cot_ref,
    hidden_ref,
    after_ref,
    att_ref,
    heads_ref,
    w_out_ref,
    mods_ref,
    perm_ref,
    gcat_ref,
    g0_ref,
    g1_ref,
    g2_ref,
    gafter_ref,
    sums_ref,
    hidden_t,
    gfeed_ref,
    gfeed_t,
    ghid_ref,
    gact_ref,
    gup_ref,
    sum_ref,
    gtaps_ref,
):
    step = pl.program_id(0)
    tag = info_ref[0]
    first_row = info_ref[1] * QROWS - HALO
    chans = up_ref.shape[2]
    dps, per = w_up_ref.shape[0], w_up_ref.shape[2]

    @pl.when(step == 0)
    def _():
        gate_two = mod_part(mods_ref, 5)

        def part(start, size):
            rows = pl.ds(start, size)
            perm = perm_ref[0:size, 0:size]
            gfeed_ref[rows, :] = by_half(dot_nn(perm, cot_ref[rows, :]), gate_two).astype(BF16)

        def loop(i, carry):
            part(pl.multiple_of(i * 256, 256), 256)
            return carry

        lax.fori_loop(0, XTOK // 256, loop, 0)
        hidden_t[...] = jnp.transpose(hidden_ref[...])
        gfeed_t[...] = jnp.transpose(gfeed_ref[pl.ds(128, QTOK), :])
        ghid_ref[...] = jnp.zeros_like(ghid_ref)

    @pl.when(step < pl.num_programs(0) - 1)
    def _():
        w_up = w_up_ref[...].reshape(D, chans)
        w_down = w_down_ref[...].reshape(chans, D)

        def gact_loop(i, carry):
            rows = pl.ds(pl.multiple_of(i * 576, 64), 576)
            out = dot_nt(gfeed_ref[pl.ds(pl.multiple_of(64 + i * 576, 64), 576), :], w_down)
            gact_ref[rows, :] = out * slope_ref[0, rows, :]
            return carry

        lax.fori_loop(0, 2, gact_loop, 0)

        for lane in range(0, chans, 128):
            lanes = slice(lane, lane + 128)
            masks = column_masks(tag, 128)
            taps = [taps_ref[0, 8 - t : 9 - t, lanes] for t in range(9)]

            def one(n, carry, sums):
                start = pl.multiple_of(n * SIDE, SIDE)
                low, high = pl.ds(start, 32), pl.ds(start + 32, 32)
                even, odd = gact_ref[low, lanes], gact_ref[high, lanes]
                row = first_row + 1 + n
                down, up = row_scales(tag, row)
                done, carry, shifted = conv_step(even, odd, masks, taps, down, up, carry)
                if sums is not None:
                    above = jnp.where((row == 0) | ((tag == 0) & (row == 32)), 0.0, 1.0)
                    below = jnp.where((row == SIDE - 1) | ((tag == 0) & (row == 31)), 0.0, 1.0)
                    for i, scale in ((0, above), (1, None), (2, below)):
                        at = pl.multiple_of((n + i) * SIDE, SIDE)
                        plain = (up_ref[0, pl.ds(at, 32), lanes], up_ref[0, pl.ds(at + 32, 32), lanes])
                        sums = kernel_sums(sums, even, odd, *shifted, plain, scale, 3 * i)
                return done, carry, sums

            def put(n, done):
                for k in range(2):
                    start = pl.multiple_of((n - 2) * SIDE + 32 * k, 32)
                    gup_ref[pl.ds(start, 32), lanes] = done[k].astype(BF16)

            def loop(n, state):
                done, carry, sums = one(n, state[0], list(state[1]))
                put(n, done)
                return carry, tuple(sums)

            zero = jnp.zeros((8, 128), F32)
            _, carry, _ = one(0, no_carry(128), None)
            _, carry, sums = one(1, carry, [zero] * 9)
            carry, sums = lax.fori_loop(2, QROWS + 1, loop, (carry, tuple(sums)))
            done, carry, _ = one(QROWS + 1, carry, None)
            put(QROWS + 1, done)
            for t in range(9):
                gtaps_ref[t : t + 1, lanes] = jnp.sum(sums[t], axis=0, keepdims=True)

        def token_loop(i, carry):
            rows = pl.ds(pl.multiple_of(i * 512, 512), 512)
            ghid_ref[rows, :] += dot_nt(gup_ref[rows, :], w_up)
            return carry

        lax.fori_loop(0, 2, token_loop, 0)

        def weight_loop(i, carry):
            rows = pl.ds(pl.multiple_of(i * 384, 128), 384)
            blocks = pl.ds(i * (dps // 2), dps // 2)
            out = dot_nn(hidden_t[rows, :], gup_ref[...])
            gcat_ref[blocks, 0, 0:per, :] = out.reshape(dps // 2, per, chans).astype(BF16)
            out = dot_nn(gfeed_t[rows, :], act_ref[0, pl.ds(64, QTOK), :])
            gcat_ref[blocks, 0, per : 2 * per, :] = out.reshape(dps // 2, per, chans).astype(BF16)
            return carry

        lax.fori_loop(0, 2, weight_loop, 0)
        sums = jnp.concatenate([gtaps_ref[0:9, :], jnp.zeros((7, chans), F32)], axis=0)
        for d in range(dps):
            part_sums = jnp.concatenate([sums[:, d * per : d * per + per], jnp.zeros((16, chans - per), F32)], axis=1)
            gcat_ref[d, 0, 2 * per : 2 * per + 16, :] = part_sums.astype(BF16)

    @pl.when(step == pl.num_programs(0) - 1)
    def _():
        gate_one, scale_two = mod_part(mods_ref, 2), 1.0 + mod_part(mods_ref, 4)
        groups = w_out_ref.shape[0]
        sum_ref[...] = jnp.zeros_like(sum_ref)

        def loop(i, carry):
            rows = pl.ds(pl.multiple_of(i * 256, 256), 256)
            wide = pl.ds(pl.multiple_of(128 + i * 256, 128), 256)
            cot = dot_nn(perm_ref[...], cot_ref[wide, :])
            unit, rstd = normalised(after_ref[rows, :])
            grad = ghid_ref[rows, :]
            sum_ref[1] += half_sums(grad)
            sum_ref[2] += half_sums(grad * unit)
            inner = by_half(grad, scale_two)
            mean = jnp.mean(inner, axis=-1, keepdims=True)
            along = jnp.mean(inner * unit, axis=-1, keepdims=True)
            gafter = cot + rstd * (inner - mean - unit * along)
            sum_ref[0] += half_sums(gafter * att_ref[rows, :].astype(F32))
            gafter_ref[rows, :] = gafter
            gatt = by_half(gafter, gate_one).astype(BF16)
            gup_ref[rows, :] = gatt
            for g in range(groups):
                target = lax.rem(info_ref[1] + g, groups)
                out = dot_nt(gatt, w_out_ref[target]).astype(BF16).reshape(4, 2, 32, w_out_ref.shape[1])
                for head, ref in enumerate((g0_ref, g1_ref, g2_ref)):
                    for b in range(2):
                        ref[g, pl.ds(i * 4, 4), :, b * 64 : b * 64 + 64] = out[:, b, :, head * 64 : head * 64 + 64]
            return carry

        lax.fori_loop(0, 4, loop, 0)
        out = dot_tn(gup_ref[...], heads_ref[...])
        gcat_ref[:, 0, 0:per, :] = out.reshape(dps, per, D).astype(BF16)
        gcat_ref[:, 0, per:, :] = jnp.zeros((dps, per + 16, D), BF16)
        sums_ref[...] = jnp.sum(sum_ref[...], axis=2)


def feed_back_stage(info, up, slope, act, w_rows, taps, cot, hidden, after, att, heads, w_out, mods, perm):
    dps, chunks, tall, chans = w_rows.shape
    groups = w_out.shape[0]
    per = D // dps
    once = pl.Buffered(1)
    whole = lambda shape: pl.BlockSpec(shape, lambda s: (0,) * len(shape), pipeline_mode=once)
    at = lambda s: jnp.minimum(s, chunks - 1)
    chunk = lambda rows: pl.BlockSpec((1, rows, chans), lambda s: (at(s), 0, 0))
    sent = (groups, QROWS, 32, 128)
    return pl.pallas_call(
        feed_back_kernel,
        grid=(chunks + 1,),
        in_specs=[
            pl.BlockSpec(memory_space=pltpu.SMEM),
            chunk(XTOK),
            chunk(XTOK - 128),
            chunk(XTOK - 128),
            pl.BlockSpec((dps, 1, per, chans), lambda s: (0, at(s), 0, 0)),
            pl.BlockSpec((dps, 1, per, chans), lambda s: (0, at(s), 1, 0)),
            chunk(9),
            whole((XTOK, D)),
            whole((QTOK, D)),
            whole((QTOK, D)),
            whole((QTOK, D)),
            whole((QTOK, D)),
            whole(w_out.shape),
            whole((2, 6 * D)),
            whole((256, 256)),
        ],
        out_specs=[
            pl.BlockSpec((dps, 1, 2 * per + 16, chans), lambda s: (0, s, 0, 0)),
            whole(sent),
            whole(sent),
            whole(sent),
            whole((QTOK, D)),
            whole((3, 2, D)),
        ],
        out_shape=[
            jax.ShapeDtypeStruct((dps, chunks + 1, 2 * per + 16, chans), BF16),
            jax.ShapeDtypeStruct(sent, BF16),
            jax.ShapeDtypeStruct(sent, BF16),
            jax.ShapeDtypeStruct(sent, BF16),
            jax.ShapeDtypeStruct((QTOK, D), F32),
            jax.ShapeDtypeStruct((3, 2, D), F32),
        ],
        scratch_shapes=[
            pltpu.VMEM((D, QTOK), BF16),
            pltpu.VMEM((XTOK, D), BF16),
            pltpu.VMEM((D, QTOK), BF16),
            pltpu.VMEM((QTOK, D), F32),
            pltpu.VMEM((XTOK - 128, chans), F32),
            pltpu.VMEM((QTOK, chans), BF16),
            pltpu.VMEM((3, 2, 16, D), F32),
            pltpu.VMEM((16, chans), F32),
        ],
        compiler_params=pltpu.CompilerParams(vmem_limit_bytes=VMEM_MAX),
        cost_estimate=pl.CostEstimate(flops=30_000_000_000, transcendentals=8_000_000, bytes_accessed=80_000_000),
        name="feed_back_stage",
    )(info, up, slope, act, w_rows, w_rows, taps, cot, hidden, after, att, heads, w_out, mods, perm)


MESH = pl.DeviceIdType.MESH
HEADS_DEV = 3
GROUPS = 4


def back_kernel(
    tag_ref,
    x_ref,
    o0_ref,
    o1_ref,
    o2_ref,
    lse0_ref,
    lse1_ref,
    lse2_ref,
    proj_ref,
    taps_ref,
    mods_ref,
    perm_ref,
    gh0_hbm,
    gh1_hbm,
    gh2_hbm,
    hid_hbm,
    w_hbm,
    tok_hbm,
    gafter_hbm,
    out_ref,
    gw_ref,
    gtaps_ref,
    sums_ref,
    do_buf,
    gsend,
    grecv,
    kv_buf,
    qz_buf,
    zd_buf,
    row_buf,
    taps_buf,
    acc_ref,
    field,
    flat,
    hid_buf,
    w_buf,
    tok_buf,
    gafter_buf,
    ghid_ref,
    sum_ref,
    turn_ref,
    local_sem,
    own_sem,
    do_send,
    do_recv,
    g_send,
    g_recv,
):
    step = pl.program_id(0)
    tag = tag_ref[0]
    split = tag == 0
    rank = lax.axis_index("tp")
    gh_hbm = (gh0_hbm, gh1_hbm, gh2_hbm)

    def do_copy(head, slot):
        peer = lax.rem(rank + slot, 4)
        return pltpu.make_async_remote_copy(
            gh_hbm[head].at[slot],
            do_buf.at[head, slot],
            do_send.at[head, slot],
            do_recv.at[head, slot],
            device_id={"tp": peer},
            device_id_type=MESH,
        )

    def own_copy(head):
        return pltpu.make_async_copy(gh_hbm[head].at[0], do_buf.at[head, 0], own_sem.at[head])

    def g_copy(head, slot):
        peer = lax.rem(rank + slot, 4)
        return pltpu.make_async_remote_copy(
            gsend.at[head, slot],
            grecv.at[head, slot],
            g_send.at[head, slot],
            g_recv.at[head, slot],
            device_id={"tp": peer},
            device_id_type=MESH,
        )

    loads = [
        pltpu.make_async_copy(hid_hbm, hid_buf, local_sem.at[0]),
        pltpu.make_async_copy(w_hbm, w_buf, local_sem.at[1]),
        pltpu.make_async_copy(tok_hbm, tok_buf, local_sem.at[2]),
        pltpu.make_async_copy(gafter_hbm, gafter_buf, local_sem.at[3]),
    ]

    @pl.when(step == 0)
    def _():
        barrier = pltpu.get_barrier_semaphore()
        for slot in range(1, 4):
            peer = lax.rem(rank + slot, 4)
            pl.semaphore_signal(barrier, inc=1, device_id={"tp": peer}, device_id_type=MESH)
        pl.semaphore_wait(barrier, 3)
        for head in range(HEADS_DEV):
            for slot in range(1, 4):
                do_copy(head, slot).start()
            own_copy(head).start()
        for load in loads:
            load.start()

    for head, (o_ref, lse_ref) in enumerate(((o0_ref, lse0_ref), (o1_ref, lse1_ref), (o2_ref, lse2_ref))):

        @pl.when(step == head)
        def _():
            base = head * 192
            taps_buf[0:9, :] = taps_ref[:, base : base + 192]
            zero = jnp.zeros((1024, 64), BF16)
            for g in range(GROUPS):
                a, b = g // 2, g % 2
                kv_buf[g] = x_ref[:, a, b, :, base + 64 : base + 192].reshape(1024, 128)
                query = x_ref[:, a, b, :, base : base + 64].reshape(1024, 64) * jnp.asarray(0.125, BF16)
                qz_buf[g] = jnp.concatenate([query, zero], axis=1)
            own_copy(head).wait()
            for slot in range(1, 4):
                do_copy(head, slot).wait_recv()
            for g in range(GROUPS):
                a, b = g // 2, g % 2
                for quarter in range(4):
                    slot = lax.rem(rank - quarter + 4, 4)
                    rows = slice(quarter * 256, quarter * 256 + 256)
                    grad = do_buf[head, slot, :, :, b * 64 : b * 64 + 64].reshape(8, 2, 32, 64)[:, a].reshape(256, 64)
                    zd_buf[g, rows, :] = jnp.concatenate([zero[0:256], grad], axis=1)
                    out = o_ref[quarter * 8 : quarter * 8 + 8, a, :, b * 64 : b * 64 + 64].reshape(256, 64)
                    delta = jnp.sum(grad.astype(F32) * out.astype(F32), axis=-1, keepdims=True)
                    row_buf[g, 0:1, rows] = to_row(delta, 256)
                row_buf[g, 1:2, :] = lse_ref[g, 0:1, :]

    @pl.when(step < HEADS_DEV)
    def _():
        def group(g, carry):
            acc_ref[...] = jnp.zeros_like(acc_ref)

            def chunk(c, carry):
                mine = pl.ds(pl.multiple_of(c * 256, 256), 256)
                delta = row_buf[g, 0:1, mine]
                lse = row_buf[g, 1:2, mine]
                place = lax.broadcasted_iota(jnp.int32, (1, 256), 1) & 16
                far = jnp.float32(1e30)
                by_j = [jnp.where(split & (place != 0), far, 0.0), jnp.where(split & (place == 0), far, 0.0)]
                by_i = [jnp.where(split & (c >= 2), far, 0.0), jnp.where(split & (c < 2), far, 0.0)]
                kv = kv_buf[g]
                query, grad = qz_buf[g, mine, :], zd_buf[g, mine, :]
                logits = dot_nt(kv, query).reshape(2, 16, 2, 16, 256)
                probs = [
                    [jnp.exp(logits[i, :, j] - (lse + by_i[i] + by_j[j])[:, None, :]) for j in range(2)] for i in range(2)
                ]
                probs = jnp.stack([jnp.stack(p, axis=1) for p in probs], axis=0).reshape(1024, 256)
                scores = (probs * (dot_nt(kv, grad) - delta)).astype(BF16)
                acc_ref[...] += dot_nn(scores, query) + dot_nn(probs.astype(BF16), grad)
                grad_query = dot_tn(scores, kv)[:, 0:64] * 0.125
                field[pl.ds(c * 8, 8), g // 2, g % 2, :, 0:64] = grad_query.reshape(8, 32, 64)
                return carry

            lax.fori_loop(0, 4, chunk, 0)
            field[:, g // 2, g % 2, :, 64:192] = acc_ref[...].reshape(32, 32, 128)
            return carry

        lax.fori_loop(0, GROUPS, group, 0)
        for start_lane, size in ((0, 128), (128, 64)):
            lanes = slice(start_lane, start_lane + size)
            masks = column_masks(tag, size)
            taps = [taps_buf[8 - t : 9 - t, lanes] for t in range(9)]

            def one(row, carry, sums, has_above, has_below):
                even = field[row // 2, row % 2, 0, :, lanes]
                odd = field[row // 2, row % 2, 1, :, lanes]
                down, up = row_scales(tag, row)
                done, carry, shifted = conv_step(even, odd, masks, taps, down, up, carry)
                for i in range(3):
                    if (i == 0 and not has_above) or (i == 2 and not has_below):
                        continue
                    at = pl.multiple_of((row + i - 1) * SIDE, SIDE)
                    plain = (proj_ref[0, pl.ds(at, 32), lanes], proj_ref[0, pl.ds(at + 32, 32), lanes])
                    scale = (up, None, down)[i]
                    sums = kernel_sums(sums, even, odd, *shifted, plain, scale, 3 * i)
                return done, carry, sums

            def put(row, done):
                quarter = row // QROWS
                slot = lax.rem(quarter - rank + 4, 4)
                for k in range(2):
                    out = done[k].astype(BF16)
                    at = k * 192 + start_lane
                    gsend[step, slot, row - quarter * QROWS, :, at : at + size] = out
                    flat[pl.ds(pl.multiple_of(row * SIDE + 32 * k, 32), 32), lanes] = out

            def loop(row, state):
                done, carry, sums = one(row, state[0], list(state[1]), True, True)
                put(row - 1, done)
                return carry, tuple(sums)

            zero = jnp.zeros((8, size), F32)
            _, carry, sums = one(0, no_carry(size), [zero] * 9, False, True)
            carry, sums = lax.fori_loop(1, SIDE - 1, loop, (carry, tuple(sums)))
            done, carry, sums = one(SIDE - 1, carry, list(sums), True, False)
            put(SIDE - 2, done)
            put(SIDE - 1, carry[0:2])
            for t in range(9):
                gtaps_ref[0, t : t + 1, lanes] = jnp.sum(sums[t], axis=0, keepdims=True)

    for head in range(HEADS_DEV):

        @pl.when(step == head)
        def _():
            for slot in range(1, 4):
                g_copy(head, slot).start()
            if head == 0:
                loads[0].wait()

    @pl.when(step < HEADS_DEV)
    def _():
        gw_ref[0] = jnp.zeros((192, D), F32)

        def part(i, carry):
            rows = pl.ds(pl.multiple_of(i * 512, 512), 512)
            gw_ref[0] += dot_tn(flat[rows, :], hid_buf[rows, :])
            return carry

        lax.fori_loop(0, TOK // 512, part, 0)

    @pl.when(step == HEADS_DEV)
    def _():
        for load in loads[1:]:
            load.wait()
        for head in range(HEADS_DEV):
            for slot in range(1, 4):
                g_copy(head, slot).wait()
                do_copy(head, slot).wait_send()
        for slot in range(4):
            source = lax.rem(rank - slot + 4, 4)
            weight = w_buf[:, source].reshape(D, w_buf.shape[-1])
            for head in range(HEADS_DEV):
                ref = gsend if slot == 0 else grecv
                for b in range(2):
                    part = ref[head, slot, :, :, b * 192 : b * 192 + 192].reshape(QROWS * 32, 192)
                    term = dot_nt(part, weight[:, head * 192 : head * 192 + 192]).reshape(QROWS, 32, D)
                    if slot == 0 and head == 0:
                        ghid_ref[:, b] = term
                    else:
                        ghid_ref[:, b] += term
        scale = 1.0 + mods_ref[:, D : 2 * D]
        sum_ref[...] = jnp.zeros_like(sum_ref)

        def loop(i, carry):
            rows = pl.ds(pl.multiple_of(i * 256, 256), 256)
            ordered = dot_nn(perm_ref[...], tok_buf[rows, :])
            unit, rstd = normalised(ordered)
            grad = ghid_ref[pl.ds(i * 4, 4)].reshape(256, D)
            sum_ref[0] += half_sums(grad)
            sum_ref[1] += half_sums(grad * unit)
            inner = by_half(grad, scale)
            mean = jnp.mean(inner, axis=-1, keepdims=True)
            along = jnp.mean(inner * unit, axis=-1, keepdims=True)
            out = gafter_buf[rows, :] + rstd * (inner - mean - unit * along)
            for lane in range(D // 128):
                for r in range(4):
                    for parity in range(2):
                        at = r * 64 + parity * 32
                        turn_ref[lane, pl.ds(r * 64 + parity, 32, stride=2), :] = out[
                            at : at + 32, lane * 128 : lane * 128 + 128
                        ]
                out_ref[rows, lane * 128 : lane * 128 + 128] = turn_ref[lane]
            return carry

        lax.fori_loop(0, QTOK // 256, loop, 0)
        sums_ref[...] = jnp.sum(sum_ref[...], axis=2)


def back_stage(tag, mixed_qkv, heads_out, lse, proj, taps, mods, perm, gheads, hidden, w_qkv, tok, gafter):
    once = pl.Buffered(1)
    whole = lambda shape: pl.BlockSpec(shape, lambda s: (0,) * len(shape), pipeline_mode=once)
    hbm = pl.BlockSpec(memory_space=pl.ANY)
    at = lambda s: jnp.minimum(s, HEADS_DEV - 1)
    return pl.pallas_call(
        back_kernel,
        grid=(HEADS_DEV + 1,),
        in_specs=[
            pl.BlockSpec(memory_space=pltpu.SMEM),
            whole(mixed_qkv.shape),
            *[whole(o.shape) for o in heads_out],
            *[whole(v.shape) for v in lse],
            pl.BlockSpec((1, TOK, 192), lambda s: (at(s), 0, 0)),
            whole(taps.shape),
            whole(mods.shape),
            whole(perm.shape),
            *[hbm] * 7,
        ],
        out_specs=[
            whole((QTOK, D)),
            pl.BlockSpec((1, 192, D), lambda s: (at(s), 0, 0)),
            pl.BlockSpec((1, 9, 192), lambda s: (at(s), 0, 0)),
            whole((2, 2, D)),
        ],
        out_shape=[
            jax.ShapeDtypeStruct((QTOK, D), F32),
            jax.ShapeDtypeStruct((HEADS_DEV, 192, D), F32),
            jax.ShapeDtypeStruct((HEADS_DEV, 9, 192), F32),
            jax.ShapeDtypeStruct((2, 2, D), F32),
        ],
        scratch_shapes=[
            pltpu.VMEM((HEADS_DEV, 4, QROWS, 32, 128), BF16),
            pltpu.VMEM((HEADS_DEV, 4, QROWS, 32, 384), BF16),
            pltpu.VMEM((HEADS_DEV, 4, QROWS, 32, 384), BF16),
            pltpu.VMEM((GROUPS, 1024, 128), BF16),
            pltpu.VMEM((GROUPS, 1024, 128), BF16),
            pltpu.VMEM((GROUPS, 1024, 128), BF16),
            pltpu.VMEM((GROUPS, 8, 1024), F32),
            pltpu.VMEM((16, 192), F32),
            pltpu.VMEM((1024, 128), F32),
            pltpu.VMEM((32, 2, 2, 32, 192), F32),
            pltpu.VMEM((TOK, 192), BF16),
            pltpu.VMEM((TOK, D), BF16),
            pltpu.VMEM(w_qkv.shape, BF16),
            pltpu.VMEM((QTOK, D), BF16),
            pltpu.VMEM((QTOK, D), F32),
            pltpu.VMEM((QROWS, 2, 32, D), F32),
            pltpu.VMEM((2, 2, 16, D), F32),
            pltpu.VMEM((D // 128, 256, 128), F32),
            pltpu.SemaphoreType.DMA((4,)),
            pltpu.SemaphoreType.DMA((HEADS_DEV,)),
            pltpu.SemaphoreType.DMA((HEADS_DEV, 4)),
            pltpu.SemaphoreType.DMA((HEADS_DEV, 4)),
            pltpu.SemaphoreType.DMA((HEADS_DEV, 4)),
            pltpu.SemaphoreType.DMA((HEADS_DEV, 4)),
        ],
        compiler_params=pltpu.CompilerParams(vmem_limit_bytes=VMEM_MAX, collective_id=0, has_side_effects=True),
        cost_estimate=pl.CostEstimate(flops=40_000_000_000, transcendentals=12_000_000, bytes_accessed=60_000_000),
        name="back_stage",
    )(tag, mixed_qkv, *heads_out, *lse, proj, taps, mods, perm, *gheads, hidden, w_qkv, tok, gafter)


def per_device(
    tokens,
    cotangent,
    size_tags,
    time_index,
    class_index,
    time_table,
    class_table,
    w_mod,
    w_qkv,
    conv_qkv,
    w_out,
    w_up,
    conv_ffn,
    w_down,
):
    tp_count = lax.axis_size("tp")
    dp_count = lax.axis_size("dp")
    tp_rank = lax.axis_index("tp")
    dp_rank = lax.axis_index("dp")
    tag = size_tags[0]
    heads = w_out.shape[0] // HEAD_SIZE
    perm = parity_matrix()
    share = D // dp_count
    fold = 8

    def slice_rows(weight):
        size = weight.shape[0] // dp_count
        return lax.dynamic_slice_in_dim(weight, dp_rank * size, size, 0)

    def eight(stacked):
        if dp_count == fold:
            return stacked
        rows, width = stacked.shape[2:]
        inner = stacked.reshape(fold, dp_count // fold, tp_count, rows, width)
        return inner.transpose(0, 2, 1, 3, 4).reshape(fold, tp_count, rows * dp_count // fold, width)

    def gather_all(rows):
        stacked = lax.all_gather(rows, ("dp", "tp"), axis=0)
        return stacked.reshape((dp_count, tp_count) + rows.shape)

    packed = jnp.concatenate([slice_rows(w_up), slice_rows(w_down), slice_rows(w_out)], axis=0)
    packed = gather_all(packed)
    w_rows = jnp.concatenate([eight(packed[:, :, 0:share]), eight(packed[:, :, share : 2 * share])], axis=2)
    if dp_count == fold:
        w_rows = packed
    else:
        w_rows = jnp.concatenate([w_rows, jnp.zeros((fold, tp_count, 24, D), BF16)], axis=2)
    w_out_all = packed[:, :, 2 * share :].transpose(1, 0, 2, 3).reshape(tp_count, D // tp_count, D)
    w_qkv_all = eight(gather_all(slice_rows(w_qkv)))
    turn = [[(i, (i + s) % tp_count) for i in range(tp_count)] for s in range(tp_count)]
    w_mod_mine = slice_rows(w_mod)
    w_mod_slots = [w_mod_mine] + [lax.ppermute(w_mod_mine, "tp", turn[s]) for s in range(1, tp_count)]

    time_rows = jnp.take(time_table, time_index, axis=0).astype(F32)
    class_rows = jnp.take(class_table, class_index, axis=0).astype(F32)
    condition_all = time_rows + class_rows
    activated_all = jax.nn.silu(condition_all).astype(BF16)
    activated = lax.dynamic_slice_in_dim(activated_all, dp_rank * SLOTS, SLOTS, 0)
    mod_part = jnp.dot(activated, w_mod, preferred_element_type=F32)
    small = jnp.concatenate([mod_part.reshape(-1), conv_ffn.astype(F32).reshape(-1)])
    small = lax.all_gather(small.reshape(-1, 128), "tp", axis=0).reshape(tp_count, -1)
    modulation = small[:, : mod_part.size].reshape(tp_count, SLOTS, -1).transpose(1, 0, 2).reshape(SLOTS, 6 * D)
    conv_ffn_all = small[:, mod_part.size :].reshape(tp_count, 9, -1)
    per_quad = jnp.where(tag == 1, jnp.broadcast_to(modulation[0:1], modulation.shape), modulation)
    quads = per_quad.reshape(2, 2, 6 * D)
    quad_row = tp_rank * QROWS // (SIDE // 2)
    mods = lax.dynamic_index_in_dim(quads, quad_row, 0, keepdims=False)

    tag_word = size_tags.astype(jnp.int32)
    taps_qkv = conv_qkv.astype(F32)
    hidden_one, projected, mixed_qkv = first_stage(
        tag_word, tokens, quads[..., 0:D], quads[..., D : 2 * D], w_qkv, taps_qkv, perm
    )
    mixed_qkv = mixed_qkv.reshape(32, 2, 2, 32, 192 * heads)

    def exchange(slots):
        return [slots[0]] + [lax.ppermute(slots[s], "tp", turn[s]) for s in range(1, tp_count)]

    heads_out, lse, heads_in = [], [], []
    for head in range(heads):
        out, sums = attend_stage(tag_word, mixed_qkv, head)
        heads_out.append(out)
        lse.append(sums)
        wide = jnp.pad(out.reshape(SIDE, 32, 128), ((HALO, HALO), (0, 0), (0, 0)))
        places = [lax.rem(tp_rank + s, tp_count) * QROWS for s in range(tp_count)]
        heads_in += exchange([lax.dynamic_slice_in_dim(wide, p, XTOK // SIDE, 0) for p in places])
    pad = ((HALO * SIDE, HALO * SIDE), (0, 0))
    tok_wide = lax.dynamic_slice_in_dim(jnp.pad(tokens, pad), tp_rank * QTOK, XTOK, 0)
    cot_wide = lax.dynamic_slice_in_dim(jnp.pad(cotangent, pad), tp_rank * QTOK, XTOK, 0)
    info = jnp.stack([tag, tp_rank]).astype(jnp.int32)
    mixed_q, up, slope, act, after, att, hidden_two, heads_rows, sums_gate = feed_stage(
        info, heads_in, w_out_all, tok_wide, cot_wide, mods, w_rows, conv_ffn_all, perm
    )
    mixed = lax.all_gather(mixed_q, "tp", axis=0, tiled=True)
    g_cat, *gheads, g_after, sums_two = feed_back_stage(
        info, up, slope, act, w_rows, conv_ffn_all, cot_wide, hidden_two, after, att, heads_rows, w_out_all, mods, perm
    )
    tok_mine = lax.dynamic_slice_in_dim(tokens, tp_rank * QTOK, QTOK, 0)
    grad_tokens, grad_w, grad_taps, sums_one = back_stage(
        tag_word,
        mixed_qkv,
        heads_out,
        lse,
        projected,
        taps_qkv,
        mods,
        perm,
        gheads,
        hidden_one,
        w_qkv_all,
        tok_mine,
        g_after,
    )

    def regroup(values):
        rows, width = values.shape[-2:]
        if dp_count == fold:
            return values
        inner = values.reshape(fold, -1, dp_count // fold, rows * fold // dp_count, width)
        return inner.transpose(0, 2, 1, 3, 4).reshape(dp_count, -1, rows * fold // dp_count, width)

    def scatter(values, axis, dim=0):
        return lax.psum_scatter(values, axis, scatter_dimension=dim, tiled=True)

    def out_rows(values):
        return values.reshape(values.shape[0], tp_count, -1)[:, np.array([0, 3, 2, 1])].transpose(1, 2, 0)

    def sum_slots(slots):
        return sum(part.astype(F32) for part in exchange(slots))

    width = w_qkv.shape[1]
    w_cols = grad_w.reshape(width, D).T.reshape(dp_count, share, width)
    taps_rows = grad_taps.transpose(1, 0, 2).reshape(9, dp_count, width // dp_count).transpose(1, 0, 2)
    if dp_count == fold:
        mine = scatter(g_cat, "dp")[0]
        rows_out = out_rows(mine[tp_count, 0:share]).reshape(tp_count, -1, D)
        slots = []
        for s in range(tp_count):
            part = lax.dynamic_index_in_dim(mine, lax.rem(tp_rank + s, tp_count), 0, keepdims=False)
            slots.append(jnp.concatenate([part, rows_out[s]], axis=0))
        mine = sum_slots(slots)
        summed_up, summed_down = mine[0:share], mine[share : 2 * share].T
        summed_conv_ffn = mine[2 * share : 2 * share + 9, 0:share]
        summed_out = mine[2 * share + 16 :].reshape(-1, share)
        taps_rows = jnp.pad(taps_rows, ((0, 0), (0, 7), (0, width - taps_rows.shape[2])))
        both = jnp.concatenate([w_cols, taps_rows], axis=1)
        mine = jnp.sum(lax.all_to_all(both, "dp", split_axis=0, concat_axis=0, tiled=True), axis=0)
        summed_qkv, summed_conv_qkv = mine[0:share], mine[share : share + 9, 0 : width // dp_count]
    else:
        per = D // fold
        body = g_cat[:, 0:tp_count]
        summed_up = scatter(scatter(regroup(body[:, :, 0:per]), "dp")[0], "tp")[0].astype(F32)
        summed_down = scatter(scatter(regroup(body[:, :, per : 2 * per]), "dp")[0], "tp")[0].astype(F32).T
        taps_part = body[:, :, 2 * per : 2 * per + 9, 0:per].transpose(1, 2, 0, 3).reshape(tp_count, 9, D)
        taps_part = scatter(taps_part.astype(F32), "tp")[0]
        summed_conv_ffn = scatter(taps_part, "dp", 1)
        g_out = scatter(regroup(g_cat[:, tp_count:, 0:per]), "dp")[0, 0]
        rows_out = out_rows(g_out)
        summed_out = sum_slots([rows_out[s] for s in range(tp_count)])
        summed_qkv = scatter(w_cols, "dp")[0]
        summed_conv_qkv = scatter(taps_rows, "dp")[0]

    quad_rows = jnp.concatenate(
        [sums_one[0], sums_one[1], sums_two[0], sums_two[1], sums_two[2], sums_gate], axis=-1
    )
    by_rank = lax.all_gather(quad_rows, "tp", axis=0)
    grad_quads = jnp.sum(by_rank.reshape(2, tp_count // 2, 2, 6 * D), axis=1).reshape(4, 6 * D)
    merged = jnp.concatenate(
        [jnp.sum(grad_quads, axis=0, keepdims=True), jnp.zeros((SLOTS - 1, 6 * D), F32)], axis=0
    )
    grad_slots = jnp.where(tag == 1, merged, grad_quads)
    mod_all = lax.all_gather(grad_slots, "dp", axis=0, tiled=True)
    my_act = lax.dynamic_slice_in_dim(activated_all, dp_rank * share, share, 1).astype(F32)
    my_cond = lax.dynamic_slice_in_dim(condition_all, dp_rank * share, share, 1)
    mod_cols = lax.dynamic_slice_in_dim(mod_all, tp_rank * w_mod.shape[1], w_mod.shape[1], 1)
    summed_mod = jnp.dot(my_act.T, mod_cols, precision=lax.Precision.HIGHEST)
    by_group = mod_all.reshape(mod_all.shape[0], tp_count, -1)
    grad_act = jnp.zeros((mod_all.shape[0], share), F32)
    for s in range(tp_count):
        cols = lax.dynamic_index_in_dim(by_group, lax.rem(tp_rank - s + tp_count, tp_count), 1, keepdims=False)
        grad_act += jnp.dot(cols, w_mod_slots[s].astype(F32).T, precision=lax.Precision.HIGHEST)
    _, silu_pull = jax.vjp(jax.nn.silu, my_cond)
    grad_cols = silu_pull(grad_act)[0]
    time_iota = lax.broadcasted_iota(jnp.int32, (time_index.shape[0], time_table.shape[0]), 1)
    time_hits = (time_index[:, None] == time_iota).astype(F32)
    grad_time = jnp.dot(time_hits.T, grad_cols, precision=lax.Precision.HIGHEST)
    class_iota = lax.broadcasted_iota(jnp.int32, (class_index.shape[0], class_table.shape[0]), 1)
    class_hits = (class_index[:, None] == class_iota).astype(F32)
    grad_class = jnp.dot(class_hits.T, grad_cols, precision=lax.Precision.HIGHEST)
    return (
        mixed,
        grad_tokens,
        grad_time,
        grad_class,
        summed_mod,
        summed_qkv,
        summed_conv_qkv,
        summed_out,
        summed_up,
        summed_conv_ffn,
        summed_down,
    )


def solution(mesh):
    in_specs = (
        P("dp", None),
        P("dp", None),
        P("dp"),
        P(),
        P(),
        P(),
        P(),
        P(None, "tp"),
        P(None, "tp"),
        P(None, "tp"),
        P("tp", None),
        P(None, "tp"),
        P(None, "tp"),
        P("tp", None),
    )
    out_specs = (
        P("dp", None),
        P(("dp", "tp"), None),
        P(None, "dp"),
        P(None, "dp"),
        P("dp", "tp"),
        P("dp", "tp"),
        P(None, ("tp", "dp")),
        P("tp", "dp"),
        P("dp", "tp"),
        P(None, ("tp", "dp")),
        P("tp", "dp"),
    )
    return jax.shard_map(
        per_device, mesh=mesh, in_specs=in_specs, out_specs=out_specs, check_vma=False
    )
```

```python
from functools import partial

import jax
import jax.numpy as jnp
import numpy as np
from jax import lax
from jax.experimental import pallas as pl
from jax.experimental.pallas import tpu as pltpu
from jax.sharding import PartitionSpec as P

D = 768
HEAD_SIZE = 64
SIDE = 64
SLOTS = 4
TOK = SIDE * SIDE
HALO = 2
QROWS = 16
QTOK = QROWS * SIDE
XTOK = (QROWS + 2 * HALO) * SIDE
F32 = jnp.float32
BF16 = jnp.bfloat16
VMEM_MAX = 66_000_000
MESH = pl.DeviceIdType.MESH
HEADS_DEV = 3
GROUPS = 4
HIGHEST = lax.Precision.HIGHEST


def dot_nn(a, b):
    return lax.dot_general(a, b, (((1,), (0,)), ((), ())), preferred_element_type=F32)


def dot_nt(a, b):
    return lax.dot_general(a, b, (((1,), (1,)), ((), ())), preferred_element_type=F32)


def dot_tn(a, b):
    return lax.dot_general(a, b, (((0,), (0,)), ((), ())), preferred_element_type=F32)


def parity_matrix():
    one = np.zeros((SIDE, SIDE), np.float32)
    for parity in range(2):
        for j in range(SIDE // 2):
            one[parity * 32 + j, 2 * j + parity] = 1.0
    return jnp.asarray(np.kron(np.eye(4, dtype=np.float32), one), BF16)


def normalised(values):
    mean = jnp.mean(values, axis=-1, keepdims=True)
    centred = values - mean
    variance = jnp.mean(centred * centred, axis=-1, keepdims=True)
    rstd = lax.rsqrt(variance + 1e-06)
    return centred * rstd, rstd


def by_half(values, part):
    rows = values.shape[0]
    shaped = values.reshape(rows // 32, 2, 16, values.shape[-1])
    return (shaped * part[None, :, None, :]).reshape(values.shape)


def spread(part, rows):
    width = part.shape[-1]
    full = jnp.broadcast_to(part[None, :, None, :], (rows // 32, 2, 16, width))
    return full.reshape(rows, width)


def half_sums(values):
    return jnp.sum(values.reshape(values.shape[0] // 32, 2, 16, values.shape[-1]), axis=0)


def column_masks(tag, width):
    j = lax.broadcasted_iota(jnp.int32, (32, width), 0)
    split = tag == 0
    left = jnp.where((j == 0) | ((j == 16) & split), 0.0, 1.0)
    right = jnp.where((j == 31) | ((j == 15) & split), 0.0, 1.0)
    return left, right


def row_scales(tag, row):
    inside = (row >= 0) & (row < SIDE)
    down = jnp.where(inside & jnp.logical_not((tag == 0) & (row == 31)), 1.0, 0.0)
    up = jnp.where(inside & jnp.logical_not((tag == 0) & (row == 32)), 1.0, 0.0)
    return down, up


def conv_step(even, odd, masks, taps, down, up, carry):
    left, right = masks
    odd_left = pltpu.roll(odd, 1, 0) * left
    even_right = pltpu.roll(even, 31, 0) * right
    before_e, before_o, here_e, here_o = carry

    def terms(k):
        return (
            k[0] * odd_left + k[1] * even + k[2] * odd,
            k[0] * even + k[1] * odd + k[2] * even_right,
        )

    last = [t * up for t in taps[6:9]]
    middle = taps[3:6]
    first = [t * down for t in taps[0:3]]
    last_e, last_o = terms(last)
    mid_e, mid_o = terms(middle)
    first_e, first_o = terms(first)
    done = (before_e + last_e, before_o + last_o)
    return done, (here_e + mid_e, here_o + mid_o, first_e, first_o), (odd_left, even_right)


def no_carry(width):
    zero = jnp.zeros((32, width), F32)
    return (zero, zero, zero, zero)


def first_kernel(tag_ref, tok_ref, shift_ref, scale_ref, w_ref, taps_ref, perm_ref, hid_ref, proj_ref, mix_ref, field):
    step = pl.program_id(0)
    tag = tag_ref[0]
    width = w_ref.shape[1]

    @pl.when(step == 0)
    def _():
        field[pl.ds(0, SIDE), :] = jnp.zeros((SIDE, width), F32)
        field[pl.ds((SIDE + 1) * SIDE, SIDE), :] = jnp.zeros((SIDE, width), F32)

    @pl.when(step < 4)
    def _():
        half = step // 2
        shift = shift_ref[half]
        scale = 1.0 + scale_ref[half]

        def chunk(i, carry):
            rows = pl.ds(pl.multiple_of(i * 256, 256), 256)
            ordered = dot_nn(perm_ref[...], tok_ref[rows, :])
            unit, _ = normalised(ordered)
            hidden = (by_half(unit, scale) + spread(shift, 256)).astype(BF16)
            hid_ref[rows, :] = hidden
            out = dot_nn(hidden, w_ref[...])
            for head in range(proj_ref.shape[0]):
                proj_ref[head, rows, :] = out[:, head * 192 : head * 192 + 192]
            field[pl.ds(pl.multiple_of((step * 16 + 1) * SIDE + i * 256, 64), 256), :] = out
            return carry

        lax.fori_loop(0, 4, chunk, 0)

    @pl.when(step > 0)
    def _():
        base = (step - 1) * 16 - 1
        for lane in range(0, width, 128):
            size = min(128, width - lane)
            lanes = slice(lane, lane + size)
            masks = column_masks(tag, size)
            taps = [taps_ref[t : t + 1, lanes] for t in range(9)]

            def one(n, carry):
                row = base + n
                start = pl.multiple_of((row + 1) * SIDE, SIDE)
                even = field[pl.ds(start, 32), lanes]
                odd = field[pl.ds(start + 32, 32), lanes]
                down, up = row_scales(tag, row)
                done, carry, _ = conv_step(even, odd, masks, taps, down, up, carry)
                return done, carry

            def loop(n, carry):
                done, carry = one(n, carry)
                start = pl.multiple_of((n - 2) * SIDE, SIDE)
                for k in range(2):
                    out = done[k].astype(BF16)
                    mix_ref[pl.ds(start + 32 * k, 32), lanes] = out
                return carry

            _, carry = one(0, no_carry(size))
            _, carry = one(1, carry)
            lax.fori_loop(2, 18, loop, carry)


def first_stage(tag, tokens, shift, scale, w_qkv, taps, perm):
    width = w_qkv.shape[1]
    heads = width // 192
    whole = lambda shape: pl.BlockSpec(shape, lambda s: (0,) * len(shape))
    ahead = lambda w: pl.BlockSpec((1024, w), lambda s: (jnp.minimum(s, 3), 0))
    return pl.pallas_call(
        first_kernel,
        grid=(5,),
        in_specs=[
            pl.BlockSpec(memory_space=pltpu.SMEM),
            ahead(D),
            whole((2, 2, D)),
            whole((2, 2, D)),
            whole((D, width)),
            whole((9, width)),
            whole((256, 256)),
        ],
        out_specs=[
            ahead(D),
            pl.BlockSpec((heads, 1024, 192), lambda s: (0, jnp.minimum(s, 3), 0)),
            pl.BlockSpec((1024, width), lambda s: (jnp.maximum(s - 1, 0), 0)),
        ],
        out_shape=[
            jax.ShapeDtypeStruct((TOK, D), BF16),
            jax.ShapeDtypeStruct((heads, TOK, 192), F32),
            jax.ShapeDtypeStruct((TOK, width), BF16),
        ],
        scratch_shapes=[pltpu.VMEM(((SIDE + 2) * SIDE, width), F32)],
        compiler_params=pltpu.CompilerParams(vmem_limit_bytes=VMEM_MAX),
        name="first_stage",
    )(tag, tokens, shift, scale, w_qkv, taps, perm)


def to_row(column, count):
    return jnp.transpose(jnp.broadcast_to(column, (count, 128)))[0:1, :]


def attend_kernel(tag_ref, x_ref, o_ref, lse_ref, *, base):
    tag = tag_ref[0]
    parity = pl.program_id(0) % 2

    def run(split):
        def chunk(c, carry):
            query = x_ref[pl.ds(c * 8, 8), 0, 0, :, base : base + 64].reshape(256, 64)
            query = query * jnp.asarray(0.125, BF16)
            if split:
                rows = pl.ds((c // 2) * 16, 16)
                count = 512
            else:
                rows = pl.ds(0, 32)
                count = 1024
            keys = x_ref[rows, 0, 0, :, base + 64 : base + 128].reshape(count, 64)
            values = x_ref[rows, 0, 0, :, base + 128 : base + 192].reshape(count, 64)
            scores = dot_nt(query, keys)
            if split:
                qj = lax.broadcasted_iota(jnp.int32, (256, count), 0) & 16
                kj = lax.broadcasted_iota(jnp.int32, (256, count), 1) & 16
                scores = jnp.where(qj == kj, scores, -1e30)
            top = jnp.max(scores, axis=-1, keepdims=True)
            expo = jnp.exp(scores - top)
            total = jnp.sum(expo, axis=-1, keepdims=True)
            out = dot_nn(expo.astype(BF16), values) / total
            out = out.astype(BF16).reshape(8, 32, 64)
            for b in range(2):

                @pl.when(parity == b)
                def _():
                    o_ref[pl.ds(c * 8, 8), 0, :, b * 64 : b * 64 + 64] = out

            lse_ref[0, 0:1, pl.ds(pl.multiple_of(c * 256, 256), 256)] = to_row(top + jnp.log(total), 256)
            return carry

        lax.fori_loop(0, 4, chunk, 0)

    pl.when(tag == 1)(lambda: run(False))
    pl.when(tag != 1)(lambda: run(True))


def group_block(width):
    at = lambda g: jnp.minimum(g, 3)
    return pl.BlockSpec((32, 1, 1, 32, width), lambda g: (0, at(g) // 2, at(g) % 2, 0, 0))


def pair_block():
    return pl.BlockSpec((32, 1, 32, 128), lambda g: (0, jnp.minimum(g, 3) // 2, 0, 0))


def lse_block():
    return pl.BlockSpec((1, 8, 1024), lambda g: (jnp.minimum(g, 3), 0, 0))


def attend_stage(tag, mixed_qkv, head):
    out, lse = pl.pallas_call(
        partial(attend_kernel, base=head * 192),
        grid=(4,),
        in_specs=[pl.BlockSpec(memory_space=pltpu.SMEM), group_block(mixed_qkv.shape[-1])],
        out_specs=[pair_block(), lse_block()],
        out_shape=[
            jax.ShapeDtypeStruct((32, 2, 32, 128), BF16),
            jax.ShapeDtypeStruct((4, 8, 1024), F32),
        ],
        compiler_params=pltpu.CompilerParams(vmem_limit_bytes=VMEM_MAX),
        cost_estimate=pl.CostEstimate(flops=2_000_000_000, transcendentals=4_000_000, bytes_accessed=4_000_000),
        name="attend_stage",
    )(tag, mixed_qkv)
    return out, lse


def kernel_sums(acc, even, odd, odd_left, even_right, plain, scale, first):
    plain_e, plain_o = plain

    def fold(values):
        return jnp.sum(values.reshape(4, 8, values.shape[-1]), axis=0)

    terms = [
        fold(odd * plain_e) + fold(even_right * plain_o),
        fold(even * plain_e) + fold(odd * plain_o),
        fold(odd_left * plain_e) + fold(even * plain_o),
    ]
    out = list(acc)
    for t in range(3):
        term = terms[t] if scale is None else terms[t] * scale
        out[first + t] = acc[first + t] + term
    return out


POLY = (
    0.13241715506535054,
    0.12108811680396304,
    0.17555028579228482,
    -0.0796444980816301,
    0.3217932733518851,
    -0.21571441684424994,
    0.04451008654080756,
)


def gelu_parts(z):
    size = jnp.abs(z)
    t = 1.0 / (1.0 + 0.33 * size)
    expo = jnp.exp(z * z * -0.5)
    poly = POLY[6]
    for c in POLY[5::-1]:
        poly = poly * t + c
    tail = poly * t * expo
    cdf = jnp.where(z >= 0.0, 1.0 - tail, tail)
    value = z * cdf
    slope = cdf + z * (expo * 0.3989422804014327)
    return value, slope


def mod_part(mods_ref, i):
    return mods_ref[:, i * D : (i + 1) * D]


def feed_kernel(
    info_ref,
    *refs,
):
    heads_refs, refs = refs[0:12], refs[12:]
    feed_body(info_ref, heads_refs, *refs)


def feed_body(
    info_ref,
    heads_refs,
    w_out_ref,
    tok_ref,
    cot_ref,
    mods_ref,
    w_up_ref,
    w_down_ref,
    taps_ref,
    perm_ref,
    mixed_ref,
    up_ref,
    slope_ref,
    act_ref,
    after_ref,
    att_ref,
    hidden_out,
    heads_out,
    sums_ref,
    hidden_ref,
    hcat_ref,
    feed_ref,
    sum_ref,
):
    step = pl.program_id(0)
    tag = info_ref[0]
    first_row = info_ref[1] * QROWS - HALO
    chans = up_ref.shape[2]
    groups = w_out_ref.shape[0]
    heads = len(heads_refs) // groups
    rank = info_ref[1]

    @pl.when(step == 0)
    def _():
        gate_one, shift_two, scale_two = mod_part(mods_ref, 2), mod_part(mods_ref, 3), 1.0 + mod_part(mods_ref, 4)

        def unpack(i, carry):
            for g in range(groups):
                for head in range(heads):
                    ref = heads_refs[head * groups + g]
                    for b in range(2):
                        rows = pl.ds(pl.multiple_of(i * SIDE + b * 32, 32), 32)
                        lane = (g * heads + head) * 64
                        hcat_ref[rows, lane : lane + 64] = ref[i, :, b * 64 : b * 64 + 64]
            return carry

        lax.fori_loop(0, XTOK // SIDE, unpack, 0)

        def part(start, size):
            rows = pl.ds(start, size)
            perm = perm_ref[0:size, 0:size]
            ordered = dot_nn(perm, tok_ref[rows, :])
            attention = jnp.zeros((size, D), F32)
            width = heads * HEAD_SIZE
            for g in range(groups):
                source = lax.rem(rank - g + groups, groups)
                term = dot_nn(hcat_ref[rows, g * width : g * width + width], w_out_ref[source])
                attention = attention + term.astype(BF16).astype(F32)
            after = ordered + by_half(attention, gate_one)
            unit, _ = normalised(after)
            hidden = (by_half(unit, scale_two) + spread(shift_two, size)).astype(BF16)
            hidden_ref[rows, :] = hidden
            if size == 256:
                mine = pl.ds(pl.multiple_of(start - 128, 256), 256)
                att_ref[mine, :] = attention.astype(BF16)
                after_ref[mine, :] = after
                hidden_out[mine, :] = hidden
                heads_out[mine, :] = hcat_ref[rows, :]

        part(0, 128)
        part(XTOK - 128, 128)

        def loop(i, carry):
            part(pl.multiple_of(128 + i * 256, 128), 256)
            return carry

        lax.fori_loop(0, 4, loop, 0)
        feed_ref[...] = jnp.zeros_like(feed_ref)

    w_up = w_up_ref[...].reshape(D, chans)
    w_down = w_down_ref[...].reshape(chans, D)

    def up_loop(i, carry):
        rows = pl.ds(pl.multiple_of(i * 640, 128), 640)
        up_ref[0, rows, :] = dot_nn(hidden_ref[rows, :], w_up)
        return carry

    lax.fori_loop(0, 2, up_loop, 0)

    for lane in range(0, chans, 128):
        lanes = slice(lane, lane + 128)
        masks = column_masks(tag, 128)
        taps = [taps_ref[0, t : t + 1, lanes] for t in range(9)]

        def one(n, carry):
            start = pl.multiple_of(n * SIDE, SIDE)
            even = up_ref[0, pl.ds(start, 32), lanes]
            odd = up_ref[0, pl.ds(start + 32, 32), lanes]
            down, up = row_scales(tag, first_row + n)
            done, carry, _ = conv_step(even, odd, masks, taps, down, up, carry)
            return done, carry

        def loop(n, carry):
            done, carry = one(n, carry)
            for k in range(2):
                start = pl.multiple_of((n - 2) * SIDE + 32 * k, 32)
                value, slope = gelu_parts(done[k])
                act_ref[0, pl.ds(start, 32), lanes] = value.astype(BF16)
                slope_ref[0, pl.ds(start, 32), lanes] = slope
            return carry

        _, carry = one(0, no_carry(128))
        _, carry = one(1, carry)
        lax.fori_loop(2, QROWS + 2 * HALO, loop, carry)

    def token_loop(i, carry):
        rows = pl.ds(pl.multiple_of(i * 512, 512), 512)
        feed_ref[rows, :] += dot_nn(act_ref[0, pl.ds(pl.multiple_of(64 + i * 512, 64), 512), :], w_down)
        return carry

    lax.fori_loop(0, 2, token_loop, 0)

    @pl.when(step == pl.num_programs(0) - 1)
    def _():
        gate_two = mod_part(mods_ref, 5)
        sum_ref[...] = jnp.zeros_like(sum_ref)

        def loop(i, carry):
            rows = pl.ds(pl.multiple_of(i * 256, 256), 256)
            wide = pl.ds(pl.multiple_of(128 + i * 256, 128), 256)
            feed = feed_ref[rows, :]
            result = (after_ref[rows, :] + by_half(feed, gate_two)).astype(BF16)
            mixed_ref[rows, :] = dot_tn(perm_ref[...], result).astype(BF16)
            sum_ref[...] += half_sums(dot_nn(perm_ref[...], cot_ref[wide, :]) * feed)
            return carry

        lax.fori_loop(0, 4, loop, 0)
        sums_ref[...] = jnp.sum(sum_ref[...], axis=1)


def feed_stage(info, heads, w_out, tok, cot, mods, w_rows, taps, perm):
    dps, chunks, tall, chans = w_rows.shape
    per = D // dps
    once = pl.Buffered(1)
    whole = lambda shape: pl.BlockSpec(shape, lambda s: (0,) * len(shape), pipeline_mode=once)
    chunk = lambda rows: pl.BlockSpec((1, rows, chans), lambda s: (s, 0, 0))
    return pl.pallas_call(
        feed_kernel,
        grid=(chunks,),
        in_specs=[
            pl.BlockSpec(memory_space=pltpu.SMEM),
            *[whole(h.shape) for h in heads],
            whole(w_out.shape),
            whole((XTOK, D)),
            whole((XTOK, D)),
            whole((2, 6 * D)),
            pl.BlockSpec((dps, 1, per, chans), lambda s: (0, s, 0, 0)),
            pl.BlockSpec((dps, 1, per, chans), lambda s: (0, s, 1, 0)),
            chunk(9),
            whole((256, 256)),
        ],
        out_specs=[
            whole((QTOK, D)),
            chunk(XTOK),
            chunk(XTOK - 128),
            chunk(XTOK - 128),
            whole((QTOK, D)),
            whole((QTOK, D)),
            whole((QTOK, D)),
            whole((QTOK, D)),
            whole((2, D)),
        ],
        out_shape=[
            jax.ShapeDtypeStruct((QTOK, D), BF16),
            jax.ShapeDtypeStruct((chunks, XTOK, chans), F32),
            jax.ShapeDtypeStruct((chunks, XTOK - 128, chans), F32),
            jax.ShapeDtypeStruct((chunks, XTOK - 128, chans), BF16),
            jax.ShapeDtypeStruct((QTOK, D), F32),
            jax.ShapeDtypeStruct((QTOK, D), BF16),
            jax.ShapeDtypeStruct((QTOK, D), BF16),
            jax.ShapeDtypeStruct((QTOK, D), BF16),
            jax.ShapeDtypeStruct((2, D), F32),
        ],
        scratch_shapes=[
            pltpu.VMEM((XTOK, D), BF16),
            pltpu.VMEM((XTOK, D), BF16),
            pltpu.VMEM((QTOK, D), F32),
            pltpu.VMEM((2, 16, D), F32),
        ],
        compiler_params=pltpu.CompilerParams(vmem_limit_bytes=VMEM_MAX),
        cost_estimate=pl.CostEstimate(flops=20_000_000_000, transcendentals=8_000_000, bytes_accessed=80_000_000),
        name="feed_stage",
    )(info, *heads, w_out, tok, cot, mods, w_rows, w_rows, taps, perm)


def greet(axis, count):
    barrier = pltpu.get_barrier_semaphore()
    me = lax.axis_index(axis)

    def one(i, carry):
        pl.semaphore_signal(barrier, inc=1, device_id={axis: lax.rem(me + i, count)}, device_id_type=MESH)
        return carry

    lax.fori_loop(1, count, one, 0)
    return barrier


def pass_on(direction, stage, half, source, target, send, recv):
    rank = lax.axis_index("tp")
    quarter = rank - (stage - 1) * direction
    rows = pl.ds(pl.multiple_of(quarter * QTOK + half * 512, 512), 512)
    mine = pl.ds(half * 512, 512)
    at = (0 if direction > 0 else 1, half)
    return pltpu.make_async_remote_copy(
        source.at[mine] if stage == 1 else target.at[rows],
        target.at[rows],
        send.at[at],
        recv.at[at],
        device_id={"tp": rank + direction},
        device_id_type=MESH,
    )


def sends(direction, stage):
    rank = lax.axis_index("tp")
    quarter = rank - (stage - 1) * direction
    return (rank + direction >= 0) & (rank + direction < 4) & (quarter >= 0) & (quarter < 4)


def receives(direction, stage):
    quarter = lax.axis_index("tp") - stage * direction
    return (quarter >= 0) & (quarter < 4)


def stage_start(stage, half, source, target, send, recv):
    for direction in (1, -1):

        @pl.when(sends(direction, stage))
        def _():
            pass_on(direction, stage, half, source, target, send, recv).start()


def stage_wait(stage, half, source, target, send, recv, sent=True, received=True):
    for direction in (1, -1):
        if sent:

            @pl.when(sends(direction, stage))
            def _():
                pass_on(direction, stage, half, source, target, send, recv).wait_send()

        if received:

            @pl.when(receives(direction, stage))
            def _():
                rank = lax.axis_index("tp")
                quarter = rank - stage * direction
                rows = pl.ds(pl.multiple_of(quarter * QTOK + half * 512, 512), 512)
                at = (0 if direction > 0 else 1, half)
                pltpu.make_async_remote_copy(
                    target.at[rows],
                    target.at[rows],
                    send.at[at],
                    recv.at[at],
                    device_id={"tp": rank - direction},
                    device_id_type=MESH,
                ).wait_recv()


def feed_back_kernel(
    tag_ref,
    mixed_hbm,
    up_ref,
    slope_ref,
    act_ref,
    w_up_ref,
    w_down_ref,
    taps_ref,
    cot_ref,
    hidden_ref,
    after_ref,
    att_ref,
    heads_ref,
    w_out_ref,
    mods_ref,
    perm_ref,
    mixed_all,
    gcat_ref,
    g0_ref,
    g1_ref,
    g2_ref,
    gafter_ref,
    sums_ref,
    hidden_t,
    gfeed_ref,
    gfeed_t,
    ghid_ref,
    gact_ref,
    gup_ref,
    sum_ref,
    gtaps_ref,
    own_sem,
    one_send,
    one_recv,
    two_send,
    two_recv,
):
    step = pl.program_id(0)
    tag = tag_ref[0]
    rank = lax.axis_index("tp")
    first_row = rank * QROWS - HALO
    one_args = (mixed_hbm, mixed_all, one_send, one_recv)
    two_args = (mixed_hbm, mixed_all, two_send, two_recv)
    mine = pl.ds(pl.multiple_of(rank * QTOK, QTOK), QTOK)

    @pl.when(step == 0)
    def _():
        pl.semaphore_wait(greet("tp", 4), 3)
        for half in range(2):
            stage_start(1, half, *one_args)
        pltpu.make_async_copy(mixed_hbm, gup_ref, own_sem.at[0]).start()

    @pl.when(step == 2)
    def _():
        stage_wait(1, 0, *one_args, sent=False)
        stage_start(2, 0, *two_args)

    @pl.when(step == 3)
    def _():
        stage_wait(1, 1, *one_args, sent=False)
        stage_start(2, 1, *two_args)

    chans = up_ref.shape[2]
    dps, per = w_up_ref.shape[0], w_up_ref.shape[2]

    @pl.when(step == 0)
    def _():
        gate_two = mod_part(mods_ref, 5)

        def part(start, size):
            rows = pl.ds(start, size)
            perm = perm_ref[0:size, 0:size]
            gfeed_ref[rows, :] = by_half(dot_nn(perm, cot_ref[rows, :]), gate_two).astype(BF16)

        def loop(i, carry):
            part(pl.multiple_of(i * 256, 256), 256)
            return carry

        lax.fori_loop(0, XTOK // 256, loop, 0)
        hidden_t[...] = jnp.transpose(hidden_ref[...])
        gfeed_t[...] = jnp.transpose(gfeed_ref[pl.ds(128, QTOK), :])
        ghid_ref[...] = jnp.zeros_like(ghid_ref)
        pltpu.make_async_copy(mixed_hbm, gup_ref, own_sem.at[0]).wait()
        put = pltpu.make_async_copy(gup_ref, mixed_all.at[mine], own_sem.at[1])
        put.start()
        put.wait()

    @pl.when(step < pl.num_programs(0) - 1)
    def _():
        w_up = w_up_ref[...].reshape(D, chans)
        w_down = w_down_ref[...].reshape(chans, D)

        def gact_loop(i, carry):
            rows = pl.ds(pl.multiple_of(i * 576, 64), 576)
            out = dot_nt(gfeed_ref[pl.ds(pl.multiple_of(64 + i * 576, 64), 576), :], w_down)
            gact_ref[rows, :] = out * slope_ref[0, rows, :]
            return carry

        lax.fori_loop(0, 2, gact_loop, 0)

        for lane in range(0, chans, 128):
            lanes = slice(lane, lane + 128)
            masks = column_masks(tag, 128)
            taps = [taps_ref[0, 8 - t : 9 - t, lanes] for t in range(9)]

            def one(n, carry, sums):
                start = pl.multiple_of(n * SIDE, SIDE)
                low, high = pl.ds(start, 32), pl.ds(start + 32, 32)
                even, odd = gact_ref[low, lanes], gact_ref[high, lanes]
                row = first_row + 1 + n
                down, up = row_scales(tag, row)
                done, carry, shifted = conv_step(even, odd, masks, taps, down, up, carry)
                if sums is not None:
                    above = jnp.where((row == 0) | ((tag == 0) & (row == 32)), 0.0, 1.0)
                    below = jnp.where((row == SIDE - 1) | ((tag == 0) & (row == 31)), 0.0, 1.0)
                    for i, scale in ((0, above), (1, None), (2, below)):
                        at = pl.multiple_of((n + i) * SIDE, SIDE)
                        plain = (up_ref[0, pl.ds(at, 32), lanes], up_ref[0, pl.ds(at + 32, 32), lanes])
                        sums = kernel_sums(sums, even, odd, *shifted, plain, scale, 3 * i)
                return done, carry, sums

            def put(n, done):
                for k in range(2):
                    start = pl.multiple_of((n - 2) * SIDE + 32 * k, 32)
                    gup_ref[pl.ds(start, 32), lanes] = done[k].astype(BF16)

            def loop(n, state):
                done, carry, sums = one(n, state[0], list(state[1]))
                put(n, done)
                return carry, tuple(sums)

            zero = jnp.zeros((8, 128), F32)
            _, carry, _ = one(0, no_carry(128), None)
            _, carry, sums = one(1, carry, [zero] * 9)
            carry, sums = lax.fori_loop(2, QROWS + 1, loop, (carry, tuple(sums)))
            done, carry, _ = one(QROWS + 1, carry, None)
            put(QROWS + 1, done)
            for t in range(9):
                gtaps_ref[t : t + 1, lanes] = jnp.sum(sums[t], axis=0, keepdims=True)

        def token_loop(i, carry):
            rows = pl.ds(pl.multiple_of(i * 512, 512), 512)
            ghid_ref[rows, :] += dot_nt(gup_ref[rows, :], w_up)
            return carry

        lax.fori_loop(0, 2, token_loop, 0)

        def weight_loop(i, carry):
            rows = pl.ds(pl.multiple_of(i * 384, 128), 384)
            blocks = pl.ds(i * (dps // 2), dps // 2)
            out = dot_nn(hidden_t[rows, :], gup_ref[...])
            gcat_ref[blocks, 0, 0:per, :] = out.reshape(dps // 2, per, chans).astype(BF16)
            out = dot_nn(gfeed_t[rows, :], act_ref[0, pl.ds(64, QTOK), :])
            gcat_ref[blocks, 0, per : 2 * per, :] = out.reshape(dps // 2, per, chans).astype(BF16)
            return carry

        lax.fori_loop(0, 2, weight_loop, 0)
        sums = jnp.concatenate([gtaps_ref[0:9, :], jnp.zeros((7, chans), F32)], axis=0)
        for d in range(dps):
            part_sums = jnp.concatenate([sums[:, d * per : d * per + per], jnp.zeros((16, chans - per), F32)], axis=1)
            gcat_ref[d, 0, 2 * per : 2 * per + 16, :] = part_sums.astype(BF16)

    @pl.when(step == pl.num_programs(0) - 1)
    def _():
        gate_one, scale_two = mod_part(mods_ref, 2), 1.0 + mod_part(mods_ref, 4)
        groups = w_out_ref.shape[0]
        sum_ref[...] = jnp.zeros_like(sum_ref)

        def loop(i, carry):
            rows = pl.ds(pl.multiple_of(i * 256, 256), 256)
            wide = pl.ds(pl.multiple_of(128 + i * 256, 128), 256)
            cot = dot_nn(perm_ref[...], cot_ref[wide, :])
            unit, rstd = normalised(after_ref[rows, :])
            grad = ghid_ref[rows, :]
            sum_ref[1] += half_sums(grad)
            sum_ref[2] += half_sums(grad * unit)
            inner = by_half(grad, scale_two)
            mean = jnp.mean(inner, axis=-1, keepdims=True)
            along = jnp.mean(inner * unit, axis=-1, keepdims=True)
            gafter = cot + rstd * (inner - mean - unit * along)
            sum_ref[0] += half_sums(gafter * att_ref[rows, :].astype(F32))
            gafter_ref[rows, :] = gafter
            gatt = by_half(gafter, gate_one).astype(BF16)
            gup_ref[rows, :] = gatt
            for g in range(groups):
                target = lax.rem(rank + g, groups)
                out = dot_nt(gatt, w_out_ref[target]).astype(BF16).reshape(4, 2, 32, w_out_ref.shape[1])
                for head, ref in enumerate((g0_ref, g1_ref, g2_ref)):
                    for b in range(2):
                        ref[g, pl.ds(i * 4, 4), :, b * 64 : b * 64 + 64] = out[:, b, :, head * 64 : head * 64 + 64]
            return carry

        lax.fori_loop(0, 4, loop, 0)
        out = dot_tn(gup_ref[...], heads_ref[...])
        gcat_ref[:, 0, 0:per, :] = out.reshape(dps, per, D).astype(BF16)
        gcat_ref[:, 0, per:, :] = jnp.zeros((dps, per + 16, D), BF16)
        sums_ref[...] = jnp.sum(sum_ref[...], axis=2)
        for half in range(2):
            stage_wait(1, half, *one_args, received=False)
            stage_wait(2, half, *two_args)


def feed_back_stage(tag, mixed_q, up, slope, act, w_rows, taps, cot, hidden, after, att, heads, w_out, mods, perm):
    dps, chunks, tall, chans = w_rows.shape
    groups = w_out.shape[0]
    per = D // dps
    once = pl.Buffered(1)
    whole = lambda shape: pl.BlockSpec(shape, lambda s: (0,) * len(shape), pipeline_mode=once)
    at = lambda s: jnp.minimum(s, chunks - 1)
    chunk = lambda rows: pl.BlockSpec((1, rows, chans), lambda s: (at(s), 0, 0))
    sent = (groups, QROWS, 32, 128)
    return pl.pallas_call(
        feed_back_kernel,
        grid=(chunks + 1,),
        in_specs=[
            pl.BlockSpec(memory_space=pltpu.SMEM),
            pl.BlockSpec(memory_space=pl.ANY),
            chunk(XTOK),
            chunk(XTOK - 128),
            chunk(XTOK - 128),
            pl.BlockSpec((dps, 1, per, chans), lambda s: (0, at(s), 0, 0)),
            pl.BlockSpec((dps, 1, per, chans), lambda s: (0, at(s), 1, 0)),
            chunk(9),
            whole((XTOK, D)),
            whole((QTOK, D)),
            whole((QTOK, D)),
            whole((QTOK, D)),
            whole((QTOK, D)),
            whole(w_out.shape),
            whole((2, 6 * D)),
            whole((256, 256)),
        ],
        out_specs=[
            pl.BlockSpec(memory_space=pl.ANY),
            pl.BlockSpec((dps, 1, 2 * per + 16, chans), lambda s: (0, s, 0, 0)),
            whole(sent),
            whole(sent),
            whole(sent),
            whole((QTOK, D)),
            whole((3, 2, D)),
        ],
        out_shape=[
            jax.ShapeDtypeStruct((TOK, D), BF16),
            jax.ShapeDtypeStruct((dps, chunks + 1, 2 * per + 16, chans), BF16),
            jax.ShapeDtypeStruct(sent, BF16),
            jax.ShapeDtypeStruct(sent, BF16),
            jax.ShapeDtypeStruct(sent, BF16),
            jax.ShapeDtypeStruct((QTOK, D), F32),
            jax.ShapeDtypeStruct((3, 2, D), F32),
        ],
        scratch_shapes=[
            pltpu.VMEM((D, QTOK), BF16),
            pltpu.VMEM((XTOK, D), BF16),
            pltpu.VMEM((D, QTOK), BF16),
            pltpu.VMEM((QTOK, D), F32),
            pltpu.VMEM((XTOK - 128, chans), F32),
            pltpu.VMEM((QTOK, chans), BF16),
            pltpu.VMEM((3, 2, 16, D), F32),
            pltpu.VMEM((16, chans), F32),
            pltpu.SemaphoreType.DMA((2,)),
            *[pltpu.SemaphoreType.DMA((2, 2))] * 4,
        ],
        compiler_params=pltpu.CompilerParams(vmem_limit_bytes=VMEM_MAX, collective_id=1, has_side_effects=True),
        cost_estimate=pl.CostEstimate(flops=30_000_000_000, transcendentals=8_000_000, bytes_accessed=80_000_000),
        name="feed_back_stage",
    )(tag, mixed_q, up, slope, act, w_rows, w_rows, taps, cot, hidden, after, att, heads, w_out, mods, perm)


def back_kernel(
    tag_ref,
    x_ref,
    o0_ref,
    o1_ref,
    o2_ref,
    lse0_ref,
    lse1_ref,
    lse2_ref,
    proj_ref,
    taps_ref,
    gh0_hbm,
    gh1_hbm,
    gh2_hbm,
    hid_hbm,
    mixed_in,
    mixed_all,
    g_all,
    gw_ref,
    gtaps_ref,
    do_buf,
    gsend,
    kv_buf,
    qz_buf,
    zd_buf,
    row_buf,
    taps_buf,
    acc_ref,
    field,
    flat,
    hid_buf,
    gw_buf,
    local_sem,
    own_sem,
    do_send,
    do_recv,
    g_send,
    g_recv,
    m_send,
    m_recv,
):
    step = pl.program_id(0)
    tag = tag_ref[0]
    last_args = (mixed_all, mixed_all, m_send, m_recv)
    split = tag == 0
    rank = lax.axis_index("tp")
    gh_hbm = (gh0_hbm, gh1_hbm, gh2_hbm)

    def do_copy(head, slot):
        peer = lax.rem(rank + slot, 4)
        return pltpu.make_async_remote_copy(
            gh_hbm[head].at[slot],
            do_buf.at[head, slot],
            do_send.at[head, slot],
            do_recv.at[head, slot],
            device_id={"tp": peer},
            device_id_type=MESH,
        )

    def own_copy(head):
        return pltpu.make_async_copy(gh_hbm[head].at[0], do_buf.at[head, 0], own_sem.at[head])

    def g_copy(head, slot):
        peer = lax.rem(rank + slot, 4)
        return pltpu.make_async_remote_copy(
            gsend.at[head, slot],
            g_all.at[head, slot],
            g_send.at[head, slot],
            g_recv.at[head, slot],
            device_id={"tp": peer},
            device_id_type=MESH,
        )

    def keep_copy(head):
        return pltpu.make_async_copy(gsend.at[head, 0], g_all.at[head, 0], local_sem.at[head])

    load = pltpu.make_async_copy(hid_hbm, hid_buf, local_sem.at[HEADS_DEV])

    @pl.when(step == 0)
    def _():
        pl.semaphore_wait(greet("tp", 4), 3)
        for head in range(HEADS_DEV):
            for slot in range(1, 4):
                do_copy(head, slot).start()
            own_copy(head).start()
        load.start()

    @pl.when(step == 1)
    def _():
        for half in range(2):
            stage_start(3, half, *last_args)

    for head, (o_ref, lse_ref) in enumerate(((o0_ref, lse0_ref), (o1_ref, lse1_ref), (o2_ref, lse2_ref))):

        @pl.when(step == head)
        def _():
            base = head * 192
            taps_buf[0:9, :] = taps_ref[:, base : base + 192]
            zero = jnp.zeros((1024, 64), BF16)
            for g in range(GROUPS):
                a, b = g // 2, g % 2
                kv_buf[g] = x_ref[:, a, b, :, base + 64 : base + 192].reshape(1024, 128)
                query = x_ref[:, a, b, :, base : base + 64].reshape(1024, 64) * jnp.asarray(0.125, BF16)
                qz_buf[g] = jnp.concatenate([query, zero], axis=1)
            own_copy(head).wait()
            for slot in range(1, 4):
                do_copy(head, slot).wait_recv()
            for g in range(GROUPS):
                a, b = g // 2, g % 2
                for quarter in range(4):
                    slot = lax.rem(rank - quarter + 4, 4)
                    rows = slice(quarter * 256, quarter * 256 + 256)
                    grad = do_buf[head, slot, :, :, b * 64 : b * 64 + 64].reshape(8, 2, 32, 64)[:, a].reshape(256, 64)
                    zd_buf[g, rows, :] = jnp.concatenate([zero[0:256], grad], axis=1)
                    out = o_ref[quarter * 8 : quarter * 8 + 8, a, :, b * 64 : b * 64 + 64].reshape(256, 64)
                    delta = jnp.sum(grad.astype(F32) * out.astype(F32), axis=-1, keepdims=True)
                    row_buf[g, 0:1, rows] = to_row(delta, 256)
                row_buf[g, 1:2, :] = lse_ref[g, 0:1, :]

    def attend_all():
        def group(g, carry):
            acc_ref[...] = jnp.zeros_like(acc_ref)

            def chunk(c, carry):
                mine = pl.ds(pl.multiple_of(c * 256, 256), 256)
                delta = row_buf[g, 0:1, mine]
                lse = row_buf[g, 1:2, mine]
                place = lax.broadcasted_iota(jnp.int32, (1, 256), 1) & 16
                far = jnp.float32(1e30)
                by_j = [jnp.where(split & (place != 0), far, 0.0), jnp.where(split & (place == 0), far, 0.0)]
                by_i = [jnp.where(split & (c >= 2), far, 0.0), jnp.where(split & (c < 2), far, 0.0)]
                kv = kv_buf[g]
                query, grad = qz_buf[g, mine, :], zd_buf[g, mine, :]
                logits = dot_nt(kv, query).reshape(2, 16, 2, 16, 256)
                probs = [
                    [jnp.exp(logits[i, :, j] - (lse + by_i[i] + by_j[j])[:, None, :]) for j in range(2)] for i in range(2)
                ]
                probs = jnp.stack([jnp.stack(p, axis=1) for p in probs], axis=0).reshape(1024, 256)
                scores = (probs * (dot_nt(kv, grad) - delta)).astype(BF16)
                acc_ref[...] += dot_nn(scores, query) + dot_nn(probs.astype(BF16), grad)
                grad_query = dot_tn(scores, kv)[:, 0:64] * 0.125
                field[pl.ds(c * 8, 8), g // 2, g % 2, :, 0:64] = grad_query.reshape(8, 32, 64)
                return carry

            lax.fori_loop(0, 4, chunk, 0)
            field[:, g // 2, g % 2, :, 64:192] = acc_ref[...].reshape(32, 32, 128)
            return carry

        lax.fori_loop(0, GROUPS, group, 0)
        for start_lane, size in ((0, 128), (128, 64)):
            lanes = slice(start_lane, start_lane + size)
            masks = column_masks(tag, size)
            taps = [taps_buf[8 - t : 9 - t, lanes] for t in range(9)]

            def one(row, carry, sums, has_above, has_below):
                even = field[row // 2, row % 2, 0, :, lanes]
                odd = field[row // 2, row % 2, 1, :, lanes]
                down, up = row_scales(tag, row)
                done, carry, shifted = conv_step(even, odd, masks, taps, down, up, carry)
                for i in range(3):
                    if (i == 0 and not has_above) or (i == 2 and not has_below):
                        continue
                    at = pl.multiple_of((row + i - 1) * SIDE, SIDE)
                    plain = (proj_ref[0, pl.ds(at, 32), lanes], proj_ref[0, pl.ds(at + 32, 32), lanes])
                    scale = (up, None, down)[i]
                    sums = kernel_sums(sums, even, odd, *shifted, plain, scale, 3 * i)
                return done, carry, sums

            def put(row, done):
                quarter = row // QROWS
                slot = lax.rem(quarter - rank + 4, 4)
                for k in range(2):
                    out = done[k].astype(BF16)
                    at = k * 192 + start_lane
                    gsend[step, slot, row - quarter * QROWS, :, at : at + size] = out
                    flat[pl.ds(pl.multiple_of(row * SIDE + 32 * k, 32), 32), lanes] = out

            def loop(row, state):
                done, carry, sums = one(row, state[0], list(state[1]), True, True)
                put(row - 1, done)
                return carry, tuple(sums)

            zero = jnp.zeros((8, size), F32)
            _, carry, sums = one(0, no_carry(size), [zero] * 9, False, True)
            carry, sums = lax.fori_loop(1, SIDE - 1, loop, (carry, tuple(sums)))
            done, carry, sums = one(SIDE - 1, carry, list(sums), True, False)
            put(SIDE - 2, done)
            put(SIDE - 1, carry[0:2])
            for t in range(9):
                gtaps_ref[0, t : t + 1, lanes] = jnp.sum(sums[t], axis=0, keepdims=True)

    attend_all()
    for head in range(HEADS_DEV):

        @pl.when(step == head)
        def _():
            for slot in range(1, 4):
                g_copy(head, slot).start()
            keep_copy(head).start()
            if head == 0:
                load.wait()

    gw_buf[...] = jnp.zeros_like(gw_buf)

    def part(i, carry):
        rows = pl.ds(pl.multiple_of(i * 512, 512), 512)
        gw_buf[...] += dot_tn(flat[rows, :], hid_buf[rows, :])
        return carry

    lax.fori_loop(0, TOK // 512, part, 0)
    gw_ref[0] = jnp.transpose(gw_buf[...]).astype(BF16)

    @pl.when(step == HEADS_DEV - 1)
    def _():
        for head in range(HEADS_DEV):
            keep_copy(head).wait()
            for slot in range(1, 4):
                do_copy(head, slot).wait_send()
                g_copy(head, slot).wait()
        for half in range(2):
            stage_wait(3, half, *last_args)


def back_stage(tag, mixed_qkv, heads_out, lse, proj, taps, gheads, hidden, mixed_all):
    once = pl.Buffered(1)
    whole = lambda shape: pl.BlockSpec(shape, lambda s: (0,) * len(shape), pipeline_mode=once)
    hbm = pl.BlockSpec(memory_space=pl.ANY)
    return pl.pallas_call(
        back_kernel,
        grid=(HEADS_DEV,),
        in_specs=[
            pl.BlockSpec(memory_space=pltpu.SMEM),
            whole(mixed_qkv.shape),
            *[whole(o.shape) for o in heads_out],
            *[whole(v.shape) for v in lse],
            pl.BlockSpec((1, TOK, 192), lambda s: (s, 0, 0)),
            whole(taps.shape),
            *[hbm] * 5,
        ],
        out_specs=[
            hbm,
            hbm,
            pl.BlockSpec((1, D, 192), lambda s: (s, 0, 0)),
            pl.BlockSpec((1, 9, 192), lambda s: (s, 0, 0)),
        ],
        out_shape=[
            jax.ShapeDtypeStruct((TOK, D), BF16),
            jax.ShapeDtypeStruct((HEADS_DEV, 4, QROWS, 32, 384), BF16),
            jax.ShapeDtypeStruct((HEADS_DEV, D, 192), BF16),
            jax.ShapeDtypeStruct((HEADS_DEV, 9, 192), F32),
        ],
        scratch_shapes=[
            pltpu.VMEM((HEADS_DEV, 4, QROWS, 32, 128), BF16),
            pltpu.VMEM((HEADS_DEV, 4, QROWS, 32, 384), BF16),
            pltpu.VMEM((GROUPS, 1024, 128), BF16),
            pltpu.VMEM((GROUPS, 1024, 128), BF16),
            pltpu.VMEM((GROUPS, 1024, 128), BF16),
            pltpu.VMEM((GROUPS, 8, 1024), F32),
            pltpu.VMEM((16, 192), F32),
            pltpu.VMEM((1024, 128), F32),
            pltpu.VMEM((32, 2, 2, 32, 192), F32),
            pltpu.VMEM((TOK, 192), BF16),
            pltpu.VMEM((TOK, D), BF16),
            pltpu.VMEM((192, D), F32),
            pltpu.SemaphoreType.DMA((HEADS_DEV + 1,)),
            pltpu.SemaphoreType.DMA((HEADS_DEV,)),
            *[pltpu.SemaphoreType.DMA((HEADS_DEV, 4))] * 4,
            *[pltpu.SemaphoreType.DMA((2, 2))] * 2,
        ],
        input_output_aliases={14: 0},
        compiler_params=pltpu.CompilerParams(vmem_limit_bytes=VMEM_MAX, collective_id=0, has_side_effects=True),
        cost_estimate=pl.CostEstimate(flops=40_000_000_000, transcendentals=12_000_000, bytes_accessed=60_000_000),
        name="back_stage",
    )(tag, mixed_qkv, *heads_out, *lse, proj, taps, *gheads, hidden, mixed_all)


def last_kernel(info_ref, g_ref, w_ref, tok_ref, gafter_ref, mods_ref, perm_ref, out_ref, sums_ref, sum_ref, turn_ref, ghid_ref):
    scale = 1.0 + mods_ref[:, D : 2 * D]
    sum_ref[...] = jnp.zeros_like(sum_ref)
    for b in range(2):
        total = jnp.zeros((QROWS * 32, D), F32)
        groups = w_ref.shape[1]
        for slot in range(groups):
            source = lax.rem(info_ref[1] - slot + groups, groups)
            weight = w_ref[:, source].reshape(D, w_ref.shape[-1])
            for head in range(HEADS_DEV):
                part = g_ref[head, slot, :, :, b * 192 : b * 192 + 192].reshape(QROWS * 32, 192)
                total += dot_nt(part, weight[:, head * 192 : head * 192 + 192])
        ghid_ref[:, b] = total.reshape(QROWS, 32, D)

    def loop(i, carry):
        rows = pl.ds(pl.multiple_of(i * 256, 256), 256)
        ordered = dot_nn(perm_ref[...], tok_ref[rows, :])
        unit, rstd = normalised(ordered)
        grad = ghid_ref[pl.ds(i * 4, 4)].reshape(256, D)
        sum_ref[0] += half_sums(grad)
        sum_ref[1] += half_sums(grad * unit)
        inner = by_half(grad, scale)
        mean = jnp.mean(inner, axis=-1, keepdims=True)
        along = jnp.mean(inner * unit, axis=-1, keepdims=True)
        out = gafter_ref[rows, :] + rstd * (inner - mean - unit * along)
        for lane in range(D // 128):
            for r in range(4):
                for parity in range(2):
                    at = r * 64 + parity * 32
                    turn_ref[lane, pl.ds(r * 64 + parity, 32, stride=2), :] = out[
                        at : at + 32, lane * 128 : lane * 128 + 128
                    ]
            out_ref[rows, lane * 128 : lane * 128 + 128] = turn_ref[lane]
        return carry

    lax.fori_loop(0, QTOK // 256, loop, 0)
    sums_ref[...] = jnp.sum(sum_ref[...], axis=2)


def last_stage(info, grads, w_qkv, tok, gafter, mods, perm):
    space = pl.BlockSpec(memory_space=pltpu.VMEM)
    return pl.pallas_call(
        last_kernel,
        in_specs=[pl.BlockSpec(memory_space=pltpu.SMEM)] + [space] * 6,
        out_specs=[space] * 2,
        out_shape=[jax.ShapeDtypeStruct((QTOK, D), F32), jax.ShapeDtypeStruct((2, 2, D), F32)],
        scratch_shapes=[pltpu.VMEM((2, 2, 16, D), F32), pltpu.VMEM((D // 128, 256, 128), F32), pltpu.VMEM((QROWS, 2, 32, D), F32)],
        compiler_params=pltpu.CompilerParams(vmem_limit_bytes=VMEM_MAX),
        name="last_stage",
    )(info, grads, w_qkv, tok, gafter, mods, perm)


def tail_kernel(
    tag_ref,
    one_ref,
    two_ref,
    gate_ref,
    act_ref,
    cond_ref,
    w_mod_ref,
    time_ref,
    class_ref,
    gw_hbm,
    taps_hbm,
    gmod_ref,
    gtime_ref,
    gclass_ref,
    gqkv_ref,
    gtaps_ref,
    rows_buf,
    rows_recv,
    slots_buf,
    slots_recv,
    part_buf,
    part_recv,
    gw_recv,
    taps_recv,
    own_sem,
    sems_tp,
    sems_dp,
    sems_gw,
):
    tp_count, dp_count = rows_recv.shape[0], slots_recv.shape[0]
    rank, place = lax.axis_index("tp"), lax.axis_index("dp")
    barrier = greet("tp", tp_count)
    greet("dp", dp_count)
    pl.semaphore_wait(barrier, tp_count + dp_count - 2)

    def to_tp(source, target, kind, slot):
        return pltpu.make_async_remote_copy(
            source,
            target,
            sems_tp.at[kind, 0, slot],
            sems_tp.at[kind, 1, slot],
            device_id={"tp": lax.rem(rank + slot, tp_count)},
            device_id_type=MESH,
        )

    def to_dp(source, target, sems, slot):
        return pltpu.make_async_remote_copy(
            source,
            target,
            sems.at[0, slot],
            sems.at[1, slot],
            device_id={"dp": lax.rem(place + slot, dp_count)},
            device_id_type=MESH,
        )

    def each(count, body):
        def one(i, carry):
            body(i)
            return carry

        lax.fori_loop(1, count, one, 0)

    width = rows_buf.shape[2]
    parts = (one_ref[0], one_ref[1], two_ref[0], two_ref[1], two_ref[2], gate_ref[...])
    rows_buf[...] = jnp.zeros_like(rows_buf)
    slots_buf[...] = jnp.zeros_like(slots_buf)
    for group in range(tp_count):
        low = group * width
        while low < (group + 1) * width:
            kind, at = low // D, low % D
            high = min((group + 1) * width, (kind + 1) * D)
            rows_buf[group, 0:2, low - group * width : high - group * width] = parts[kind][:, at : at + high - low]
            low = high
    row_copy = lambda slot: to_tp(rows_buf.at[lax.rem(rank + slot, tp_count)], rows_recv.at[slot], 0, slot)
    each(tp_count, lambda slot: row_copy(slot).start())

    def gw_copies(slot):
        peer = lax.rem(place + slot, dp_count)
        out = [to_dp(gw_hbm.at[h, peer], gw_recv.at[slot, h], sems_gw.at[h], slot) for h in range(HEADS_DEV)]
        return out + [to_dp(taps_hbm.at[peer], taps_recv.at[slot], sems_gw.at[HEADS_DEV], slot)]

    owns = [pltpu.make_async_copy(gw_hbm.at[h, place], gw_recv.at[0, h], own_sem.at[h]) for h in range(HEADS_DEV)]
    owns.append(pltpu.make_async_copy(taps_hbm.at[place], taps_recv.at[0], own_sem.at[HEADS_DEV]))
    for own in owns:
        own.start()
    each(tp_count, lambda slot: row_copy(slot).wait())

    sums = [jnp.zeros((2, width), F32), jnp.zeros((2, width), F32)]
    for slot in range(tp_count):
        source = lax.rem(rank - slot + tp_count, tp_count)
        rows = rows_buf[rank, 0:2, :] if slot == 0 else rows_recv[slot, 0:2, :]
        low_half = source * QROWS < SIDE // 2
        sums = [sums[0] + jnp.where(low_half, rows, 0.0), sums[1] + jnp.where(low_half, 0.0, rows)]
    quads = jnp.concatenate(sums, axis=0)
    total = jnp.sum(quads, axis=0, keepdims=True)
    merged = jnp.concatenate([total, jnp.zeros((SLOTS - 1, width), F32)], axis=0)
    slots_buf[0:SLOTS, :] = jnp.where(tag_ref[0] == 1, merged, quads)
    slot_copy = lambda slot: to_dp(slots_buf, slots_recv.at[slot], sems_dp, slot)
    each(dp_count, lambda slot: slot_copy(slot).start())

    def start_gw(slot):
        for copy in gw_copies(slot):
            copy.start()

    each(dp_count, start_gw)
    slots_recv[0] = slots_buf[...]
    each(dp_count, lambda slot: slot_copy(slot).wait())

    mods = slots_recv[:, 0:SLOTS, :].reshape(dp_count * SLOTS, width)
    act = act_ref[...].reshape(dp_count * SLOTS, act_ref.shape[2])
    part = lax.dot_general(mods, w_mod_ref[...], (((1,), (1,)), ((), ())), precision=HIGHEST, preferred_element_type=F32)
    part_buf[...] = part
    part_copy = lambda slot: to_tp(part_buf, part_recv.at[slot], 1, slot)
    each(tp_count, lambda slot: part_copy(slot).start())
    gmod_ref[...] = lax.dot_general(act, mods, (((0,), (0,)), ((), ())), precision=HIGHEST, preferred_element_type=F32)
    each(tp_count, lambda slot: part_copy(slot).wait())
    grad = part_buf[...]
    for slot in range(1, tp_count):
        grad = grad + part_recv[slot]
    cond = cond_ref[...].reshape(grad.shape)
    gate = 1.0 / (1.0 + jnp.exp(-cond))
    grad = grad * (gate * (1.0 + cond * (1.0 - gate)))
    for index_ref, out_ref in ((time_ref, gtime_ref), (class_ref, gclass_ref)):
        rows = lax.broadcasted_iota(jnp.int32, (out_ref.shape[0], grad.shape[0]), 0)
        hits = jnp.where(rows == index_ref[...], 1.0, 0.0)
        out_ref[...] = lax.dot_general(hits, grad, (((1,), (0,)), ((), ())), precision=HIGHEST, preferred_element_type=F32)

    def wait_gw(slot):
        for copy in gw_copies(slot):
            copy.wait()

    each(dp_count, wait_gw)
    for own in owns:
        own.wait()
    for head in range(HEADS_DEV):
        total = jnp.sum(gw_recv[:, head].astype(F32), axis=0)
        gqkv_ref[:, head * 192 : head * 192 + 192] = total
    gtaps_ref[...] = jnp.sum(taps_recv[...], axis=0)


def tail_stage(tag, sums_one, sums_two, sums_gate, act, cond, w_mod, times, classes, gw, taps, tsteps, cls):
    tp_count = lax.axis_size("tp")
    dp_count, _, share = act.shape
    width = w_mod.shape[1]
    space = pl.BlockSpec(memory_space=pltpu.VMEM)
    hbm = pl.BlockSpec(memory_space=pl.ANY)
    return pl.pallas_call(
        tail_kernel,
        in_specs=[pl.BlockSpec(memory_space=pltpu.SMEM)] + [space] * 8 + [hbm] * 2,
        out_specs=[space] * 5,
        out_shape=[
            jax.ShapeDtypeStruct((share, width), F32),
            jax.ShapeDtypeStruct((tsteps, share), F32),
            jax.ShapeDtypeStruct((cls, share), F32),
            jax.ShapeDtypeStruct((share, HEADS_DEV * 192), F32),
            jax.ShapeDtypeStruct(taps.shape[1:], F32),
        ],
        scratch_shapes=[
            pltpu.VMEM((tp_count, 8, width), F32),
            pltpu.VMEM((tp_count, 8, width), F32),
            pltpu.VMEM((8, width), F32),
            pltpu.VMEM((dp_count, 8, width), F32),
            pltpu.VMEM((dp_count * SLOTS, share), F32),
            pltpu.VMEM((tp_count, dp_count * SLOTS, share), F32),
            pltpu.VMEM((dp_count, HEADS_DEV, share, 192), BF16),
            pltpu.VMEM((dp_count,) + taps.shape[1:], F32),
            pltpu.SemaphoreType.DMA((HEADS_DEV + 1,)),
            pltpu.SemaphoreType.DMA((2, 2, tp_count)),
            pltpu.SemaphoreType.DMA((2, dp_count)),
            pltpu.SemaphoreType.DMA((HEADS_DEV + 1, 2, dp_count)),
        ],
        compiler_params=pltpu.CompilerParams(vmem_limit_bytes=VMEM_MAX, collective_id=2, has_side_effects=True),
        name="tail_stage",
    )(tag, sums_one, sums_two, sums_gate, act, cond, w_mod, times, classes, gw, taps)


def per_device(
    tokens,
    cotangent,
    size_tags,
    time_index,
    class_index,
    time_table,
    class_table,
    w_mod,
    w_qkv,
    conv_qkv,
    w_out,
    w_up,
    conv_ffn,
    w_down,
):
    tp_count = lax.axis_size("tp")
    dp_count = lax.axis_size("dp")
    tp_rank = lax.axis_index("tp")
    dp_rank = lax.axis_index("dp")
    tag = size_tags[0]
    heads = w_out.shape[0] // HEAD_SIZE
    perm = parity_matrix()
    share = D // dp_count
    fold = 8

    def slice_rows(weight):
        size = weight.shape[0] // dp_count
        return lax.dynamic_slice_in_dim(weight, dp_rank * size, size, 0)

    def eight(stacked):
        if dp_count == fold:
            return stacked
        rows, width = stacked.shape[2:]
        inner = stacked.reshape(fold, dp_count // fold, tp_count, rows, width)
        return inner.transpose(0, 2, 1, 3, 4).reshape(fold, tp_count, rows * dp_count // fold, width)

    def gather_all(rows):
        stacked = lax.all_gather(rows, ("dp", "tp"), axis=0)
        return stacked.reshape((dp_count, tp_count) + rows.shape)

    packed = jnp.concatenate([slice_rows(w_up), slice_rows(w_down), slice_rows(w_out)], axis=0)
    packed = gather_all(packed)
    w_rows = jnp.concatenate([eight(packed[:, :, 0:share]), eight(packed[:, :, share : 2 * share])], axis=2)
    if dp_count == fold:
        w_rows = packed
    else:
        w_rows = jnp.concatenate([w_rows, jnp.zeros((fold, tp_count, 24, D), BF16)], axis=2)
    w_out_all = packed[:, :, 2 * share :].transpose(1, 0, 2, 3).reshape(tp_count, D // tp_count, D)
    turn = [[(i, (i + s) % tp_count) for i in range(tp_count)] for s in range(tp_count)]

    time_rows = jnp.take(time_table, time_index, axis=0).astype(F32)
    class_rows = jnp.take(class_table, class_index, axis=0).astype(F32)
    condition_all = time_rows + class_rows
    activated_all = jax.nn.silu(condition_all).astype(BF16)
    activated = lax.dynamic_slice_in_dim(activated_all, dp_rank * SLOTS, SLOTS, 0)
    mod_part = jnp.dot(activated, w_mod, preferred_element_type=F32)
    small = jnp.concatenate([mod_part.reshape(-1), conv_ffn.astype(F32).reshape(-1)])
    small = lax.all_gather(small.reshape(-1, 128), "tp", axis=0).reshape(tp_count, -1)
    modulation = small[:, : mod_part.size].reshape(tp_count, SLOTS, -1).transpose(1, 0, 2).reshape(SLOTS, 6 * D)
    conv_ffn_all = small[:, mod_part.size :].reshape(tp_count, 9, -1)
    per_quad = jnp.where(tag == 1, jnp.broadcast_to(modulation[0:1], modulation.shape), modulation)
    quads = per_quad.reshape(2, 2, 6 * D)
    quad_row = tp_rank * QROWS // (SIDE // 2)
    mods = lax.dynamic_index_in_dim(quads, quad_row, 0, keepdims=False)

    tag_word = size_tags.astype(jnp.int32)
    taps_qkv = conv_qkv.astype(F32)
    hidden_one, projected, mixed_qkv = first_stage(
        tag_word, tokens, quads[..., 0:D], quads[..., D : 2 * D], w_qkv, taps_qkv, perm
    )
    mixed_qkv = mixed_qkv.reshape(32, 2, 2, 32, 192 * heads)

    def exchange(slots):
        return [slots[0]] + [lax.ppermute(slots[s], "tp", turn[s]) for s in range(1, tp_count)]

    heads_out, lse, heads_in = [], [], []
    for head in range(heads):
        out, sums = attend_stage(tag_word, mixed_qkv, head)
        heads_out.append(out)
        lse.append(sums)
        wide = jnp.pad(out.reshape(SIDE, 32, 128), ((HALO, HALO), (0, 0), (0, 0)))
        places = [lax.rem(tp_rank + s, tp_count) * QROWS for s in range(tp_count)]
        heads_in += exchange([lax.dynamic_slice_in_dim(wide, p, XTOK // SIDE, 0) for p in places])
    w_qkv_mine, _, heads_in = lax.optimization_barrier((slice_rows(w_qkv), w_out_all, heads_in))
    w_qkv_all = eight(gather_all(w_qkv_mine))
    pad = ((HALO * SIDE, HALO * SIDE), (0, 0))
    tok_wide = lax.dynamic_slice_in_dim(jnp.pad(tokens, pad), tp_rank * QTOK, XTOK, 0)
    cot_wide = lax.dynamic_slice_in_dim(jnp.pad(cotangent, pad), tp_rank * QTOK, XTOK, 0)
    info = jnp.stack([tag, tp_rank]).astype(jnp.int32)
    mixed_q, up, slope, act, after, att, hidden_two, heads_rows, sums_gate = feed_stage(
        info, heads_in, w_out_all, tok_wide, cot_wide, mods, w_rows, conv_ffn_all, perm
    )
    cot_wide, w_qkv_all = lax.optimization_barrier((cot_wide, w_qkv_all))
    mixed, g_cat, *gheads, g_after, sums_two = feed_back_stage(
        tag_word, mixed_q, up, slope, act, w_rows, conv_ffn_all, cot_wide, hidden_two, after, att, heads_rows, w_out_all, mods, perm
    )
    tok_mine = lax.dynamic_slice_in_dim(tokens, tp_rank * QTOK, QTOK, 0)
    mixed, grads, grad_w, grad_taps = back_stage(
        tag_word, mixed_qkv, heads_out, lse, projected, taps_qkv, gheads, hidden_one, mixed
    )
    grad_tokens, sums_one = last_stage(info, grads, w_qkv_all, tok_mine, g_after, mods, perm)

    def regroup(values):
        rows, width = values.shape[-2:]
        if dp_count == fold:
            return values
        inner = values.reshape(fold, -1, dp_count // fold, rows * fold // dp_count, width)
        return inner.transpose(0, 2, 1, 3, 4).reshape(dp_count, -1, rows * fold // dp_count, width)

    def scatter(values, axis, dim=0):
        return lax.psum_scatter(values, axis, scatter_dimension=dim, tiled=True)

    def out_rows(values):
        return values.reshape(values.shape[0], tp_count, -1)[:, np.array([0, 3, 2, 1])].transpose(1, 2, 0)

    def sum_slots(slots):
        return sum(part.astype(F32) for part in exchange(slots))

    width = w_qkv.shape[1]
    taps_rows = grad_taps.transpose(1, 0, 2).reshape(9, dp_count, width // dp_count).transpose(1, 0, 2)
    taps_rows = jnp.pad(taps_rows, ((0, 0), (0, 7), (0, 128 - width // dp_count)))

    def from_here(values):
        turned = (dp_rank - lax.iota(jnp.int32, dp_count) + dp_count) % dp_count
        return jnp.take(values.reshape((dp_count, SLOTS) + values.shape[1:]), turned, axis=0)

    my_act = lax.dynamic_slice_in_dim(activated_all, dp_rank * share, share, 1).astype(F32)
    my_cond = lax.dynamic_slice_in_dim(condition_all, dp_rank * share, share, 1)
    summed_mod, grad_time, grad_class, summed_qkv, taps_sum = tail_stage(
        tag_word,
        sums_one,
        sums_two,
        sums_gate,
        from_here(my_act),
        from_here(my_cond),
        slice_rows(w_mod).astype(F32),
        from_here(time_index).reshape(1, -1),
        from_here(class_index).reshape(1, -1),
        grad_w.reshape(HEADS_DEV, dp_count, share, 192),
        taps_rows,
        time_table.shape[0],
        class_table.shape[0],
    )
    summed_conv_qkv = taps_sum[0:9, 0 : width // dp_count]
    if dp_count == fold:
        mine, _ = lax.optimization_barrier((scatter(g_cat, "dp")[0], grad_taps))
        rows_out = out_rows(mine[tp_count, 0:share]).reshape(tp_count, -1, D)
        slots = []
        for s in range(tp_count):
            part = lax.dynamic_index_in_dim(mine, lax.rem(tp_rank + s, tp_count), 0, keepdims=False)
            slots.append(jnp.concatenate([part, rows_out[s]], axis=0))
        mine = sum_slots(slots)
        summed_up, summed_down = mine[0:share], mine[share : 2 * share].T
        summed_conv_ffn = mine[2 * share : 2 * share + 9, 0:share]
        summed_out = mine[2 * share + 16 :].reshape(-1, share)
    else:
        per = D // fold
        body = g_cat[:, 0:tp_count]
        summed_up = scatter(scatter(regroup(body[:, :, 0:per]), "dp")[0], "tp")[0].astype(F32)
        summed_down = scatter(scatter(regroup(body[:, :, per : 2 * per]), "dp")[0], "tp")[0].astype(F32).T
        taps_part = body[:, :, 2 * per : 2 * per + 9, 0:per].transpose(1, 2, 0, 3).reshape(tp_count, 9, D)
        taps_part = scatter(taps_part.astype(F32), "tp")[0]
        summed_conv_ffn = scatter(taps_part, "dp", 1)
        g_out = scatter(regroup(g_cat[:, tp_count:, 0:per]), "dp")[0, 0]
        rows_out = out_rows(g_out)
        summed_out = sum_slots([rows_out[s] for s in range(tp_count)])

    return (
        mixed,
        grad_tokens,
        grad_time,
        grad_class,
        summed_mod,
        summed_qkv,
        summed_conv_qkv,
        summed_out,
        summed_up,
        summed_conv_ffn,
        summed_down,
    )


def solution(mesh):
    in_specs = (
        P("dp", None),
        P("dp", None),
        P("dp"),
        P(),
        P(),
        P(),
        P(),
        P(None, "tp"),
        P(None, "tp"),
        P(None, "tp"),
        P("tp", None),
        P(None, "tp"),
        P(None, "tp"),
        P("tp", None),
    )
    out_specs = (
        P("dp", None),
        P(("dp", "tp"), None),
        P(None, "dp"),
        P(None, "dp"),
        P("dp", "tp"),
        P("dp", "tp"),
        P(None, ("tp", "dp")),
        P("tp", "dp"),
        P("dp", "tp"),
        P(None, ("tp", "dp")),
        P("tp", "dp"),
    )
    return jax.shard_map(
        per_device, mesh=mesh, in_specs=in_specs, out_specs=out_specs, check_vma=False
    )
```

```python
from functools import partial

import jax
import jax.numpy as jnp
import numpy as np
from jax import lax
from jax.experimental import pallas as pl
from jax.experimental.pallas import tpu as pltpu
from jax.sharding import PartitionSpec as P

D = 768
HEAD_SIZE = 64
SIDE = 64
SLOTS = 4
TOK = SIDE * SIDE
HALO = 2
QROWS = 16
QTOK = QROWS * SIDE
XTOK = (QROWS + 2 * HALO) * SIDE
F32 = jnp.float32
BF16 = jnp.bfloat16
VMEM_MAX = 66_000_000
MESH = pl.DeviceIdType.MESH
HEADS_DEV = 3
GROUPS = 4
HIGHEST = lax.Precision.HIGHEST


def dot_nn(a, b):
    return lax.dot_general(a, b, (((1,), (0,)), ((), ())), preferred_element_type=F32)


def dot_nt(a, b):
    return lax.dot_general(a, b, (((1,), (1,)), ((), ())), preferred_element_type=F32)


def dot_tn(a, b):
    return lax.dot_general(a, b, (((0,), (0,)), ((), ())), preferred_element_type=F32)


def parity_matrix():
    one = np.zeros((SIDE, SIDE), np.float32)
    for parity in range(2):
        for j in range(SIDE // 2):
            one[parity * 32 + j, 2 * j + parity] = 1.0
    return jnp.asarray(np.kron(np.eye(4, dtype=np.float32), one), BF16)


def normalised(values):
    mean = jnp.mean(values, axis=-1, keepdims=True)
    centred = values - mean
    variance = jnp.mean(centred * centred, axis=-1, keepdims=True)
    rstd = lax.rsqrt(variance + 1e-06)
    return centred * rstd, rstd


def by_half(values, part):
    rows = values.shape[0]
    shaped = values.reshape(rows // 32, 2, 16, values.shape[-1])
    return (shaped * part[None, :, None, :]).reshape(values.shape)


def spread(part, rows):
    width = part.shape[-1]
    full = jnp.broadcast_to(part[None, :, None, :], (rows // 32, 2, 16, width))
    return full.reshape(rows, width)


def half_sums(values):
    return jnp.sum(values.reshape(values.shape[0] // 32, 2, 16, values.shape[-1]), axis=0)


def column_masks(tag, width):
    j = lax.broadcasted_iota(jnp.int32, (32, width), 0)
    split = tag == 0
    left = jnp.where((j == 0) | ((j == 16) & split), 0.0, 1.0)
    right = jnp.where((j == 31) | ((j == 15) & split), 0.0, 1.0)
    return left, right


def row_scales(tag, row):
    inside = (row >= 0) & (row < SIDE)
    down = jnp.where(inside & jnp.logical_not((tag == 0) & (row == 31)), 1.0, 0.0)
    up = jnp.where(inside & jnp.logical_not((tag == 0) & (row == 32)), 1.0, 0.0)
    return down, up


def conv_step(even, odd, masks, taps, down, up, carry):
    left, right = masks
    odd_left = pltpu.roll(odd, 1, 0) * left
    even_right = pltpu.roll(even, 31, 0) * right
    before_e, before_o, here_e, here_o = carry

    def terms(k):
        return (
            k[0] * odd_left + k[1] * even + k[2] * odd,
            k[0] * even + k[1] * odd + k[2] * even_right,
        )

    last = [t * up for t in taps[6:9]]
    middle = taps[3:6]
    first = [t * down for t in taps[0:3]]
    last_e, last_o = terms(last)
    mid_e, mid_o = terms(middle)
    first_e, first_o = terms(first)
    done = (before_e + last_e, before_o + last_o)
    return done, (here_e + mid_e, here_o + mid_o, first_e, first_o), (odd_left, even_right)


def no_carry(width):
    zero = jnp.zeros((32, width), F32)
    return (zero, zero, zero, zero)


def first_kernel(tag_ref, tok_ref, shift_ref, scale_ref, w_ref, taps_ref, perm_ref, hid_ref, proj_ref, mix_ref, field):
    step = pl.program_id(0)
    tag = tag_ref[0]
    width = w_ref.shape[1]

    @pl.when(step == 0)
    def _():
        field[pl.ds(0, SIDE), :] = jnp.zeros((SIDE, width), F32)
        field[pl.ds((SIDE + 1) * SIDE, SIDE), :] = jnp.zeros((SIDE, width), F32)

    @pl.when(step < 4)
    def _():
        half = step // 2
        shift = shift_ref[half]
        scale = 1.0 + scale_ref[half]

        def chunk(i, carry):
            rows = pl.ds(pl.multiple_of(i * 256, 256), 256)
            ordered = dot_nn(perm_ref[...], tok_ref[rows, :])
            unit, _ = normalised(ordered)
            hidden = (by_half(unit, scale) + spread(shift, 256)).astype(BF16)
            hid_ref[rows, :] = hidden
            out = dot_nn(hidden, w_ref[...])
            for head in range(proj_ref.shape[0]):
                proj_ref[head, rows, :] = out[:, head * 192 : head * 192 + 192]
            field[pl.ds(pl.multiple_of((step * 16 + 1) * SIDE + i * 256, 64), 256), :] = out
            return carry

        lax.fori_loop(0, 4, chunk, 0)

    @pl.when(step > 0)
    def _():
        base = (step - 1) * 16 - 1
        for lane in range(0, width, 128):
            size = min(128, width - lane)
            lanes = slice(lane, lane + size)
            masks = column_masks(tag, size)
            taps = [taps_ref[t : t + 1, lanes] for t in range(9)]

            def one(n, carry):
                row = base + n
                start = pl.multiple_of((row + 1) * SIDE, SIDE)
                even = field[pl.ds(start, 32), lanes]
                odd = field[pl.ds(start + 32, 32), lanes]
                down, up = row_scales(tag, row)
                done, carry, _ = conv_step(even, odd, masks, taps, down, up, carry)
                return done, carry

            def loop(n, carry):
                done, carry = one(n, carry)
                start = pl.multiple_of((n - 2) * SIDE, SIDE)
                for k in range(2):
                    out = done[k].astype(BF16)
                    mix_ref[pl.ds(start + 32 * k, 32), lanes] = out
                return carry

            _, carry = one(0, no_carry(size))
            _, carry = one(1, carry)
            lax.fori_loop(2, 18, loop, carry)


def first_stage(tag, tokens, shift, scale, w_qkv, taps, perm):
    width = w_qkv.shape[1]
    heads = width // 192
    whole = lambda shape: pl.BlockSpec(shape, lambda s: (0,) * len(shape))
    ahead = lambda w: pl.BlockSpec((1024, w), lambda s: (jnp.minimum(s, 3), 0))
    return pl.pallas_call(
        first_kernel,
        grid=(5,),
        in_specs=[
            pl.BlockSpec(memory_space=pltpu.SMEM),
            ahead(D),
            whole((2, 2, D)),
            whole((2, 2, D)),
            whole((D, width)),
            whole((9, width)),
            whole((256, 256)),
        ],
        out_specs=[
            ahead(D),
            pl.BlockSpec((heads, 1024, 192), lambda s: (0, jnp.minimum(s, 3), 0)),
            pl.BlockSpec((1024, width), lambda s: (jnp.maximum(s - 1, 0), 0)),
        ],
        out_shape=[
            jax.ShapeDtypeStruct((TOK, D), BF16),
            jax.ShapeDtypeStruct((heads, TOK, 192), F32),
            jax.ShapeDtypeStruct((TOK, width), BF16),
        ],
        scratch_shapes=[pltpu.VMEM(((SIDE + 2) * SIDE, width), F32)],
        compiler_params=pltpu.CompilerParams(vmem_limit_bytes=VMEM_MAX),
        name="first_stage",
    )(tag, tokens, shift, scale, w_qkv, taps, perm)


def to_row(column, count):
    return jnp.transpose(jnp.broadcast_to(column, (count, 128)))[0:1, :]


def attend_kernel(tag_ref, x_ref, o_ref, lse_ref, *, base):
    tag = tag_ref[0]
    parity = pl.program_id(0) % 2

    def run(split):
        def chunk(c, carry):
            query = x_ref[pl.ds(c * 8, 8), 0, 0, :, base : base + 64].reshape(256, 64)
            query = query * jnp.asarray(0.125, BF16)
            if split:
                rows = pl.ds((c // 2) * 16, 16)
                count = 512
            else:
                rows = pl.ds(0, 32)
                count = 1024
            keys = x_ref[rows, 0, 0, :, base + 64 : base + 128].reshape(count, 64)
            values = x_ref[rows, 0, 0, :, base + 128 : base + 192].reshape(count, 64)
            scores = dot_nt(query, keys)
            if split:
                qj = lax.broadcasted_iota(jnp.int32, (256, count), 0) & 16
                kj = lax.broadcasted_iota(jnp.int32, (256, count), 1) & 16
                scores = jnp.where(qj == kj, scores, -1e30)
            top = jnp.max(scores, axis=-1, keepdims=True)
            expo = jnp.exp(scores - top)
            total = jnp.sum(expo, axis=-1, keepdims=True)
            out = dot_nn(expo.astype(BF16), values) / total
            out = out.astype(BF16).reshape(8, 32, 64)
            for b in range(2):

                @pl.when(parity == b)
                def _():
                    o_ref[pl.ds(c * 8, 8), 0, :, b * 64 : b * 64 + 64] = out

            lse_ref[0, 0:1, pl.ds(pl.multiple_of(c * 256, 256), 256)] = to_row(top + jnp.log(total), 256)
            return carry

        lax.fori_loop(0, 4, chunk, 0)

    pl.when(tag == 1)(lambda: run(False))
    pl.when(tag != 1)(lambda: run(True))


def group_block(width):
    at = lambda g: jnp.minimum(g, 3)
    return pl.BlockSpec((32, 1, 1, 32, width), lambda g: (0, at(g) // 2, at(g) % 2, 0, 0))


def pair_block():
    return pl.BlockSpec((32, 1, 32, 128), lambda g: (0, jnp.minimum(g, 3) // 2, 0, 0))


def lse_block():
    return pl.BlockSpec((1, 8, 1024), lambda g: (jnp.minimum(g, 3), 0, 0))


def attend_stage(tag, mixed_qkv, head):
    out, lse = pl.pallas_call(
        partial(attend_kernel, base=head * 192),
        grid=(4,),
        in_specs=[pl.BlockSpec(memory_space=pltpu.SMEM), group_block(mixed_qkv.shape[-1])],
        out_specs=[pair_block(), lse_block()],
        out_shape=[
            jax.ShapeDtypeStruct((32, 2, 32, 128), BF16),
            jax.ShapeDtypeStruct((4, 8, 1024), F32),
        ],
        compiler_params=pltpu.CompilerParams(vmem_limit_bytes=VMEM_MAX),
        cost_estimate=pl.CostEstimate(flops=2_000_000_000, transcendentals=4_000_000, bytes_accessed=4_000_000),
        name="attend_stage",
    )(tag, mixed_qkv)
    return out, lse


def kernel_sums(acc, even, odd, odd_left, even_right, plain, scale, first):
    plain_e, plain_o = plain

    def fold(values):
        return jnp.sum(values.reshape(4, 8, values.shape[-1]), axis=0)

    terms = [
        fold(odd * plain_e) + fold(even_right * plain_o),
        fold(even * plain_e) + fold(odd * plain_o),
        fold(odd_left * plain_e) + fold(even * plain_o),
    ]
    out = list(acc)
    for t in range(3):
        term = terms[t] if scale is None else terms[t] * scale
        out[first + t] = acc[first + t] + term
    return out


POLY = (
    0.13241715506535054,
    0.12108811680396304,
    0.17555028579228482,
    -0.0796444980816301,
    0.3217932733518851,
    -0.21571441684424994,
    0.04451008654080756,
)


def gelu_parts(z):
    size = jnp.abs(z)
    t = 1.0 / (1.0 + 0.33 * size)
    expo = jnp.exp(z * z * -0.5)
    poly = POLY[6]
    for c in POLY[5::-1]:
        poly = poly * t + c
    tail = poly * t * expo
    cdf = jnp.where(z >= 0.0, 1.0 - tail, tail)
    value = z * cdf
    slope = cdf + z * (expo * 0.3989422804014327)
    return value, slope


def mod_part(mods_ref, i):
    return mods_ref[:, i * D : (i + 1) * D]


def feed_kernel(
    info_ref,
    *refs,
):
    heads_refs, refs = refs[0:12], refs[12:]
    feed_body(info_ref, heads_refs, *refs)


def feed_body(
    info_ref,
    heads_refs,
    w_out_ref,
    tok_ref,
    cot_ref,
    mods_ref,
    w_up_ref,
    w_down_ref,
    taps_ref,
    perm_ref,
    mixed_ref,
    up_ref,
    slope_ref,
    act_ref,
    after_ref,
    att_ref,
    hidden_out,
    heads_out,
    sums_ref,
    hidden_ref,
    hcat_ref,
    feed_ref,
    sum_ref,
):
    step = pl.program_id(0)
    tag = info_ref[0]
    first_row = info_ref[1] * QROWS - HALO
    chans = up_ref.shape[2]
    groups = w_out_ref.shape[0]
    heads = len(heads_refs) // groups
    rank = info_ref[1]

    @pl.when(step == 0)
    def _():
        gate_one, shift_two, scale_two = mod_part(mods_ref, 2), mod_part(mods_ref, 3), 1.0 + mod_part(mods_ref, 4)

        def unpack(i, carry):
            for g in range(groups):
                for head in range(heads):
                    ref = heads_refs[head * groups + g]
                    for b in range(2):
                        rows = pl.ds(pl.multiple_of(i * SIDE + b * 32, 32), 32)
                        lane = (g * heads + head) * 64
                        hcat_ref[rows, lane : lane + 64] = ref[i, :, b * 64 : b * 64 + 64]
            return carry

        lax.fori_loop(0, XTOK // SIDE, unpack, 0)

        def part(start, size):
            rows = pl.ds(start, size)
            perm = perm_ref[0:size, 0:size]
            ordered = dot_nn(perm, tok_ref[rows, :])
            attention = jnp.zeros((size, D), F32)
            width = heads * HEAD_SIZE
            for g in range(groups):
                source = lax.rem(rank - g + groups, groups)
                term = dot_nn(hcat_ref[rows, g * width : g * width + width], w_out_ref[source])
                attention = attention + term.astype(BF16).astype(F32)
            after = ordered + by_half(attention, gate_one)
            unit, _ = normalised(after)
            hidden = (by_half(unit, scale_two) + spread(shift_two, size)).astype(BF16)
            hidden_ref[rows, :] = hidden
            if size == 256:
                mine = pl.ds(pl.multiple_of(start - 128, 256), 256)
                att_ref[mine, :] = attention.astype(BF16)
                after_ref[mine, :] = after
                hidden_out[mine, :] = hidden
                heads_out[mine, :] = hcat_ref[rows, :]

        part(0, 128)
        part(XTOK - 128, 128)

        def loop(i, carry):
            part(pl.multiple_of(128 + i * 256, 128), 256)
            return carry

        lax.fori_loop(0, 4, loop, 0)
        feed_ref[...] = jnp.zeros_like(feed_ref)

    w_up = w_up_ref[...].reshape(D, chans)
    w_down = w_down_ref[...].reshape(chans, D)

    def up_loop(i, carry):
        rows = pl.ds(pl.multiple_of(i * 640, 128), 640)
        up_ref[0, rows, :] = dot_nn(hidden_ref[rows, :], w_up)
        return carry

    lax.fori_loop(0, 2, up_loop, 0)

    for lane in range(0, chans, 128):
        lanes = slice(lane, lane + 128)
        masks = column_masks(tag, 128)
        taps = [taps_ref[0, t : t + 1, lanes] for t in range(9)]

        def one(n, carry):
            start = pl.multiple_of(n * SIDE, SIDE)
            even = up_ref[0, pl.ds(start, 32), lanes]
            odd = up_ref[0, pl.ds(start + 32, 32), lanes]
            down, up = row_scales(tag, first_row + n)
            done, carry, _ = conv_step(even, odd, masks, taps, down, up, carry)
            return done, carry

        def loop(n, carry):
            done, carry = one(n, carry)
            for k in range(2):
                start = pl.multiple_of((n - 2) * SIDE + 32 * k, 32)
                value, slope = gelu_parts(done[k])
                act_ref[0, pl.ds(start, 32), lanes] = value.astype(BF16)
                slope_ref[0, pl.ds(start, 32), lanes] = slope
            return carry

        _, carry = one(0, no_carry(128))
        _, carry = one(1, carry)
        lax.fori_loop(2, QROWS + 2 * HALO, loop, carry)

    def token_loop(i, carry):
        rows = pl.ds(pl.multiple_of(i * 512, 512), 512)
        feed_ref[rows, :] += dot_nn(act_ref[0, pl.ds(pl.multiple_of(64 + i * 512, 64), 512), :], w_down)
        return carry

    lax.fori_loop(0, 2, token_loop, 0)

    @pl.when(step == pl.num_programs(0) - 1)
    def _():
        gate_two = mod_part(mods_ref, 5)
        sum_ref[...] = jnp.zeros_like(sum_ref)

        def loop(i, carry):
            rows = pl.ds(pl.multiple_of(i * 256, 256), 256)
            wide = pl.ds(pl.multiple_of(128 + i * 256, 128), 256)
            feed = feed_ref[rows, :]
            result = (after_ref[rows, :] + by_half(feed, gate_two)).astype(BF16)
            mixed_ref[rows, :] = dot_tn(perm_ref[...], result).astype(BF16)
            sum_ref[...] += half_sums(dot_nn(perm_ref[...], cot_ref[wide, :]) * feed)
            return carry

        lax.fori_loop(0, 4, loop, 0)
        sums_ref[...] = jnp.sum(sum_ref[...], axis=1)


def feed_stage(info, heads, w_out, tok, cot, mods, w_rows, taps, perm):
    dps, chunks, tall, chans = w_rows.shape
    per = D // dps
    once = pl.Buffered(1)
    whole = lambda shape: pl.BlockSpec(shape, lambda s: (0,) * len(shape), pipeline_mode=once)
    chunk = lambda rows: pl.BlockSpec((1, rows, chans), lambda s: (s, 0, 0))
    return pl.pallas_call(
        feed_kernel,
        grid=(chunks,),
        in_specs=[
            pl.BlockSpec(memory_space=pltpu.SMEM),
            *[whole(h.shape) for h in heads],
            whole(w_out.shape),
            whole((XTOK, D)),
            whole((XTOK, D)),
            whole((2, 6 * D)),
            pl.BlockSpec((dps, 1, per, chans), lambda s: (0, s, 0, 0)),
            pl.BlockSpec((dps, 1, per, chans), lambda s: (0, s, 1, 0)),
            chunk(9),
            whole((256, 256)),
        ],
        out_specs=[
            whole((QTOK, D)),
            chunk(XTOK),
            chunk(XTOK - 128),
            chunk(XTOK - 128),
            whole((QTOK, D)),
            whole((QTOK, D)),
            whole((QTOK, D)),
            whole((QTOK, D)),
            whole((2, D)),
        ],
        out_shape=[
            jax.ShapeDtypeStruct((QTOK, D), BF16),
            jax.ShapeDtypeStruct((chunks, XTOK, chans), F32),
            jax.ShapeDtypeStruct((chunks, XTOK - 128, chans), F32),
            jax.ShapeDtypeStruct((chunks, XTOK - 128, chans), BF16),
            jax.ShapeDtypeStruct((QTOK, D), F32),
            jax.ShapeDtypeStruct((QTOK, D), BF16),
            jax.ShapeDtypeStruct((QTOK, D), BF16),
            jax.ShapeDtypeStruct((QTOK, D), BF16),
            jax.ShapeDtypeStruct((2, D), F32),
        ],
        scratch_shapes=[
            pltpu.VMEM((XTOK, D), BF16),
            pltpu.VMEM((XTOK, D), BF16),
            pltpu.VMEM((QTOK, D), F32),
            pltpu.VMEM((2, 16, D), F32),
        ],
        compiler_params=pltpu.CompilerParams(vmem_limit_bytes=VMEM_MAX),
        cost_estimate=pl.CostEstimate(flops=20_000_000_000, transcendentals=8_000_000, bytes_accessed=80_000_000),
        name="feed_stage",
    )(info, *heads, w_out, tok, cot, mods, w_rows, w_rows, taps, perm)


def greet(axis, count):
    barrier = pltpu.get_barrier_semaphore()
    me = lax.axis_index(axis)

    def one(i, carry):
        pl.semaphore_signal(barrier, inc=1, device_id={axis: lax.rem(me + i, count)}, device_id_type=MESH)
        return carry

    lax.fori_loop(1, count, one, 0)
    return barrier


def pass_on(direction, stage, half, source, target, send, recv):
    rank = lax.axis_index("tp")
    quarter = rank - (stage - 1) * direction
    rows = pl.ds(pl.multiple_of(quarter * QTOK + half * 512, 512), 512)
    mine = pl.ds(half * 512, 512)
    at = (0 if direction > 0 else 1, half)
    return pltpu.make_async_remote_copy(
        source.at[mine] if stage == 1 else target.at[rows],
        target.at[rows],
        send.at[at],
        recv.at[at],
        device_id={"tp": rank + direction},
        device_id_type=MESH,
    )


def sends(direction, stage):
    rank = lax.axis_index("tp")
    quarter = rank - (stage - 1) * direction
    return (rank + direction >= 0) & (rank + direction < 4) & (quarter >= 0) & (quarter < 4)


def receives(direction, stage):
    quarter = lax.axis_index("tp") - stage * direction
    return (quarter >= 0) & (quarter < 4)


def stage_start(stage, half, source, target, send, recv):
    for direction in (1, -1):

        @pl.when(sends(direction, stage))
        def _():
            pass_on(direction, stage, half, source, target, send, recv).start()


def stage_wait(stage, half, source, target, send, recv, sent=True, received=True):
    for direction in (1, -1):
        if sent:

            @pl.when(sends(direction, stage))
            def _():
                pass_on(direction, stage, half, source, target, send, recv).wait_send()

        if received:

            @pl.when(receives(direction, stage))
            def _():
                rank = lax.axis_index("tp")
                quarter = rank - stage * direction
                rows = pl.ds(pl.multiple_of(quarter * QTOK + half * 512, 512), 512)
                at = (0 if direction > 0 else 1, half)
                pltpu.make_async_remote_copy(
                    target.at[rows],
                    target.at[rows],
                    send.at[at],
                    recv.at[at],
                    device_id={"tp": rank - direction},
                    device_id_type=MESH,
                ).wait_recv()


def feed_back_kernel(
    tag_ref,
    mixed_hbm,
    up_ref,
    slope_ref,
    act_ref,
    w_up_ref,
    w_down_ref,
    taps_ref,
    cot_ref,
    hidden_ref,
    after_ref,
    att_ref,
    heads_ref,
    w_out_ref,
    mods_ref,
    perm_ref,
    mixed_all,
    gcat_ref,
    g0_ref,
    g1_ref,
    g2_ref,
    gafter_ref,
    sums_ref,
    hidden_t,
    gfeed_ref,
    gfeed_t,
    ghid_ref,
    gact_ref,
    gup_ref,
    sum_ref,
    gtaps_ref,
    own_sem,
    one_send,
    one_recv,
    two_send,
    two_recv,
):
    step = pl.program_id(0)
    tag = tag_ref[0]
    rank = lax.axis_index("tp")
    first_row = rank * QROWS - HALO
    one_args = (mixed_hbm, mixed_all, one_send, one_recv)
    two_args = (mixed_hbm, mixed_all, two_send, two_recv)
    mine = pl.ds(pl.multiple_of(rank * QTOK, QTOK), QTOK)

    @pl.when(step == 0)
    def _():
        pl.semaphore_wait(greet("tp", 4), 3)
        for half in range(2):
            stage_start(1, half, *one_args)
        pltpu.make_async_copy(mixed_hbm, gup_ref, own_sem.at[0]).start()

    @pl.when(step == 2)
    def _():
        stage_wait(1, 0, *one_args, sent=False)
        stage_start(2, 0, *two_args)

    @pl.when(step == 3)
    def _():
        stage_wait(1, 1, *one_args, sent=False)
        stage_start(2, 1, *two_args)

    chans = up_ref.shape[2]
    dps, per = w_up_ref.shape[0], w_up_ref.shape[2]

    @pl.when(step == 0)
    def _():
        gate_two = mod_part(mods_ref, 5)

        def part(start, size):
            rows = pl.ds(start, size)
            perm = perm_ref[0:size, 0:size]
            gfeed_ref[rows, :] = by_half(dot_nn(perm, cot_ref[rows, :]), gate_two).astype(BF16)

        def loop(i, carry):
            part(pl.multiple_of(i * 256, 256), 256)
            return carry

        lax.fori_loop(0, XTOK // 256, loop, 0)
        hidden_t[...] = jnp.transpose(hidden_ref[...])
        gfeed_t[...] = jnp.transpose(gfeed_ref[pl.ds(128, QTOK), :])
        ghid_ref[...] = jnp.zeros_like(ghid_ref)
        pltpu.make_async_copy(mixed_hbm, gup_ref, own_sem.at[0]).wait()
        put = pltpu.make_async_copy(gup_ref, mixed_all.at[mine], own_sem.at[1])
        put.start()
        put.wait()

    @pl.when(step < pl.num_programs(0) - 1)
    def _():
        w_up = w_up_ref[...].reshape(D, chans)
        w_down = w_down_ref[...].reshape(chans, D)

        def gact_loop(i, carry):
            rows = pl.ds(pl.multiple_of(i * 576, 64), 576)
            out = dot_nt(gfeed_ref[pl.ds(pl.multiple_of(64 + i * 576, 64), 576), :], w_down)
            gact_ref[rows, :] = out * slope_ref[0, rows, :]
            return carry

        lax.fori_loop(0, 2, gact_loop, 0)

        for lane in range(0, chans, 128):
            lanes = slice(lane, lane + 128)
            masks = column_masks(tag, 128)
            taps = [taps_ref[0, 8 - t : 9 - t, lanes] for t in range(9)]

            def one(n, carry, sums):
                start = pl.multiple_of(n * SIDE, SIDE)
                low, high = pl.ds(start, 32), pl.ds(start + 32, 32)
                even, odd = gact_ref[low, lanes], gact_ref[high, lanes]
                row = first_row + 1 + n
                down, up = row_scales(tag, row)
                done, carry, shifted = conv_step(even, odd, masks, taps, down, up, carry)
                if sums is not None:
                    above = jnp.where((row == 0) | ((tag == 0) & (row == 32)), 0.0, 1.0)
                    below = jnp.where((row == SIDE - 1) | ((tag == 0) & (row == 31)), 0.0, 1.0)
                    for i, scale in ((0, above), (1, None), (2, below)):
                        at = pl.multiple_of((n + i) * SIDE, SIDE)
                        plain = (up_ref[0, pl.ds(at, 32), lanes], up_ref[0, pl.ds(at + 32, 32), lanes])
                        sums = kernel_sums(sums, even, odd, *shifted, plain, scale, 3 * i)
                return done, carry, sums

            def put(n, done):
                for k in range(2):
                    start = pl.multiple_of((n - 2) * SIDE + 32 * k, 32)
                    gup_ref[pl.ds(start, 32), lanes] = done[k].astype(BF16)

            def loop(n, state):
                done, carry, sums = one(n, state[0], list(state[1]))
                put(n, done)
                return carry, tuple(sums)

            zero = jnp.zeros((8, 128), F32)
            _, carry, _ = one(0, no_carry(128), None)
            _, carry, sums = one(1, carry, [zero] * 9)
            carry, sums = lax.fori_loop(2, QROWS + 1, loop, (carry, tuple(sums)))
            done, carry, _ = one(QROWS + 1, carry, None)
            put(QROWS + 1, done)
            for t in range(9):
                gtaps_ref[t : t + 1, lanes] = jnp.sum(sums[t], axis=0, keepdims=True)

        def token_loop(i, carry):
            rows = pl.ds(pl.multiple_of(i * 512, 512), 512)
            ghid_ref[rows, :] += dot_nt(gup_ref[rows, :], w_up)
            return carry

        lax.fori_loop(0, 2, token_loop, 0)

        def weight_loop(i, carry):
            rows = pl.ds(pl.multiple_of(i * 384, 128), 384)
            blocks = pl.ds(i * (dps // 2), dps // 2)
            out = dot_nn(hidden_t[rows, :], gup_ref[...])
            gcat_ref[blocks, 0, 0:per, :] = out.reshape(dps // 2, per, chans).astype(BF16)
            out = dot_nn(gfeed_t[rows, :], act_ref[0, pl.ds(64, QTOK), :])
            gcat_ref[blocks, 0, per : 2 * per, :] = out.reshape(dps // 2, per, chans).astype(BF16)
            return carry

        lax.fori_loop(0, 2, weight_loop, 0)
        sums = jnp.concatenate([gtaps_ref[0:9, :], jnp.zeros((7, chans), F32)], axis=0)
        for d in range(dps):
            part_sums = jnp.concatenate([sums[:, d * per : d * per + per], jnp.zeros((16, chans - per), F32)], axis=1)
            gcat_ref[d, 0, 2 * per : 2 * per + 16, :] = part_sums.astype(BF16)

    @pl.when(step == pl.num_programs(0) - 1)
    def _():
        gate_one, scale_two = mod_part(mods_ref, 2), 1.0 + mod_part(mods_ref, 4)
        groups = w_out_ref.shape[0]
        sum_ref[...] = jnp.zeros_like(sum_ref)

        def loop(i, carry):
            rows = pl.ds(pl.multiple_of(i * 256, 256), 256)
            wide = pl.ds(pl.multiple_of(128 + i * 256, 128), 256)
            cot = dot_nn(perm_ref[...], cot_ref[wide, :])
            unit, rstd = normalised(after_ref[rows, :])
            grad = ghid_ref[rows, :]
            sum_ref[1] += half_sums(grad)
            sum_ref[2] += half_sums(grad * unit)
            inner = by_half(grad, scale_two)
            mean = jnp.mean(inner, axis=-1, keepdims=True)
            along = jnp.mean(inner * unit, axis=-1, keepdims=True)
            gafter = cot + rstd * (inner - mean - unit * along)
            sum_ref[0] += half_sums(gafter * att_ref[rows, :].astype(F32))
            gafter_ref[rows, :] = gafter
            gatt = by_half(gafter, gate_one).astype(BF16)
            gup_ref[rows, :] = gatt
            for g in range(groups):
                target = lax.rem(rank + g, groups)
                out = dot_nt(gatt, w_out_ref[target]).astype(BF16).reshape(4, 2, 32, w_out_ref.shape[1])
                for head, ref in enumerate((g0_ref, g1_ref, g2_ref)):
                    for b in range(2):
                        ref[g, pl.ds(i * 4, 4), :, b * 64 : b * 64 + 64] = out[:, b, :, head * 64 : head * 64 + 64]
            return carry

        lax.fori_loop(0, 4, loop, 0)
        out = dot_tn(gup_ref[...], heads_ref[...])
        gcat_ref[:, 0, 0:per, :] = out.reshape(dps, per, D).astype(BF16)
        gcat_ref[:, 0, per:, :] = jnp.zeros((dps, per + 16, D), BF16)
        sums_ref[...] = jnp.sum(sum_ref[...], axis=2)
        for half in range(2):
            stage_wait(1, half, *one_args, received=False)
            stage_wait(2, half, *two_args)


def feed_back_stage(tag, mixed_q, up, slope, act, w_rows, taps, cot, hidden, after, att, heads, w_out, mods, perm):
    dps, chunks, tall, chans = w_rows.shape
    groups = w_out.shape[0]
    per = D // dps
    once = pl.Buffered(1)
    whole = lambda shape: pl.BlockSpec(shape, lambda s: (0,) * len(shape), pipeline_mode=once)
    at = lambda s: jnp.minimum(s, chunks - 1)
    chunk = lambda rows: pl.BlockSpec((1, rows, chans), lambda s: (at(s), 0, 0))
    sent = (groups, QROWS, 32, 128)
    return pl.pallas_call(
        feed_back_kernel,
        grid=(chunks + 1,),
        in_specs=[
            pl.BlockSpec(memory_space=pltpu.SMEM),
            pl.BlockSpec(memory_space=pl.ANY),
            chunk(XTOK),
            chunk(XTOK - 128),
            chunk(XTOK - 128),
            pl.BlockSpec((dps, 1, per, chans), lambda s: (0, at(s), 0, 0)),
            pl.BlockSpec((dps, 1, per, chans), lambda s: (0, at(s), 1, 0)),
            chunk(9),
            whole((XTOK, D)),
            whole((QTOK, D)),
            whole((QTOK, D)),
            whole((QTOK, D)),
            whole((QTOK, D)),
            whole(w_out.shape),
            whole((2, 6 * D)),
            whole((256, 256)),
        ],
        out_specs=[
            pl.BlockSpec(memory_space=pl.ANY),
            pl.BlockSpec((dps, 1, 2 * per + 16, chans), lambda s: (0, s, 0, 0)),
            whole(sent),
            whole(sent),
            whole(sent),
            whole((QTOK, D)),
            whole((3, 2, D)),
        ],
        out_shape=[
            jax.ShapeDtypeStruct((TOK, D), BF16),
            jax.ShapeDtypeStruct((dps, chunks + 1, 2 * per + 16, chans), BF16),
            jax.ShapeDtypeStruct(sent, BF16),
            jax.ShapeDtypeStruct(sent, BF16),
            jax.ShapeDtypeStruct(sent, BF16),
            jax.ShapeDtypeStruct((QTOK, D), F32),
            jax.ShapeDtypeStruct((3, 2, D), F32),
        ],
        scratch_shapes=[
            pltpu.VMEM((D, QTOK), BF16),
            pltpu.VMEM((XTOK, D), BF16),
            pltpu.VMEM((D, QTOK), BF16),
            pltpu.VMEM((QTOK, D), F32),
            pltpu.VMEM((XTOK - 128, chans), F32),
            pltpu.VMEM((QTOK, chans), BF16),
            pltpu.VMEM((3, 2, 16, D), F32),
            pltpu.VMEM((16, chans), F32),
            pltpu.SemaphoreType.DMA((2,)),
            *[pltpu.SemaphoreType.DMA((2, 2))] * 4,
        ],
        compiler_params=pltpu.CompilerParams(vmem_limit_bytes=VMEM_MAX, collective_id=1, has_side_effects=True),
        cost_estimate=pl.CostEstimate(flops=30_000_000_000, transcendentals=8_000_000, bytes_accessed=80_000_000),
        name="feed_back_stage",
    )(tag, mixed_q, up, slope, act, w_rows, w_rows, taps, cot, hidden, after, att, heads, w_out, mods, perm)


def back_kernel(
    tag_ref,
    x_ref,
    o0_ref,
    o1_ref,
    o2_ref,
    lse0_ref,
    lse1_ref,
    lse2_ref,
    proj_ref,
    taps_ref,
    gh0_hbm,
    gh1_hbm,
    gh2_hbm,
    hid_hbm,
    mixed_in,
    mixed_all,
    g_all,
    gw_ref,
    gtaps_ref,
    do_buf,
    gsend,
    kv_buf,
    qz_buf,
    zd_buf,
    row_buf,
    taps_buf,
    acc_ref,
    field,
    flat,
    hid_buf,
    gw_buf,
    local_sem,
    own_sem,
    do_send,
    do_recv,
    g_send,
    g_recv,
    m_send,
    m_recv,
):
    step = pl.program_id(0)
    tag = tag_ref[0]
    last_args = (mixed_all, mixed_all, m_send, m_recv)
    split = tag == 0
    rank = lax.axis_index("tp")
    gh_hbm = (gh0_hbm, gh1_hbm, gh2_hbm)

    def do_copy(head, slot):
        peer = lax.rem(rank + slot, 4)
        return pltpu.make_async_remote_copy(
            gh_hbm[head].at[slot],
            do_buf.at[head, slot],
            do_send.at[head, slot],
            do_recv.at[head, slot],
            device_id={"tp": peer},
            device_id_type=MESH,
        )

    def own_copy(head):
        return pltpu.make_async_copy(gh_hbm[head].at[0], do_buf.at[head, 0], own_sem.at[head])

    def g_copy(head, slot):
        peer = lax.rem(rank + slot, 4)
        return pltpu.make_async_remote_copy(
            gsend.at[head, slot],
            g_all.at[head, slot],
            g_send.at[head, slot],
            g_recv.at[head, slot],
            device_id={"tp": peer},
            device_id_type=MESH,
        )

    def keep_copy(head):
        return pltpu.make_async_copy(gsend.at[head, 0], g_all.at[head, 0], local_sem.at[head])

    load = pltpu.make_async_copy(hid_hbm, hid_buf, local_sem.at[HEADS_DEV])

    @pl.when(step == 0)
    def _():
        pl.semaphore_wait(greet("tp", 4), 3)
        for head in range(HEADS_DEV):
            for slot in range(1, 4):
                do_copy(head, slot).start()
            own_copy(head).start()
        load.start()

    @pl.when(step == 1)
    def _():
        for half in range(2):
            stage_start(3, half, *last_args)

    for head, (o_ref, lse_ref) in enumerate(((o0_ref, lse0_ref), (o1_ref, lse1_ref), (o2_ref, lse2_ref))):

        @pl.when(step == head)
        def _():
            base = head * 192
            taps_buf[0:9, :] = taps_ref[:, base : base + 192]
            zero = jnp.zeros((1024, 64), BF16)
            for g in range(GROUPS):
                a, b = g // 2, g % 2
                kv_buf[g] = x_ref[:, a, b, :, base + 64 : base + 192].reshape(1024, 128)
                query = x_ref[:, a, b, :, base : base + 64].reshape(1024, 64) * jnp.asarray(0.125, BF16)
                qz_buf[g] = jnp.concatenate([query, zero], axis=1)
            own_copy(head).wait()
            for slot in range(1, 4):
                do_copy(head, slot).wait_recv()
            for g in range(GROUPS):
                a, b = g // 2, g % 2
                for quarter in range(4):
                    slot = lax.rem(rank - quarter + 4, 4)
                    rows = slice(quarter * 256, quarter * 256 + 256)
                    grad = do_buf[head, slot, :, :, b * 64 : b * 64 + 64].reshape(8, 2, 32, 64)[:, a].reshape(256, 64)
                    zd_buf[g, rows, :] = jnp.concatenate([zero[0:256], grad], axis=1)
                    out = o_ref[quarter * 8 : quarter * 8 + 8, a, :, b * 64 : b * 64 + 64].reshape(256, 64)
                    delta = jnp.sum(grad.astype(F32) * out.astype(F32), axis=-1, keepdims=True)
                    row_buf[g, 0:1, rows] = to_row(delta, 256)
                row_buf[g, 1:2, :] = lse_ref[g, 0:1, :]

    def attend_all():
        def group(g, carry):
            acc_ref[...] = jnp.zeros_like(acc_ref)

            def chunk(c, carry):
                mine = pl.ds(pl.multiple_of(c * 256, 256), 256)
                delta = row_buf[g, 0:1, mine]
                lse = row_buf[g, 1:2, mine]
                place = lax.broadcasted_iota(jnp.int32, (1, 256), 1) & 16
                far = jnp.float32(1e30)
                by_j = [jnp.where(split & (place != 0), far, 0.0), jnp.where(split & (place == 0), far, 0.0)]
                by_i = [jnp.where(split & (c >= 2), far, 0.0), jnp.where(split & (c < 2), far, 0.0)]
                kv = kv_buf[g]
                query, grad = qz_buf[g, mine, :], zd_buf[g, mine, :]
                logits = dot_nt(kv, query).reshape(2, 16, 2, 16, 256)
                probs = [
                    [jnp.exp(logits[i, :, j] - (lse + by_i[i] + by_j[j])[:, None, :]) for j in range(2)] for i in range(2)
                ]
                probs = jnp.stack([jnp.stack(p, axis=1) for p in probs], axis=0).reshape(1024, 256)
                scores = (probs * (dot_nt(kv, grad) - delta)).astype(BF16)
                acc_ref[...] += dot_nn(scores, query) + dot_nn(probs.astype(BF16), grad)
                grad_query = dot_tn(scores, kv)[:, 0:64] * 0.125
                field[pl.ds(c * 8, 8), g // 2, g % 2, :, 0:64] = grad_query.reshape(8, 32, 64)
                return carry

            lax.fori_loop(0, 4, chunk, 0)
            field[:, g // 2, g % 2, :, 64:192] = acc_ref[...].reshape(32, 32, 128)
            return carry

        lax.fori_loop(0, GROUPS, group, 0)
        for start_lane, size in ((0, 128), (128, 64)):
            lanes = slice(start_lane, start_lane + size)
            masks = column_masks(tag, size)
            taps = [taps_buf[8 - t : 9 - t, lanes] for t in range(9)]

            def one(row, carry, sums, has_above, has_below):
                even = field[row // 2, row % 2, 0, :, lanes]
                odd = field[row // 2, row % 2, 1, :, lanes]
                down, up = row_scales(tag, row)
                done, carry, shifted = conv_step(even, odd, masks, taps, down, up, carry)
                for i in range(3):
                    if (i == 0 and not has_above) or (i == 2 and not has_below):
                        continue
                    at = pl.multiple_of((row + i - 1) * SIDE, SIDE)
                    plain = (proj_ref[0, pl.ds(at, 32), lanes], proj_ref[0, pl.ds(at + 32, 32), lanes])
                    scale = (up, None, down)[i]
                    sums = kernel_sums(sums, even, odd, *shifted, plain, scale, 3 * i)
                return done, carry, sums

            def put(row, done):
                quarter = row // QROWS
                slot = lax.rem(quarter - rank + 4, 4)
                for k in range(2):
                    out = done[k].astype(BF16)
                    at = k * 192 + start_lane
                    gsend[step, slot, row - quarter * QROWS, :, at : at + size] = out
                    flat[step, pl.ds(pl.multiple_of(row * SIDE + 32 * k, 32), 32), lanes] = out

            def loop(row, state):
                done, carry, sums = one(row, state[0], list(state[1]), True, True)
                put(row - 1, done)
                return carry, tuple(sums)

            zero = jnp.zeros((8, size), F32)
            _, carry, sums = one(0, no_carry(size), [zero] * 9, False, True)
            carry, sums = lax.fori_loop(1, SIDE - 1, loop, (carry, tuple(sums)))
            done, carry, sums = one(SIDE - 1, carry, list(sums), True, False)
            put(SIDE - 2, done)
            put(SIDE - 1, carry[0:2])
            for t in range(9):
                gtaps_ref[0, t : t + 1, lanes] = jnp.sum(sums[t], axis=0, keepdims=True)

    attend_all()
    for head in range(HEADS_DEV):

        @pl.when(step == head)
        def _():
            for slot in range(1, 4):
                g_copy(head, slot).start()
            keep_copy(head).start()

    @pl.when(step == HEADS_DEV - 1)
    def _():
        def weight(head, carry):
            gw_buf[...] = jnp.zeros_like(gw_buf)

            def part(i, carry):
                rows = pl.ds(pl.multiple_of(i * 512, 512), 512)
                gw_buf[...] += dot_tn(flat[head, rows, :], hid_buf[rows, :])
                return carry

            lax.fori_loop(0, TOK // 512, part, 0)
            gw_ref[head] = jnp.transpose(gw_buf[...]).astype(BF16)
            return carry

        load.wait()
        lax.fori_loop(0, HEADS_DEV, weight, 0)
        for head in range(HEADS_DEV):
            keep_copy(head).wait()
            for slot in range(1, 4):
                do_copy(head, slot).wait_send()
                g_copy(head, slot).wait()
        for half in range(2):
            stage_wait(3, half, *last_args)


def back_stage(tag, mixed_qkv, heads_out, lse, proj, taps, gheads, hidden, mixed_all):
    once = pl.Buffered(1)
    whole = lambda shape: pl.BlockSpec(shape, lambda s: (0,) * len(shape), pipeline_mode=once)
    hbm = pl.BlockSpec(memory_space=pl.ANY)
    return pl.pallas_call(
        back_kernel,
        grid=(HEADS_DEV,),
        in_specs=[
            pl.BlockSpec(memory_space=pltpu.SMEM),
            whole(mixed_qkv.shape),
            *[whole(o.shape) for o in heads_out],
            *[whole(v.shape) for v in lse],
            pl.BlockSpec((1, TOK, 192), lambda s: (s, 0, 0)),
            whole(taps.shape),
            *[hbm] * 5,
        ],
        out_specs=[
            hbm,
            hbm,
            whole((HEADS_DEV, D, 192)),
            pl.BlockSpec((1, 9, 192), lambda s: (s, 0, 0)),
        ],
        out_shape=[
            jax.ShapeDtypeStruct((TOK, D), BF16),
            jax.ShapeDtypeStruct((HEADS_DEV, 4, QROWS, 32, 384), BF16),
            jax.ShapeDtypeStruct((HEADS_DEV, D, 192), BF16),
            jax.ShapeDtypeStruct((HEADS_DEV, 9, 192), F32),
        ],
        scratch_shapes=[
            pltpu.VMEM((HEADS_DEV, 4, QROWS, 32, 128), BF16),
            pltpu.VMEM((HEADS_DEV, 4, QROWS, 32, 384), BF16),
            pltpu.VMEM((GROUPS, 1024, 128), BF16),
            pltpu.VMEM((GROUPS, 1024, 128), BF16),
            pltpu.VMEM((GROUPS, 1024, 128), BF16),
            pltpu.VMEM((GROUPS, 8, 1024), F32),
            pltpu.VMEM((16, 192), F32),
            pltpu.VMEM((1024, 128), F32),
            pltpu.VMEM((32, 2, 2, 32, 192), F32),
            pltpu.VMEM((HEADS_DEV, TOK, 192), BF16),
            pltpu.VMEM((TOK, D), BF16),
            pltpu.VMEM((192, D), F32),
            pltpu.SemaphoreType.DMA((HEADS_DEV + 1,)),
            pltpu.SemaphoreType.DMA((HEADS_DEV,)),
            *[pltpu.SemaphoreType.DMA((HEADS_DEV, 4))] * 4,
            *[pltpu.SemaphoreType.DMA((2, 2))] * 2,
        ],
        input_output_aliases={14: 0},
        compiler_params=pltpu.CompilerParams(vmem_limit_bytes=VMEM_MAX, collective_id=0, has_side_effects=True),
        cost_estimate=pl.CostEstimate(flops=40_000_000_000, transcendentals=12_000_000, bytes_accessed=60_000_000),
        name="back_stage",
    )(tag, mixed_qkv, *heads_out, *lse, proj, taps, *gheads, hidden, mixed_all)


def last_kernel(info_ref, g_ref, w_ref, tok_ref, gafter_ref, mods_ref, perm_ref, out_ref, sums_ref, sum_ref, turn_ref, ghid_ref):
    scale = 1.0 + mods_ref[:, D : 2 * D]
    sum_ref[...] = jnp.zeros_like(sum_ref)
    for b in range(2):
        total = jnp.zeros((QROWS * 32, D), F32)
        groups = w_ref.shape[1]
        for slot in range(groups):
            source = lax.rem(info_ref[1] - slot + groups, groups)
            weight = w_ref[:, source].reshape(D, w_ref.shape[-1])
            for head in range(HEADS_DEV):
                part = g_ref[head, slot, :, :, b * 192 : b * 192 + 192].reshape(QROWS * 32, 192)
                total += dot_nt(part, weight[:, head * 192 : head * 192 + 192])
        ghid_ref[:, b] = total.reshape(QROWS, 32, D)

    def loop(i, carry):
        rows = pl.ds(pl.multiple_of(i * 256, 256), 256)
        ordered = dot_nn(perm_ref[...], tok_ref[rows, :])
        unit, rstd = normalised(ordered)
        grad = ghid_ref[pl.ds(i * 4, 4)].reshape(256, D)
        sum_ref[0] += half_sums(grad)
        sum_ref[1] += half_sums(grad * unit)
        inner = by_half(grad, scale)
        mean = jnp.mean(inner, axis=-1, keepdims=True)
        along = jnp.mean(inner * unit, axis=-1, keepdims=True)
        out = gafter_ref[rows, :] + rstd * (inner - mean - unit * along)
        for lane in range(D // 128):
            for r in range(4):
                for parity in range(2):
                    at = r * 64 + parity * 32
                    turn_ref[lane, pl.ds(r * 64 + parity, 32, stride=2), :] = out[
                        at : at + 32, lane * 128 : lane * 128 + 128
                    ]
            out_ref[rows, lane * 128 : lane * 128 + 128] = turn_ref[lane]
        return carry

    lax.fori_loop(0, QTOK // 256, loop, 0)
    sums_ref[...] = jnp.sum(sum_ref[...], axis=2)


def last_stage(info, grads, w_qkv, tok, gafter, mods, perm):
    space = pl.BlockSpec(memory_space=pltpu.VMEM)
    return pl.pallas_call(
        last_kernel,
        in_specs=[pl.BlockSpec(memory_space=pltpu.SMEM)] + [space] * 6,
        out_specs=[space] * 2,
        out_shape=[jax.ShapeDtypeStruct((QTOK, D), F32), jax.ShapeDtypeStruct((2, 2, D), F32)],
        scratch_shapes=[pltpu.VMEM((2, 2, 16, D), F32), pltpu.VMEM((D // 128, 256, 128), F32), pltpu.VMEM((QROWS, 2, 32, D), F32)],
        compiler_params=pltpu.CompilerParams(vmem_limit_bytes=VMEM_MAX),
        name="last_stage",
    )(info, grads, w_qkv, tok, gafter, mods, perm)


def tail_kernel(
    tag_ref,
    one_ref,
    two_ref,
    gate_ref,
    act_ref,
    cond_ref,
    w_mod_ref,
    time_ref,
    class_ref,
    gw_hbm,
    taps_hbm,
    gmod_ref,
    gtime_ref,
    gclass_ref,
    gqkv_ref,
    gtaps_ref,
    rows_buf,
    rows_recv,
    slots_buf,
    slots_recv,
    part_buf,
    part_recv,
    gw_recv,
    taps_recv,
    own_sem,
    sems_tp,
    sems_dp,
    sems_gw,
):
    tp_count, dp_count = rows_recv.shape[0], slots_recv.shape[0]
    rank, place = lax.axis_index("tp"), lax.axis_index("dp")
    barrier = greet("tp", tp_count)
    greet("dp", dp_count)
    pl.semaphore_wait(barrier, tp_count + dp_count - 2)

    def to_tp(source, target, kind, slot):
        return pltpu.make_async_remote_copy(
            source,
            target,
            sems_tp.at[kind, 0, slot],
            sems_tp.at[kind, 1, slot],
            device_id={"tp": lax.rem(rank + slot, tp_count)},
            device_id_type=MESH,
        )

    def to_dp(source, target, sems, slot):
        return pltpu.make_async_remote_copy(
            source,
            target,
            sems.at[0, slot],
            sems.at[1, slot],
            device_id={"dp": lax.rem(place + slot, dp_count)},
            device_id_type=MESH,
        )

    def each(count, body):
        def one(i, carry):
            body(i)
            return carry

        lax.fori_loop(1, count, one, 0)

    width = rows_buf.shape[2]
    parts = (one_ref[0], one_ref[1], two_ref[0], two_ref[1], two_ref[2], gate_ref[...])
    rows_buf[...] = jnp.zeros_like(rows_buf)
    slots_buf[...] = jnp.zeros_like(slots_buf)
    for group in range(tp_count):
        low = group * width
        while low < (group + 1) * width:
            kind, at = low // D, low % D
            high = min((group + 1) * width, (kind + 1) * D)
            rows_buf[group, 0:2, low - group * width : high - group * width] = parts[kind][:, at : at + high - low]
            low = high
    def gw_copies(slot, kinds=range(HEADS_DEV + 1)):
        peer = lax.rem(place + slot, dp_count)
        out = []
        for kind in kinds:
            if kind < HEADS_DEV:
                out.append(to_dp(gw_hbm.at[kind, peer], gw_recv.at[slot, kind], sems_gw.at[kind], slot))
            else:
                out.append(to_dp(taps_hbm.at[peer], taps_recv.at[slot], sems_gw.at[kind], slot))
        return out

    row_copy = lambda slot: to_tp(rows_buf.at[lax.rem(rank + slot, tp_count)], rows_recv.at[slot], 0, slot)
    each(tp_count, lambda slot: row_copy(slot).start())
    each(dp_count, lambda slot: gw_copies(slot, [0])[0].start())

    owns = [pltpu.make_async_copy(gw_hbm.at[h, place], gw_recv.at[0, h], own_sem.at[h]) for h in range(HEADS_DEV)]
    owns.append(pltpu.make_async_copy(taps_hbm.at[place], taps_recv.at[0], own_sem.at[HEADS_DEV]))
    for own in owns:
        own.start()
    each(tp_count, lambda slot: row_copy(slot).wait())

    sums = [jnp.zeros((2, width), F32), jnp.zeros((2, width), F32)]
    for slot in range(tp_count):
        source = lax.rem(rank - slot + tp_count, tp_count)
        rows = rows_buf[rank, 0:2, :] if slot == 0 else rows_recv[slot, 0:2, :]
        low_half = source * QROWS < SIDE // 2
        sums = [sums[0] + jnp.where(low_half, rows, 0.0), sums[1] + jnp.where(low_half, 0.0, rows)]
    quads = jnp.concatenate(sums, axis=0)
    total = jnp.sum(quads, axis=0, keepdims=True)
    merged = jnp.concatenate([total, jnp.zeros((SLOTS - 1, width), F32)], axis=0)
    slots_buf[0:SLOTS, :] = jnp.where(tag_ref[0] == 1, merged, quads)
    slot_copy = lambda slot: to_dp(slots_buf, slots_recv.at[slot], sems_dp, slot)
    each(dp_count, lambda slot: slot_copy(slot).start())

    def start_gw(slot):
        for copy in gw_copies(slot, range(1, HEADS_DEV + 1)):
            copy.start()

    each(dp_count, start_gw)
    slots_recv[0] = slots_buf[...]
    each(dp_count, lambda slot: slot_copy(slot).wait())

    mods = slots_recv[:, 0:SLOTS, :].reshape(dp_count * SLOTS, width)
    act = act_ref[...].reshape(dp_count * SLOTS, act_ref.shape[2])
    part = lax.dot_general(mods, w_mod_ref[...], (((1,), (1,)), ((), ())), precision=HIGHEST, preferred_element_type=F32)
    part_buf[...] = part
    part_copy = lambda slot: to_tp(part_buf, part_recv.at[slot], 1, slot)
    each(tp_count, lambda slot: part_copy(slot).start())
    gmod_ref[...] = lax.dot_general(act, mods, (((0,), (0,)), ((), ())), precision=HIGHEST, preferred_element_type=F32)
    each(tp_count, lambda slot: part_copy(slot).wait())
    grad = part_buf[...]
    for slot in range(1, tp_count):
        grad = grad + part_recv[slot]
    cond = cond_ref[...].reshape(grad.shape)
    gate = 1.0 / (1.0 + jnp.exp(-cond))
    grad = grad * (gate * (1.0 + cond * (1.0 - gate)))
    for index_ref, out_ref in ((time_ref, gtime_ref), (class_ref, gclass_ref)):
        columns = lax.broadcasted_iota(jnp.int32, (grad.shape[0], out_ref.shape[1]), 1)
        hits = jnp.where(columns == index_ref[...], 1.0, 0.0)
        out_ref[...] = lax.dot_general(grad, hits, (((0,), (0,)), ((), ())), precision=HIGHEST, preferred_element_type=F32)

    def wait_gw(slot):
        for copy in gw_copies(slot):
            copy.wait()

    each(dp_count, wait_gw)
    for own in owns:
        own.wait()
    for head in range(HEADS_DEV):
        total = jnp.sum(gw_recv[:, head].astype(F32), axis=0)
        gqkv_ref[:, head * 192 : head * 192 + 192] = total
    gtaps_ref[...] = jnp.sum(taps_recv[...], axis=0)


def tail_stage(tag, sums_one, sums_two, sums_gate, act, cond, w_mod, times, classes, gw, taps, tsteps, cls):
    tp_count = lax.axis_size("tp")
    dp_count, _, share = act.shape
    width = w_mod.shape[1]
    space = pl.BlockSpec(memory_space=pltpu.VMEM)
    hbm = pl.BlockSpec(memory_space=pl.ANY)
    return pl.pallas_call(
        tail_kernel,
        in_specs=[pl.BlockSpec(memory_space=pltpu.SMEM)] + [space] * 8 + [hbm] * 2,
        out_specs=[space] * 5,
        out_shape=[
            jax.ShapeDtypeStruct((share, width), F32),
            jax.ShapeDtypeStruct((share, tsteps), F32),
            jax.ShapeDtypeStruct((share, cls), F32),
            jax.ShapeDtypeStruct((share, HEADS_DEV * 192), F32),
            jax.ShapeDtypeStruct(taps.shape[1:], F32),
        ],
        scratch_shapes=[
            pltpu.VMEM((tp_count, 8, width), F32),
            pltpu.VMEM((tp_count, 8, width), F32),
            pltpu.VMEM((8, width), F32),
            pltpu.VMEM((dp_count, 8, width), F32),
            pltpu.VMEM((dp_count * SLOTS, share), F32),
            pltpu.VMEM((tp_count, dp_count * SLOTS, share), F32),
            pltpu.VMEM((dp_count, HEADS_DEV, share, 192), BF16),
            pltpu.VMEM((dp_count,) + taps.shape[1:], F32),
            pltpu.SemaphoreType.DMA((HEADS_DEV + 1,)),
            pltpu.SemaphoreType.DMA((2, 2, tp_count)),
            pltpu.SemaphoreType.DMA((2, dp_count)),
            pltpu.SemaphoreType.DMA((HEADS_DEV + 1, 2, dp_count)),
        ],
        compiler_params=pltpu.CompilerParams(vmem_limit_bytes=VMEM_MAX, collective_id=2, has_side_effects=True),
        name="tail_stage",
    )(tag, sums_one, sums_two, sums_gate, act, cond, w_mod, times, classes, gw, taps)


def per_device(
    tokens,
    cotangent,
    size_tags,
    time_index,
    class_index,
    time_table,
    class_table,
    w_mod,
    w_qkv,
    conv_qkv,
    w_out,
    w_up,
    conv_ffn,
    w_down,
):
    tp_count = lax.axis_size("tp")
    dp_count = lax.axis_size("dp")
    tp_rank = lax.axis_index("tp")
    dp_rank = lax.axis_index("dp")
    tag = size_tags[0]
    heads = w_out.shape[0] // HEAD_SIZE
    perm = parity_matrix()
    share = D // dp_count
    fold = 8

    def slice_rows(weight):
        size = weight.shape[0] // dp_count
        return lax.dynamic_slice_in_dim(weight, dp_rank * size, size, 0)

    def eight(stacked):
        if dp_count == fold:
            return stacked
        rows, width = stacked.shape[2:]
        inner = stacked.reshape(fold, dp_count // fold, tp_count, rows, width)
        return inner.transpose(0, 2, 1, 3, 4).reshape(fold, tp_count, rows * dp_count // fold, width)

    def gather_all(rows):
        stacked = lax.all_gather(rows, ("dp", "tp"), axis=0)
        return stacked.reshape((dp_count, tp_count) + rows.shape)

    packed = jnp.concatenate([slice_rows(w_up), slice_rows(w_down), slice_rows(w_out)], axis=0)
    packed = gather_all(packed)
    w_rows = jnp.concatenate([eight(packed[:, :, 0:share]), eight(packed[:, :, share : 2 * share])], axis=2)
    if dp_count == fold:
        w_rows = packed
    else:
        w_rows = jnp.concatenate([w_rows, jnp.zeros((fold, tp_count, 24, D), BF16)], axis=2)
    w_out_all = packed[:, :, 2 * share :].transpose(1, 0, 2, 3).reshape(tp_count, D // tp_count, D)
    turn = [[(i, (i + s) % tp_count) for i in range(tp_count)] for s in range(tp_count)]

    time_rows = jnp.take(time_table, time_index, axis=0).astype(F32)
    class_rows = jnp.take(class_table, class_index, axis=0).astype(F32)
    condition_all = time_rows + class_rows
    activated_all = jax.nn.silu(condition_all).astype(BF16)
    activated = lax.dynamic_slice_in_dim(activated_all, dp_rank * SLOTS, SLOTS, 0)
    mod_part = jnp.dot(activated, w_mod, preferred_element_type=F32)
    small = jnp.concatenate([mod_part.reshape(-1), conv_ffn.astype(F32).reshape(-1)])
    small = lax.all_gather(small.reshape(-1, 128), "tp", axis=0).reshape(tp_count, -1)
    modulation = small[:, : mod_part.size].reshape(tp_count, SLOTS, -1).transpose(1, 0, 2).reshape(SLOTS, 6 * D)
    conv_ffn_all = small[:, mod_part.size :].reshape(tp_count, 9, -1)
    per_quad = jnp.where(tag == 1, jnp.broadcast_to(modulation[0:1], modulation.shape), modulation)
    quads = per_quad.reshape(2, 2, 6 * D)
    quad_row = tp_rank * QROWS // (SIDE // 2)
    mods = lax.dynamic_index_in_dim(quads, quad_row, 0, keepdims=False)

    tag_word = size_tags.astype(jnp.int32)
    taps_qkv = conv_qkv.astype(F32)
    hidden_one, projected, mixed_qkv = first_stage(
        tag_word, tokens, quads[..., 0:D], quads[..., D : 2 * D], w_qkv, taps_qkv, perm
    )
    mixed_qkv = mixed_qkv.reshape(32, 2, 2, 32, 192 * heads)

    def exchange(slots):
        return [slots[0]] + [lax.ppermute(slots[s], "tp", turn[s]) for s in range(1, tp_count)]

    heads_out, lse, heads_in = [], [], []
    for head in range(heads):
        out, sums = attend_stage(tag_word, mixed_qkv, head)
        heads_out.append(out)
        lse.append(sums)
        wide = jnp.pad(out.reshape(SIDE, 32, 128), ((HALO, HALO), (0, 0), (0, 0)))
        places = [lax.rem(tp_rank + s, tp_count) * QROWS for s in range(tp_count)]
        heads_in += exchange([lax.dynamic_slice_in_dim(wide, p, XTOK // SIDE, 0) for p in places])
    w_qkv_mine, _, heads_in = lax.optimization_barrier((slice_rows(w_qkv), w_out_all, heads_in))
    w_qkv_all = eight(gather_all(w_qkv_mine))
    pad = ((HALO * SIDE, HALO * SIDE), (0, 0))
    tok_wide = lax.dynamic_slice_in_dim(jnp.pad(tokens, pad), tp_rank * QTOK, XTOK, 0)
    cot_wide = lax.dynamic_slice_in_dim(jnp.pad(cotangent, pad), tp_rank * QTOK, XTOK, 0)
    info = jnp.stack([tag, tp_rank]).astype(jnp.int32)
    mixed_q, up, slope, act, after, att, hidden_two, heads_rows, sums_gate = feed_stage(
        info, heads_in, w_out_all, tok_wide, cot_wide, mods, w_rows, conv_ffn_all, perm
    )
    cot_wide, w_qkv_all = lax.optimization_barrier((cot_wide, w_qkv_all))
    mixed, g_cat, *gheads, g_after, sums_two = feed_back_stage(
        tag_word, mixed_q, up, slope, act, w_rows, conv_ffn_all, cot_wide, hidden_two, after, att, heads_rows, w_out_all, mods, perm
    )
    tok_mine = lax.dynamic_slice_in_dim(tokens, tp_rank * QTOK, QTOK, 0)
    mixed, grads, grad_w, grad_taps = back_stage(
        tag_word, mixed_qkv, heads_out, lse, projected, taps_qkv, gheads, hidden_one, mixed
    )
    grad_tokens, sums_one = last_stage(info, grads, w_qkv_all, tok_mine, g_after, mods, perm)

    def regroup(values):
        rows, width = values.shape[-2:]
        if dp_count == fold:
            return values
        inner = values.reshape(fold, -1, dp_count // fold, rows * fold // dp_count, width)
        return inner.transpose(0, 2, 1, 3, 4).reshape(dp_count, -1, rows * fold // dp_count, width)

    def scatter(values, axis, dim=0):
        return lax.psum_scatter(values, axis, scatter_dimension=dim, tiled=True)

    def out_rows(values):
        return values.reshape(values.shape[0], tp_count, -1)[:, np.array([0, 3, 2, 1])].transpose(1, 2, 0)

    def sum_slots(slots):
        return sum(part.astype(F32) for part in exchange(slots))

    width = w_qkv.shape[1]
    taps_rows = grad_taps.transpose(1, 0, 2).reshape(9, dp_count, width // dp_count).transpose(1, 0, 2)
    taps_rows = jnp.pad(taps_rows, ((0, 0), (0, 7), (0, 128 - width // dp_count)))

    def from_here(values):
        turned = (dp_rank - lax.iota(jnp.int32, dp_count) + dp_count) % dp_count
        return jnp.take(values.reshape((dp_count, SLOTS) + values.shape[1:]), turned, axis=0)

    my_act = lax.dynamic_slice_in_dim(activated_all, dp_rank * share, share, 1).astype(F32)
    my_cond = lax.dynamic_slice_in_dim(condition_all, dp_rank * share, share, 1)
    summed_mod, grad_time, grad_class, summed_qkv, taps_sum = tail_stage(
        tag_word,
        sums_one,
        sums_two,
        sums_gate,
        from_here(my_act),
        from_here(my_cond),
        slice_rows(w_mod).astype(F32),
        from_here(time_index).reshape(-1, 1),
        from_here(class_index).reshape(-1, 1),
        grad_w.reshape(HEADS_DEV, dp_count, share, 192),
        taps_rows,
        time_table.shape[0],
        class_table.shape[0],
    )
    summed_conv_qkv = taps_sum[0:9, 0 : width // dp_count]
    if dp_count == fold:
        mine, _ = lax.optimization_barrier((scatter(g_cat, "dp")[0], grad_taps))
        rows_out = out_rows(mine[tp_count, 0:share]).reshape(tp_count, -1, D)
        slots = []
        for s in range(tp_count):
            part = lax.dynamic_index_in_dim(mine, lax.rem(tp_rank + s, tp_count), 0, keepdims=False)
            slots.append(jnp.concatenate([part, rows_out[s]], axis=0))
        mine = sum_slots(slots)
        summed_up, summed_down = mine[0:share], mine[share : 2 * share].T
        summed_conv_ffn = mine[2 * share : 2 * share + 9, 0:share]
        summed_out = mine[2 * share + 16 :].reshape(-1, share)
    else:
        per = D // fold
        body = g_cat[:, 0:tp_count]
        summed_up = scatter(scatter(regroup(body[:, :, 0:per]), "dp")[0], "tp")[0].astype(F32)
        summed_down = scatter(scatter(regroup(body[:, :, per : 2 * per]), "dp")[0], "tp")[0].astype(F32).T
        taps_part = body[:, :, 2 * per : 2 * per + 9, 0:per].transpose(1, 2, 0, 3).reshape(tp_count, 9, D)
        taps_part = scatter(taps_part.astype(F32), "tp")[0]
        summed_conv_ffn = scatter(taps_part, "dp", 1)
        g_out = scatter(regroup(g_cat[:, tp_count:, 0:per]), "dp")[0, 0]
        rows_out = out_rows(g_out)
        summed_out = sum_slots([rows_out[s] for s in range(tp_count)])

    return (
        mixed,
        grad_tokens,
        grad_time.T,
        grad_class.T,
        summed_mod,
        summed_qkv,
        summed_conv_qkv,
        summed_out,
        summed_up,
        summed_conv_ffn,
        summed_down,
    )


def solution(mesh):
    in_specs = (
        P("dp", None),
        P("dp", None),
        P("dp"),
        P(),
        P(),
        P(),
        P(),
        P(None, "tp"),
        P(None, "tp"),
        P(None, "tp"),
        P("tp", None),
        P(None, "tp"),
        P(None, "tp"),
        P("tp", None),
    )
    out_specs = (
        P("dp", None),
        P(("dp", "tp"), None),
        P(None, "dp"),
        P(None, "dp"),
        P("dp", "tp"),
        P("dp", "tp"),
        P(None, ("tp", "dp")),
        P("tp", "dp"),
        P("dp", "tp"),
        P(None, ("tp", "dp")),
        P("tp", "dp"),
    )
    return jax.shard_map(
        per_device, mesh=mesh, in_specs=in_specs, out_specs=out_specs, check_vma=False
    )
```
